32 devices in a mesh: seq: 16 (over z, x, core), tp: 2 (over y).
Axes of the slice: x: 2, y: 2, z: 4, core: 2. Of those that a mesh axis runs over, the one named last changes fastest.
Arguments:
- hidden_in: bfloat16 [2048, 4096], P('seq', 'tp'), may hold values from -64 to 64
- span_order: int32 [16], replicated, may hold values from 0 to 15, each once
- norm_gain: bfloat16 [4096], P('tp'), may hold values from 0.099609375 to 1.8984375
- w_query: bfloat16 [4096, 4096], P('seq', 'tp'), may hold values from -0.09375 to 0.09375
- bias_query: bfloat16 [4096], P('tp'), may hold values from -14 to 14
- key_value_weight: bfloat16 [4096, 2, 1024], P('seq', None, 'tp'), may hold values from -0.09375 to 0.09375
- bias_kv: bfloat16 [2, 1024], P(None, 'tp'), may hold values from -14 to 14
- w_out: bfloat16 [4096, 4096], P('tp', 'seq'), may hold values from -0.09375 to 0.09375
- post_gain: bfloat16 [4096], P('tp'), may hold values from 0.099609375 to 1.8984375
Outputs:
- attn_out: bfloat16 [2048, 4096], P('seq', 'tp')
- normed: bfloat16 [2048, 4096], P('seq', 'tp')
The draws below stay inside these ranges and needn't reach their ends.
Inputs may be any that keep to these rules, and one draw needn't show every extreme that they name: Each span number appears once; row r of hidden_in belongs to span span_order[r // 128].
All inputs are finite; a program needn't handle non-finite values.
Results may differ from the reference program's by a relative error of at most 0.014.
Values may be sent and summed in bfloat16 or wider, within the bound.
A program may use at most 128 MiB of HBM per device.

```python
import math
import jax
import jax.numpy as jnp
from jax import lax

MODEL_WIDTH = 4096
QUERY_HEADS = 32
KEY_VALUE_HEADS = 8
HEAD_SIZE = 128
GROUP = 4
TOK_DEV = 128
SEQ = 2048
N_SEQ = 16
N_TP = 2


def draw_hidden_in(key, part):
    base_key, column_key, row_key = jax.random.split(key, 3)
    column_ids = jnp.arange(MODEL_WIDTH, dtype=jnp.float32) / MODEL_WIDTH
    base = jnp.clip(jax.random.normal(base_key, (SEQ, MODEL_WIDTH), jnp.float32), -4.0, 4.0)
    ramp = jnp.exp(0.5 * math.log(3.0) * column_ids)
    ramp = ramp / jnp.mean(ramp)
    columns = jnp.exp(jax.random.uniform(column_key, (MODEL_WIDTH,), jnp.float32, -1.1513, 1.1513))
    rows = jnp.exp(jax.random.uniform(row_key, (SEQ, 1), jnp.float32, -1.1513, 1.1513))
    field = jnp.clip(base * rows * (columns * ramp)[None, :], -64.0, 64.0)
    return field.astype(jnp.bfloat16)


def draw_bias_query(key, part):
    random_jitter = jax.random.normal(jax.random.fold_in(key, 11), (QUERY_HEADS * HEAD_SIZE,), jnp.float32)
    return jnp.clip(0.5 * random_jitter, -2.0, 2.0).astype(jnp.bfloat16)


def draw_bias_kv(key, part):
    random_jitter = jax.random.normal(jax.random.fold_in(key, 13), (2, KEY_VALUE_HEADS * HEAD_SIZE), jnp.float32)
    return jnp.clip(0.5 * random_jitter, -2.0, 2.0).astype(jnp.bfloat16)


def steps_of(stream_key, extent, pieces, low, top_value):
    factor_of = 1.0
    for position, shards_of in pieces:
        heights = jax.random.uniform(jax.random.fold_in(jax.random.fold_in(stream_key, 6), position), (shards_of,), jnp.float32, low / len(pieces), top_value / len(pieces))
        factor_of = factor_of * jnp.repeat(jnp.exp(heights), extent[position] // shards_of).reshape((-1,) + (1,) * (len(extent) - 1 - position))
    return factor_of


def noise(rng, dims, deviation, most, cuts=(), held_as=jnp.bfloat16):
    factor_of = steps_of(rng, dims, cuts, -0.22, 0.18) if cuts else 1.0
    result = jax.random.normal(rng, dims, jnp.float32) * deviation * factor_of
    return jnp.minimum(jnp.maximum(result, -most), most).astype(held_as)


def setup_inputs(seed: int = 0) -> dict:
    arg_keys = jax.random.split(jax.random.key(seed), 10)
    hidden_in = draw_hidden_in(jax.random.fold_in(arg_keys[9], 71), 0)
    span_order = jax.random.permutation(arg_keys[1], N_SEQ).astype(jnp.int32)
    norm_gain = jnp.clip(1.0 + 0.18 * jax.random.normal(arg_keys[2], (MODEL_WIDTH,), jnp.float32), 0.099609375, 1.8984375).astype(jnp.bfloat16)
    w_query = noise(arg_keys[3], (MODEL_WIDTH, QUERY_HEADS * HEAD_SIZE), MODEL_WIDTH ** -0.5, 0.09375, ((0, 16), (1, 2)))
    bias_query = draw_bias_query(jax.random.fold_in(arg_keys[9], 71), 0)
    key_value_weight = noise(arg_keys[5], (MODEL_WIDTH, 2, KEY_VALUE_HEADS * HEAD_SIZE), MODEL_WIDTH ** -0.5, 0.09375, ((0, 16), (2, 2)))
    bias_kv = draw_bias_kv(jax.random.fold_in(arg_keys[9], 71), 0)
    w_out = noise(arg_keys[7], (QUERY_HEADS * HEAD_SIZE, MODEL_WIDTH), (QUERY_HEADS * HEAD_SIZE) ** -0.5, 0.09375, ((0, 2), (1, 16)))
    post_gain = jnp.clip(1.0 + 0.18 * jax.random.normal(arg_keys[8], (MODEL_WIDTH,), jnp.float32), 0.099609375, 1.8984375).astype(jnp.bfloat16)
    return dict(hidden_in=hidden_in, span_order=span_order, norm_gain=norm_gain, w_query=w_query, bias_query=bias_query, key_value_weight=key_value_weight, bias_kv=bias_kv, w_out=w_out, post_gain=post_gain)


eps = 1e-06
rope_base = 1000000.0

def apply_rotary(field, token_positions):
    half = field.shape[-1] // 2
    inverse = jnp.exp(-math.log(rope_base) * jnp.arange(half, dtype=jnp.float32) / half)
    angles = token_positions.astype(jnp.float32)[:, None] * inverse[None, :]
    cosine = jnp.cos(angles)[:, None, :]
    sine = jnp.sin(angles)[:, None, :]
    first = field[..., :half]
    second = field[..., half:]
    return jnp.concatenate([first * cosine - second * sine, second * cosine + first * sine], axis=-1)

def reference(hidden_in, span_order, norm_gain, w_query, bias_query, key_value_weight, bias_kv, w_out, post_gain):
    sequence_length = hidden_in.shape[0]
    row_ids = jnp.arange(sequence_length, dtype=jnp.int32)
    token_positions = (span_order[row_ids // TOK_DEV] * TOK_DEV + row_ids % TOK_DEV).astype(jnp.int32)
    local = hidden_in.astype(jnp.float32)
    meansq = lax.optimization_barrier(jnp.mean(local * local, axis=1, keepdims=True))
    normed_in = (local * lax.rsqrt(meansq + eps) * norm_gain.astype(jnp.float32)[None, :]).astype(jnp.bfloat16)
    query_proj = jnp.dot(normed_in, w_query, preferred_element_type=jnp.float32) + bias_query.astype(jnp.float32)[None, :]
    queries = apply_rotary(query_proj.reshape(sequence_length, QUERY_HEADS, HEAD_SIZE), token_positions).astype(jnp.bfloat16)
    key_projected = jnp.dot(normed_in, key_value_weight[:, 0, :], preferred_element_type=jnp.float32) + bias_kv[0].astype(jnp.float32)[None, :]
    value_projected = jnp.dot(normed_in, key_value_weight[:, 1, :], preferred_element_type=jnp.float32) + bias_kv[1].astype(jnp.float32)[None, :]
    rotated_keys = apply_rotary(key_projected.reshape(sequence_length, KEY_VALUE_HEADS, HEAD_SIZE), token_positions).astype(jnp.bfloat16)
    value_rows = value_projected.astype(jnp.bfloat16).reshape(sequence_length, KEY_VALUE_HEADS, HEAD_SIZE)
    query_major = queries.transpose(1, 0, 2)
    key_major = jnp.repeat(rotated_keys.transpose(1, 0, 2), GROUP, axis=0)
    value_major = jnp.repeat(value_rows.transpose(1, 0, 2), GROUP, axis=0)
    allowed = token_positions[None, :] <= token_positions[:, None]
    scale = 1.0 / math.sqrt(HEAD_SIZE)

    def one_head(triple):
        query_one, key_one, value_one = triple
        scores = jnp.dot(query_one, key_one.T, preferred_element_type=jnp.float32) * scale
        scores = jnp.where(allowed, scores, -jnp.inf)
        peak = lax.optimization_barrier(jnp.max(scores, axis=1, keepdims=True))
        weights = jnp.where(allowed, jnp.exp(scores - peak), 0.0)
        totals = lax.optimization_barrier(jnp.sum(weights, axis=1, keepdims=True))
        summed = jnp.dot(weights.astype(jnp.bfloat16), value_one, preferred_element_type=jnp.float32)
        return (summed / totals).astype(jnp.bfloat16)
    attended = lax.map(one_head, (query_major, key_major, value_major))
    attended = attended.transpose(1, 0, 2).reshape(sequence_length, QUERY_HEADS * HEAD_SIZE)
    part_rows = QUERY_HEADS * HEAD_SIZE // N_TP
    mixed = jnp.zeros((sequence_length, MODEL_WIDTH), jnp.float32)
    for group in range(N_TP):
        lower = group * part_rows
        piece = jnp.dot(attended[:, lower:lower + part_rows], w_out[lower:lower + part_rows, :], preferred_element_type=jnp.float32)
        mixed = mixed + lax.optimization_barrier(piece.astype(jnp.bfloat16)).astype(jnp.float32)
    attn_out = mixed.astype(jnp.bfloat16)
    stream = local + mixed
    post_sq = lax.optimization_barrier(jnp.mean(stream * stream, axis=1, keepdims=True))
    normed = (stream * lax.rsqrt(post_sq + eps) * post_gain.astype(jnp.float32)[None, :]).astype(jnp.bfloat16)
    return (attn_out, normed)
```

```python
import math

import jax
import jax.numpy as jnp
from jax import lax
from jax.experimental import pallas as pl
from jax.experimental.pallas import tpu as pltpu
from jax.sharding import PartitionSpec as P

MODEL_WIDTH = 4096
HEAD_SIZE = 128
GROUP = 4


eps = 1e-06
rope_base = 1000000.0


def apply_rotary(field, token_positions):
    half = field.shape[-1] // 2
    inverse = jnp.exp(-math.log(rope_base) * jnp.arange(half, dtype=jnp.float32) / half)
    angles = token_positions.astype(jnp.float32)[:, None] * inverse[None, :]
    cosine = jnp.cos(angles)[:, None, :]
    sine = jnp.sin(angles)[:, None, :]
    first = field[..., :half]
    second = field[..., half:]
    return jnp.concatenate(
        [first * cosine - second * sine, second * cosine + first * sine], axis=-1
    )


def span_lookup(order, devices):
    table_ids = jnp.arange(order.shape[0], dtype=jnp.int32)
    return jnp.sum(jnp.where(devices[:, None] == table_ids[None, :], order[None, :], 0), axis=1)


def per_device_by_span(
    hidden_in,
    span_order,
    norm_gain,
    w_query,
    bias_query,
    key_value_weight,
    bias_kv,
    w_out,
    post_gain,
):
    tok_rows = hidden_in.shape[0]
    seq_index = lax.axis_index("seq")
    own_span = span_lookup(span_order, jnp.full((1,), seq_index, jnp.int32))[0]
    token_positions = own_span * tok_rows + jnp.arange(tok_rows, dtype=jnp.int32)
    local = hidden_in.astype(jnp.float32)
    raw_rows, gains = (
        lax.all_gather(hidden_in, "tp", axis=1, tiled=True),
        lax.all_gather(norm_gain[None, :], "tp", axis=1, tiled=True),
    )
    full_rows = raw_rows.astype(jnp.float32)
    meansq = jnp.mean(full_rows * full_rows, axis=1, keepdims=True)
    normed_in = (full_rows * lax.rsqrt(meansq + eps) * gains.astype(jnp.float32)).astype(
        jnp.bfloat16
    )
    columns = normed_in
    query_proj = jnp.dot(
        columns,
        lax.all_gather(w_query, "seq", axis=0, tiled=True),
        preferred_element_type=jnp.float32,
    )
    columns = normed_in
    pair_proj = jnp.einsum(
        "tr,rkc->tkc",
        columns,
        lax.all_gather(key_value_weight, "seq", axis=0, tiled=True),
        preferred_element_type=jnp.float32,
    )
    query_heads = w_query.shape[1] // HEAD_SIZE
    kv_heads = key_value_weight.shape[2] // HEAD_SIZE
    query_proj = query_proj + bias_query.astype(jnp.float32)[None, :]
    queries = apply_rotary(
        query_proj.reshape(tok_rows, query_heads, HEAD_SIZE), token_positions
    ).astype(jnp.bfloat16)
    pair_proj = pair_proj + bias_kv.astype(jnp.float32)[None, :, :]
    rotated_keys = apply_rotary(
        pair_proj[:, 0, :].reshape(tok_rows, kv_heads, HEAD_SIZE), token_positions
    )
    rotated_keys = rotated_keys.astype(jnp.bfloat16).reshape(tok_rows, kv_heads * HEAD_SIZE)
    value_rows = pair_proj[:, 1, :].astype(jnp.bfloat16)
    grouped = (
        queries.reshape(tok_rows, kv_heads, GROUP, HEAD_SIZE)
        .transpose(1, 2, 0, 3)
        .reshape(kv_heads, GROUP * tok_rows, HEAD_SIZE)
    )
    query_pos = jnp.tile(token_positions, GROUP)
    last_query = jnp.max(token_positions)
    scale = 1.0 / math.sqrt(HEAD_SIZE)
    start_state = (
        jnp.full((kv_heads, GROUP * tok_rows), -1e30, jnp.float32),
        jnp.zeros((kv_heads, GROUP * tok_rows), jnp.float32),
        jnp.zeros((kv_heads, GROUP * tok_rows, HEAD_SIZE), jnp.float32),
    )
    key_piece = lax.all_gather(rotated_keys, "seq", axis=0, tiled=True)
    value_piece = lax.all_gather(value_rows, "seq", axis=0, tiled=True)
    count = key_piece.shape[0]
    block = math.gcd(count, 1536)

    def visit(step, state):
        first = step * block
        key_block = lax.dynamic_slice_in_dim(key_piece, first, block, 0).reshape(
            block, kv_heads, HEAD_SIZE
        )
        value_block = lax.dynamic_slice_in_dim(value_piece, first, block, 0).reshape(
            block, kv_heads, HEAD_SIZE
        )
        row_ids = first + jnp.arange(block, dtype=jnp.int32)
        key_pos = span_lookup(span_order, row_ids // tok_rows) * tok_rows + row_ids % tok_rows

        def update(current):
            maxima, totals, sums = current
            scores = (
                jnp.einsum("kqd,nkd->kqn", grouped, key_block, preferred_element_type=jnp.float32)
                * scale
            )
            allowed = (key_pos[None, :] <= query_pos[:, None])[None, :, :]
            scores = jnp.where(allowed, scores, -1e30)
            fresh = jnp.maximum(maxima, jnp.max(scores, axis=2))
            weights = jnp.where(allowed, jnp.exp(scores - fresh[:, :, None]), 0.0)
            factor = jnp.exp(maxima - fresh)
            totals = totals * factor + jnp.sum(weights, axis=2)
            sums = sums * factor[:, :, None] + jnp.einsum(
                "kqn,nkd->kqd",
                weights.astype(jnp.bfloat16),
                value_block,
                preferred_element_type=jnp.float32,
            )
            return (fresh, totals, sums)

        return lax.cond(jnp.min(key_pos) <= last_query, update, lambda current: current, state)

    maxima, totals, sums = lax.fori_loop(0, count // block, visit, start_state)
    attended = (sums / totals[:, :, None]).astype(jnp.bfloat16)
    attended = (
        attended.reshape(kv_heads, GROUP, tok_rows, HEAD_SIZE)
        .transpose(2, 0, 1, 3)
        .reshape(tok_rows, query_heads * HEAD_SIZE)
    )
    partial_out = jnp.dot(
        attended,
        lax.all_gather(w_out, "seq", axis=1, tiled=True),
        preferred_element_type=jnp.float32,
    )
    mixed = lax.psum_scatter(
        partial_out.astype(jnp.bfloat16), "tp", scatter_dimension=1, tiled=True
    ).astype(jnp.float32)
    attn_out = mixed.astype(jnp.bfloat16)
    stream = local + mixed
    post_sq = lax.psum(jnp.sum(stream * stream, axis=1), "tp")
    normed = (
        stream
        * lax.rsqrt(post_sq / MODEL_WIDTH + eps)[:, None]
        * post_gain.astype(jnp.float32)[None, :]
    ).astype(jnp.bfloat16)
    return (attn_out, normed)


MESH = pl.DeviceIdType.MESH
CORES = 2
PLANE = 4
PIECES = 2
PAIR = 2 * HEAD_SIZE


def at(z, x, c):
    return z * PLANE + x * CORES + c


class Traffic:
    def __init__(self, send_sem, peer):
        self.send_sem, self.peer, self.started = send_sem, peer, []

    def send(self, source, landing, arrival, target, when=None):
        index = len(self.started)

        def copy():
            return pltpu.make_async_remote_copy(
                src_ref=source,
                dst_ref=landing,
                send_sem=self.send_sem.at[index],
                recv_sem=arrival,
                device_id=target,
                device_id_type=MESH,
            )

        guarded(when, lambda: copy().start())
        self.started.append((when, copy))

    def arrive(self, landing, arrival, when=None):
        def wait():
            pltpu.make_async_remote_copy(
                src_ref=landing,
                dst_ref=landing,
                send_sem=self.send_sem.at[0],
                recv_sem=arrival,
                device_id=self.peer,
                device_id_type=MESH,
            ).wait_recv()

        guarded(when, wait)

    def finish(self):
        for when, copy in self.started:
            guarded(when, lambda: copy().wait_send())


def guarded(when, action):
    if when is None:
        action()
    else:
        pl.when(when)(action)


def both(first, second):
    return second if first is None else jnp.logical_and(first, second)


def rotate(field, cosine, sine):
    return field * cosine + pltpu.roll(field, HEAD_SIZE // 2, 1) * sine


def column_kernel(
    depth,
    hidden, order, gain, wq, bias_q, wkv, bias_kv, w_out, post_gain,
    attn_out, normed,
    rows, full, gains, weights, outw, kvs, queries, att, acc, part, terms, others, squares,
    kv_pieces, cos_t, sin_t, key_pos, bias_b, bias_p,
    local_sem, send_sem, rows_sem, gain_sem, w_sem, out_sem, kv_sem, att_sem, term_sem, other_sem, square_sem,
):
    s, t = lax.axis_index("seq"), lax.axis_index("tp")
    z, x, c = s // PLANE, s % PLANE // CORES, s % CORES
    span, half_width = hidden.shape
    slab = wq.shape[0]
    column = x * CORES + c
    sibling, across, other = (at(z, x, 1 - c), t), (at(z, 1 - x, c), t), (s, 1 - t)
    above, below = (at(jnp.minimum(z + 1, depth - 1), x, c), t), (at(jnp.maximum(z - 1, 0), x, c), t)

    barrier = pltpu.get_barrier_semaphore()
    peers = [sibling, across, other] + [(at(lax.rem(z + d, depth), x, c), t) for d in range(1, depth)]
    for peer in peers:
        pl.semaphore_signal(barrier, inc=1, device_id=peer, device_id_type=MESH)
    pl.semaphore_wait(barrier, len(peers))

    go = Traffic(send_sem, sibling)
    edge = span // PIECES

    def bit(p):
        return pl.ds(p * edge, edge)

    for p in range(PIECES):
        for target, when in ((other, None), (above, z < depth - 1), (below, z > 0)):
            go.send(hidden.at[bit(p)], rows.at[z, t, bit(p)], rows_sem.at[z, t, p], target, when)
    go.send(gain, gains.at[t], gain_sem.at[0], other)
    own = [
        pltpu.make_async_copy(hidden, rows.at[z, t], local_sem.at[0]),
        pltpu.make_async_copy(gain, gains.at[t], local_sem.at[1]),
        pltpu.make_async_copy(bias_q.at[:, pl.ds(pl.multiple_of(z * 2 * PAIR, PAIR), 2 * PAIR)], bias_b, local_sem.at[2]),
        pltpu.make_async_copy(bias_kv.at[:, pl.ds(pl.multiple_of(z * HEAD_SIZE, HEAD_SIZE), HEAD_SIZE)], bias_p, local_sem.at[3]),
        pltpu.make_async_copy(w_out, outw.at[column], local_sem.at[4]),
    ]

    def q_piece(g, zt):
        return wq.at[:, pl.ds(pl.multiple_of(zt * 2 * PAIR + (g - 1) * PAIR, PAIR), PAIR)]

    for g in (1, 2):
        own.append(pltpu.make_async_copy(q_piece(g, z), weights.at[g, s], local_sem.at[4 + g]))
    for copy in own:
        copy.start()
    for zt in range(depth):
        for i in range(2):
            kv_pieces[zt, :, i * HEAD_SIZE : (i + 1) * HEAD_SIZE] = wkv[:, i, zt * HEAD_SIZE : (zt + 1) * HEAD_SIZE]
    weights[0, s] = kv_pieces[z]
    for g in (0, 1, 2):
        source = kv_pieces.at[z] if g == 0 else q_piece(g, z)
        for target in (across, sibling):
            go.send(source, weights.at[g, s], w_sem.at[g, s], target)
    for target in (across, sibling):
        go.send(w_out, outw.at[column], out_sem.at[column], target)

    def spread(g, distance):
        for sign in (1, -1):
            zt = z + sign * distance
            when = jnp.logical_and(zt >= 0, zt < depth)
            zt = jnp.clip(zt, 0, depth - 1)
            source = kv_pieces.at[zt] if g == 0 else q_piece(g, zt)
            go.send(source, weights.at[g, s], w_sem.at[g, s], (at(zt, x, c), t), when)

    def chain(distance, action):
        for sign in (1, -1):
            zs = z - sign * distance
            when = jnp.logical_and(zs >= 0, zs < depth)
            zs = jnp.clip(zs, 0, depth - 1)
            target, more = (above, z < depth - 1) if sign == 1 else (below, z > 0)
            action(zs, when, target, jnp.logical_and(when, more))

    def pass_rows(distance):
        for p in range(PIECES):

            def action(zs, when, target, more):
                block, sem = rows.at[zs, t, bit(p)], rows_sem.at[zs, t, p]
                go.arrive(block, sem, when)
                go.send(block, block, sem, target, more)
                go.send(block, block, sem, other, when)

            chain(distance, action)

    def take_weights(g, distance):
        def action(zs, when, target, more):
            owner = at(zs, x, c)
            block, sem = weights.at[g, owner], w_sem.at[g, owner]
            go.arrive(block, sem, when)
            go.send(block, block, sem, across, when)
            go.send(block, block, sem, sibling, when)

        chain(distance, action)

    def weights_across(g):
        for zs in range(depth):
            owner = at(zs, 1 - x, c)
            block, sem = weights.at[g, owner], w_sem.at[g, owner]
            go.arrive(block, sem)
            go.send(block, block, sem, sibling)

    def weights_beside(g):
        for zs in range(depth):
            for xs in range(CORES):
                owner = at(zs, xs, 1 - c)
                go.arrive(weights.at[g, owner], w_sem.at[g, owner])

    def normalize(zs):
        for p in range(PIECES):
            go.arrive(rows.at[zs, 1 - t, bit(p)], rows_sem.at[zs, 1 - t, p])

        def strip(i, carry):
            r = pl.ds(pl.multiple_of(i * 16, 16), 16)
            halves = [rows[zs, h, r, :].astype(jnp.float32) for h in range(2)]
            total = sum(jnp.sum(a * a, axis=1, keepdims=True) for a in halves)
            factor = lax.rsqrt(total / (2 * half_width) + eps)
            for h in range(2):
                full[zs, r, h * half_width : (h + 1) * half_width] = (
                    halves[h] * factor * gains[h].astype(jnp.float32)
                ).astype(jnp.bfloat16)
            return carry

        lax.fori_loop(0, span // 16, strip, 0)

    lane = lax.broadcasted_iota(jnp.int32, (span, HEAD_SIZE), 1)
    line = lax.broadcasted_iota(jnp.int32, (span, HEAD_SIZE), 0)
    half = HEAD_SIZE // 2
    pair_id = jnp.where(lane < half, lane, lane - half).astype(jnp.float32)
    inverse = jnp.exp(-math.log(rope_base) * pair_id / half)

    def table(zs, carry):
        angles = (order[zs * PLANE + column] * span + line).astype(jnp.float32) * inverse
        cos_t[zs] = jnp.cos(angles)
        sine = jnp.sin(angles)
        sin_t[zs] = jnp.where(lane < half, -sine, sine)
        return carry

    lax.fori_loop(0, depth, table, 0)
    for m in range(PLANE):
        for zs in range(depth):
            i = m * depth + zs
            key_pos[:, i * span : (i + 1) * span] = order[zs * PLANE + m] * span + lax.broadcasted_iota(
                jnp.int32, (1, span), 1
            )
    for copy in own:
        copy.wait()
    go.arrive(gains.at[1 - t], gain_sem.at[0])

    pass_rows(1)
    spread(0, 1)
    spread(1, 1)
    normalize(z)
    pass_rows(2)
    for g in (0, 1):
        for distance in range(2, depth):
            spread(g, distance)
    for distance in range(1, depth):
        spread(2, distance)
    outw_across, outw_side = (1 - x) * CORES + c, 1 - c
    normalize(z + 1 - 2 * lax.rem(z, 2))
    take_weights(0, 1)
    pass_rows(3)
    take_weights(1, 1)
    for distance in range(2, depth):
        take_weights(0, distance)
    normalize(lax.rem(z + 2, depth))
    normalize(depth - 1 - z)
    go.arrive(outw.at[outw_across], out_sem.at[outw_across])
    go.send(outw.at[outw_across], outw.at[outw_across], out_sem.at[outw_across], sibling)
    weights_across(0)
    weights_beside(0)

    tokens = depth * span

    def product(g):
        return jnp.dot(
            full[...].reshape(tokens, 2 * half_width),
            weights[g].reshape(2 * half_width, PAIR),
            preferred_element_type=jnp.float32,
        )

    cosine, sine = cos_t[...].reshape(tokens, HEAD_SIZE), sin_t[...].reshape(tokens, HEAD_SIZE)
    pair = product(0)
    keys = pair[:, :HEAD_SIZE] + bias_p[0:1, :].astype(jnp.float32)
    kvs[column, :, :HEAD_SIZE] = rotate(keys, cosine, sine).astype(jnp.bfloat16)
    kvs[column, :, HEAD_SIZE:] = (pair[:, HEAD_SIZE:] + bias_p[1:2, :].astype(jnp.float32)).astype(jnp.bfloat16)
    for distance in range(2, depth):
        take_weights(1, distance)
    for target in (across, sibling):
        go.send(kvs.at[column], kvs.at[column], kv_sem.at[column], target)

    scale = math.log2(math.e) / math.sqrt(HEAD_SIZE)

    def make_queries(g):
        field = product(g)
        for i in range(2):
            cut = slice(i * HEAD_SIZE, (i + 1) * HEAD_SIZE)
            wide = slice((g - 1) * PAIR + i * HEAD_SIZE, (g - 1) * PAIR + (i + 1) * HEAD_SIZE)
            head = field[:, cut] + bias_b[:, wide].astype(jnp.float32)
            turned = (rotate(head, cosine, sine) * scale).astype(jnp.bfloat16)
            queries[g - 1, :, i * span : (i + 1) * span, :] = turned.reshape(depth, span, HEAD_SIZE)

    weights_across(1)
    weights_beside(1)
    make_queries(1)
    kv_across = (1 - x) * CORES + c
    go.arrive(kvs.at[kv_across], kv_sem.at[kv_across])
    go.send(kvs.at[kv_across], kvs.at[kv_across], kv_sem.at[kv_across], sibling)
    for distance in range(1, depth):
        take_weights(2, distance)
    for xs in range(CORES):
        owner = xs * CORES + 1 - c
        go.arrive(kvs.at[owner], kv_sem.at[owner])

    att_sends = 2 * 2 * depth

    def att_copy(g, b, side):
        target = above if side == 0 else below
        block = att.at[g, z, pl.ds(pl.multiple_of(b * span, span), span)]
        return pltpu.make_async_remote_copy(
            src_ref=block,
            dst_ref=block,
            send_sem=send_sem.at[send_sem.shape[0] - att_sends + (g * depth + b) * 2 + side],
            recv_sem=att_sem.at[g, z, b],
            device_id=target,
            device_id_type=MESH,
        )

    sides = ((0, z < depth - 1), (1, z > 0))

    def attend(g):
        def block(b, carry):
            scores = lax.dot_general(
                queries[g, b],
                kvs[:, :, :HEAD_SIZE].reshape(PLANE * tokens, HEAD_SIZE),
                (((1,), (1,)), ((), ())),
                preferred_element_type=jnp.float32,
            )
            first = order[b * PLANE + column] * span
            query_pos = first + lax.rem(lax.broadcasted_iota(jnp.int32, (2 * span, 1), 0), span)
            scores = jnp.where(key_pos[...] <= query_pos, scores, -jnp.inf)
            peak = jnp.max(scores, axis=1, keepdims=True)
            shares = jnp.exp2(scores - peak)
            totals = jnp.sum(shares, axis=1, keepdims=True)
            summed = jnp.dot(
                shares.astype(jnp.bfloat16),
                kvs[:, :, HEAD_SIZE:].reshape(PLANE * tokens, HEAD_SIZE),
                preferred_element_type=jnp.float32,
            )
            result = (summed / totals).astype(jnp.bfloat16)
            place = pl.ds(pl.multiple_of(b * span, span), span)
            att[g, z, place, :HEAD_SIZE] = result[:span]
            att[g, z, place, HEAD_SIZE:] = result[span:]
            for side, when in sides:
                pl.when(when)(lambda: att_copy(g, b, side).start())
            return carry

        lax.fori_loop(0, depth, block, 0)

    def pass_heads(g, distance):
        for b in range(depth):

            def action(zs, when, target, more):
                block, sem = att.at[g, zs, pl.ds(b * span, span)], att_sem.at[g, zs, b]
                go.arrive(block, sem, when)
                go.send(block, block, sem, target, more)

            chain(distance, action)

    attend(0)
    weights_across(2)
    pass_heads(0, 1)
    weights_beside(2)
    make_queries(2)
    attend(1)
    pass_heads(0, 2)
    pass_heads(1, 1)
    pass_heads(0, 3)
    for m in (outw_side, CORES + outw_side):
        go.arrive(outw.at[m], out_sem.at[m])

    def contribution(g, place, m):
        total = None
        for zs in range(depth):
            term = jnp.dot(
                att[g, zs, place, :],
                outw[m, zs * 2 * PAIR + g * PAIR : zs * 2 * PAIR + (g + 1) * PAIR, :],
                preferred_element_type=jnp.float32,
            )
            total = term if total is None else total + term
        return total

    width = w_out.shape[1]
    for m in range(PLANE):
        acc[:, m * width : (m + 1) * width] = contribution(0, slice(None), m)
    pass_heads(1, 2)
    pass_heads(1, 3)
    for d in (1, 2, 3, 0):
        zt = lax.rem(z + d, depth)
        place = pl.ds(pl.multiple_of(zt * span, span), span)
        for m in range(PLANE):
            cut = slice(m * width, (m + 1) * width)
            value = (acc[place, cut] + contribution(1, place, m)).astype(jnp.bfloat16)
            if d:
                part[zt, :, cut] = value
            else:
                terms[z, :, cut] = value
        if d:
            go.send(part.at[zt], terms.at[z], term_sem.at[z], (at(zt, x, c), t))

    share = depth // 2

    def cross(zs):
        goal = zs // share
        go.send(terms.at[zs], others.at[lax.rem(zs, share)], other_sem.at[lax.rem(zs, share)], other, goal != t)

    cross(z)
    for d in range(1, depth):
        zs = lax.rem(z - d + depth, depth)
        go.arrive(terms.at[zs], term_sem.at[zs])
        cross(zs)
    sums = jnp.zeros((span, 1), jnp.float32)
    wide = PLANE * width
    for j in range(share):
        go.arrive(others.at[j], other_sem.at[j])
        cut = slice(j * wide, (j + 1) * wide)
        mixed = terms[t * share + j].astype(jnp.float32) + others[j].astype(jnp.float32)
        attn_out[:, cut] = mixed.astype(jnp.bfloat16)
        stream = rows[z, t, :, cut].astype(jnp.float32) + mixed
        acc[pl.ds(j * span, span), :] = stream
        sums = sums + jnp.sum(stream * stream, axis=1, keepdims=True)
    squares[t] = jnp.broadcast_to(sums, (span, HEAD_SIZE))
    go.send(squares.at[t], squares.at[t], square_sem.at[0], other)
    go.arrive(squares.at[1 - t], square_sem.at[0])
    total = squares[0] + squares[1]
    factor = lax.rsqrt(total / (2 * half_width) + eps)[:, :1]
    for j in range(share):
        cut = slice(j * wide, (j + 1) * wide)
        normed[:, cut] = (
            acc[pl.ds(j * span, span), :] * factor * post_gain[:, cut].astype(jnp.float32)
        ).astype(jnp.bfloat16)
    assert len(go.started) + att_sends <= send_sem.shape[0]
    go.finish()
    for g in range(2):
        for b in range(depth):
            for side, when in sides:
                pl.when(when)(lambda: att_copy(g, b, side).wait_send())


def per_device_by_column(
    hidden_in,
    span_order,
    norm_gain,
    w_query,
    bias_query,
    key_value_weight,
    bias_kv,
    w_out,
    post_gain,
):
    span, half_width = hidden_in.shape
    n_seq = span_order.shape[0]
    depth = n_seq // PLANE
    slab = w_query.shape[0]
    tokens = depth * span
    vmem, hbm, smem = (pl.BlockSpec(memory_space=m) for m in (pltpu.VMEM, pl.ANY, pltpu.SMEM))
    dma = pltpu.SemaphoreType.DMA
    out = jax.ShapeDtypeStruct((span, half_width), jnp.bfloat16)
    bf16 = lambda *shape: pltpu.VMEM(shape, jnp.bfloat16)
    f32 = lambda *shape: pltpu.VMEM(shape, jnp.float32)
    width = w_out.shape[1]
    return pl.pallas_call(
        lambda *refs: column_kernel(depth, *refs),
        out_shape=(out, out),
        in_specs=[hbm, smem, vmem, hbm, hbm, vmem, hbm, hbm, vmem],
        out_specs=(vmem, vmem),
        scratch_shapes=[
            bf16(depth, 2, span, half_width),
            bf16(depth, span, 2 * half_width),
            bf16(2, 1, half_width),
            bf16(3, n_seq, slab, PAIR),
            bf16(PLANE, w_out.shape[0], width),
            bf16(PLANE, tokens, PAIR),
            bf16(2, depth, 2 * span, HEAD_SIZE),
            bf16(2, depth, tokens, PAIR),
            f32(tokens, PLANE * width),
            bf16(depth, span, PLANE * width),
            bf16(depth, span, PLANE * width),
            bf16(depth // 2, span, PLANE * width),
            f32(2, span, HEAD_SIZE),
            bf16(depth, slab, PAIR),
            f32(depth, span, HEAD_SIZE),
            f32(depth, span, HEAD_SIZE),
            pltpu.VMEM((1, PLANE * tokens), jnp.int32),
            bf16(1, 2 * PAIR),
            bf16(2, HEAD_SIZE),
            dma((8,)),
            dma((224,)),
            dma((depth, 2, PIECES)),
            dma((1,)),
            dma((3, n_seq)),
            dma((PLANE,)),
            dma((PLANE,)),
            dma((2, depth, depth)),
            dma((depth,)),
            dma((depth // 2,)),
            dma((1,)),
        ],
        compiler_params=pltpu.CompilerParams(
            collective_id=0, has_side_effects=True, vmem_limit_bytes=60 * 1024 * 1024
        ),
        name="sublayer",
    )(
        hidden_in,
        span_order,
        norm_gain[None, :],
        w_query,
        bias_query[None, :],
        key_value_weight,
        bias_kv,
        w_out,
        post_gain[None, :],
    )


def per_device(*args):
    hidden_in, span_order, w_query, kv_weight = args[0], args[1], args[3], args[5]
    n_seq = span_order.shape[0]
    n_tp = MODEL_WIDTH // hidden_in.shape[1]
    heads = w_query.shape[1] // HEAD_SIZE
    kv_heads = kv_weight.shape[2] // HEAD_SIZE
    if n_tp == 2 and n_seq == 4 * PLANE and kv_heads == 4 and heads == kv_heads * GROUP:
        return per_device_by_column(*args)
    return per_device_by_span(*args)


def solution(mesh):
    placed = (
        P("seq", "tp"),
        P(),
        P("tp"),
        P("seq", "tp"),
        P("tp"),
        P("seq", None, "tp"),
        P(None, "tp"),
        P("tp", "seq"),
        P("tp"),
    )
    return jax.shard_map(
        per_device,
        mesh=mesh,
        in_specs=placed,
        out_specs=(P("seq", "tp"), P("seq", "tp")),
        check_vma=False,
    )
```

```python
import math

import jax
import jax.numpy as jnp
from jax import lax
from jax.experimental import pallas as pl
from jax.experimental.pallas import tpu as pltpu
from jax.sharding import PartitionSpec as P

MODEL_WIDTH = 4096
HEAD_SIZE = 128
GROUP = 4


eps = 1e-06
rope_base = 1000000.0


def apply_rotary(field, token_positions):
    half = field.shape[-1] // 2
    inverse = jnp.exp(-math.log(rope_base) * jnp.arange(half, dtype=jnp.float32) / half)
    angles = token_positions.astype(jnp.float32)[:, None] * inverse[None, :]
    cosine = jnp.cos(angles)[:, None, :]
    sine = jnp.sin(angles)[:, None, :]
    first = field[..., :half]
    second = field[..., half:]
    return jnp.concatenate(
        [first * cosine - second * sine, second * cosine + first * sine], axis=-1
    )


def span_lookup(order, devices):
    table_ids = jnp.arange(order.shape[0], dtype=jnp.int32)
    return jnp.sum(jnp.where(devices[:, None] == table_ids[None, :], order[None, :], 0), axis=1)


def per_device_by_span(
    hidden_in,
    span_order,
    norm_gain,
    w_query,
    bias_query,
    key_value_weight,
    bias_kv,
    w_out,
    post_gain,
):
    tok_rows = hidden_in.shape[0]
    seq_index = lax.axis_index("seq")
    own_span = span_lookup(span_order, jnp.full((1,), seq_index, jnp.int32))[0]
    token_positions = own_span * tok_rows + jnp.arange(tok_rows, dtype=jnp.int32)
    local = hidden_in.astype(jnp.float32)
    raw_rows, gains = (
        lax.all_gather(hidden_in, "tp", axis=1, tiled=True),
        lax.all_gather(norm_gain[None, :], "tp", axis=1, tiled=True),
    )
    full_rows = raw_rows.astype(jnp.float32)
    meansq = jnp.mean(full_rows * full_rows, axis=1, keepdims=True)
    normed_in = (full_rows * lax.rsqrt(meansq + eps) * gains.astype(jnp.float32)).astype(
        jnp.bfloat16
    )
    columns = normed_in
    query_proj = jnp.dot(
        columns,
        lax.all_gather(w_query, "seq", axis=0, tiled=True),
        preferred_element_type=jnp.float32,
    )
    columns = normed_in
    pair_proj = jnp.einsum(
        "tr,rkc->tkc",
        columns,
        lax.all_gather(key_value_weight, "seq", axis=0, tiled=True),
        preferred_element_type=jnp.float32,
    )
    query_heads = w_query.shape[1] // HEAD_SIZE
    kv_heads = key_value_weight.shape[2] // HEAD_SIZE
    query_proj = query_proj + bias_query.astype(jnp.float32)[None, :]
    queries = apply_rotary(
        query_proj.reshape(tok_rows, query_heads, HEAD_SIZE), token_positions
    ).astype(jnp.bfloat16)
    pair_proj = pair_proj + bias_kv.astype(jnp.float32)[None, :, :]
    rotated_keys = apply_rotary(
        pair_proj[:, 0, :].reshape(tok_rows, kv_heads, HEAD_SIZE), token_positions
    )
    rotated_keys = rotated_keys.astype(jnp.bfloat16).reshape(tok_rows, kv_heads * HEAD_SIZE)
    value_rows = pair_proj[:, 1, :].astype(jnp.bfloat16)
    grouped = (
        queries.reshape(tok_rows, kv_heads, GROUP, HEAD_SIZE)
        .transpose(1, 2, 0, 3)
        .reshape(kv_heads, GROUP * tok_rows, HEAD_SIZE)
    )
    query_pos = jnp.tile(token_positions, GROUP)
    last_query = jnp.max(token_positions)
    scale = 1.0 / math.sqrt(HEAD_SIZE)
    start_state = (
        jnp.full((kv_heads, GROUP * tok_rows), -1e30, jnp.float32),
        jnp.zeros((kv_heads, GROUP * tok_rows), jnp.float32),
        jnp.zeros((kv_heads, GROUP * tok_rows, HEAD_SIZE), jnp.float32),
    )
    key_piece = lax.all_gather(rotated_keys, "seq", axis=0, tiled=True)
    value_piece = lax.all_gather(value_rows, "seq", axis=0, tiled=True)
    count = key_piece.shape[0]
    block = math.gcd(count, 1536)

    def visit(step, state):
        first = step * block
        key_block = lax.dynamic_slice_in_dim(key_piece, first, block, 0).reshape(
            block, kv_heads, HEAD_SIZE
        )
        value_block = lax.dynamic_slice_in_dim(value_piece, first, block, 0).reshape(
            block, kv_heads, HEAD_SIZE
        )
        row_ids = first + jnp.arange(block, dtype=jnp.int32)
        key_pos = span_lookup(span_order, row_ids // tok_rows) * tok_rows + row_ids % tok_rows

        def update(current):
            maxima, totals, sums = current
            scores = (
                jnp.einsum("kqd,nkd->kqn", grouped, key_block, preferred_element_type=jnp.float32)
                * scale
            )
            allowed = (key_pos[None, :] <= query_pos[:, None])[None, :, :]
            scores = jnp.where(allowed, scores, -1e30)
            fresh = jnp.maximum(maxima, jnp.max(scores, axis=2))
            weights = jnp.where(allowed, jnp.exp(scores - fresh[:, :, None]), 0.0)
            factor = jnp.exp(maxima - fresh)
            totals = totals * factor + jnp.sum(weights, axis=2)
            sums = sums * factor[:, :, None] + jnp.einsum(
                "kqn,nkd->kqd",
                weights.astype(jnp.bfloat16),
                value_block,
                preferred_element_type=jnp.float32,
            )
            return (fresh, totals, sums)

        return lax.cond(jnp.min(key_pos) <= last_query, update, lambda current: current, state)

    maxima, totals, sums = lax.fori_loop(0, count // block, visit, start_state)
    attended = (sums / totals[:, :, None]).astype(jnp.bfloat16)
    attended = (
        attended.reshape(kv_heads, GROUP, tok_rows, HEAD_SIZE)
        .transpose(2, 0, 1, 3)
        .reshape(tok_rows, query_heads * HEAD_SIZE)
    )
    partial_out = jnp.dot(
        attended,
        lax.all_gather(w_out, "seq", axis=1, tiled=True),
        preferred_element_type=jnp.float32,
    )
    mixed = lax.psum_scatter(
        partial_out.astype(jnp.bfloat16), "tp", scatter_dimension=1, tiled=True
    ).astype(jnp.float32)
    attn_out = mixed.astype(jnp.bfloat16)
    stream = local + mixed
    post_sq = lax.psum(jnp.sum(stream * stream, axis=1), "tp")
    normed = (
        stream
        * lax.rsqrt(post_sq / MODEL_WIDTH + eps)[:, None]
        * post_gain.astype(jnp.float32)[None, :]
    ).astype(jnp.bfloat16)
    return (attn_out, normed)


MESH = pl.DeviceIdType.MESH
CORES = 2
PLANE = 4
PIECES = 2
PAIR = 2 * HEAD_SIZE


def at(z, x, c):
    return z * PLANE + x * CORES + c


class Traffic:
    def __init__(self, depth, z, sem, proxy, peer):
        self.z, self.sem, self.proxy, self.peer = z, sem, proxy, peer
        self.rows = [0] * depth

    def remote(self, source, landing, arrival, target, sem=None):
        return pltpu.make_async_remote_copy(
            src_ref=source,
            dst_ref=landing,
            send_sem=self.sem.at[0] if sem is None else sem,
            recv_sem=arrival,
            device_id=target,
            device_id_type=MESH,
        )

    def count(self, ref, where=None, times=1):
        size = math.prod(ref.shape) * times // self.proxy.shape[1]
        for k in range(len(self.rows)):
            if where is None or where(k):
                self.rows[k] += size

    def send(self, source, landing, arrival, target, where=None, also=None, sem=None):
        when = None if where is None else where(self.z)
        if also is not None:
            when = also if when is None else jnp.logical_and(when, also)
        guarded(when, lambda: self.remote(source, landing, arrival, target, sem).start())
        if sem is None and also is None:
            self.count(source, where)

    def arrive(self, landing, arrival, when=None):
        guarded(when, lambda: self.remote(landing, landing, arrival, self.peer).wait_recv())

    def left(self, source, sem, when=None):
        guarded(when, lambda: self.remote(source, source, sem, self.peer, sem).wait_send())

    def finish(self):
        for k, size in enumerate(self.rows):
            block = self.proxy.at[pl.ds(0, size)]
            self.left(block, self.sem.at[0], self.z == k)


def guarded(when, action):
    if when is None:
        action()
    else:
        pl.when(when)(action)


def rotate(field, cosine, sine):
    return field * cosine + pltpu.roll(field, HEAD_SIZE // 2, 1) * sine


def column_kernel(
    depth,
    hidden, order, vectors, wq, wkv, bias_kv, w_out,
    attn_out, normed,
    rows, full, gains, weights, outw, kvs, queries, att, acc, part, terms, others, squares,
    kv_pieces, cos_t, sin_t, key_pos, bias_b, bias_p, post_gain, proxy,
    local_sem, send_sem, small_sem, relay_sem, rows_sem, rows_side_sem,
    w_sem, w_across_sem, w_side_sem, out_sem, kv_sem, att_sem, term_sem, other_sem,
):
    s, t = lax.axis_index("seq"), lax.axis_index("tp")
    z, x, c = s // PLANE, s % PLANE // CORES, s % CORES
    last = depth - 1
    span, half_width = hidden.shape
    column = x * CORES + c
    sibling, across, other = (at(z, x, 1 - c), t), (at(z, 1 - x, c), t), (s, 1 - t)
    above, below = (at(jnp.minimum(z + 1, last), x, c), t), (at(jnp.maximum(z - 1, 0), x, c), t)

    barrier = pltpu.get_barrier_semaphore()
    peers = [sibling, across, other] + [(at(lax.rem(z + d, depth), x, c), t) for d in range(1, depth)]
    for peer in peers:
        pl.semaphore_signal(barrier, inc=1, device_id=peer, device_id_type=MESH)
    pl.semaphore_wait(barrier, len(peers))

    go = Traffic(depth, z, send_sem, proxy, sibling)
    gain, bias_q = vectors.at[0], vectors.at[1]
    edge = span // PIECES

    def bit(p):
        return pl.ds(p * edge, edge)

    go.send(gain, gains.at[t], small_sem.at[0], other, sem=small_sem.at[1])
    for p in range(PIECES):
        mine, landing = hidden.at[bit(p)], rows.at[z, t, bit(p)]
        go.send(mine, landing, rows_side_sem.at[z], other)
        go.send(mine, landing, rows_sem.at[z, p], above, lambda k: k < last)
        go.send(mine, landing, rows_sem.at[z, p], below, lambda k: k > 0)
    own = [
        pltpu.make_async_copy(hidden, rows.at[z, t], local_sem.at[0]),
        pltpu.make_async_copy(gain, gains.at[t], local_sem.at[1]),
        pltpu.make_async_copy(
            bias_q.at[:, pl.ds(pl.multiple_of(z * 2 * PAIR, PAIR), 2 * PAIR)], bias_b, local_sem.at[2]
        ),
        pltpu.make_async_copy(
            bias_kv.at[:, pl.ds(pl.multiple_of(z * HEAD_SIZE, HEAD_SIZE), HEAD_SIZE)], bias_p, local_sem.at[3]
        ),
        pltpu.make_async_copy(w_out, outw.at[column], local_sem.at[4]),
        pltpu.make_async_copy(vectors.at[2], post_gain, local_sem.at[7]),
    ]

    def q_piece(g, zt):
        return wq.at[:, pl.ds(pl.multiple_of(zt * 2 * PAIR + (g - 1) * PAIR, PAIR), PAIR)]

    for g in (1, 2):
        own.append(pltpu.make_async_copy(q_piece(g, z), weights.at[g, s], local_sem.at[4 + g]))
    for copy in own:
        copy.start()
    for zt in range(depth):
        for i in range(2):
            kv_pieces[zt, :, i * HEAD_SIZE : (i + 1) * HEAD_SIZE] = wkv[:, i, zt * HEAD_SIZE : (zt + 1) * HEAD_SIZE]
    weights[0, s] = kv_pieces[z]
    for g in (0, 1, 2):
        source = kv_pieces.at[z] if g == 0 else q_piece(g, z)
        go.send(source, weights.at[g, s], w_across_sem.at[g], across)
        go.send(source, weights.at[g, s], w_side_sem.at[g], sibling)
    go.send(w_out, outw.at[column], out_sem.at[0], across)
    go.send(w_out, outw.at[column], out_sem.at[1], sibling)

    def spread(stage, groups):
        for g in groups:
            for zt, where in ((stage, lambda k: k < stage), (last - stage, lambda k: k > last - stage)):
                source = kv_pieces.at[zt] if g == 0 else q_piece(g, zt)
                go.send(source, weights.at[g, s], w_sem.at[g, z], (at(zt, x, c), t), where)

    def take_weights(g, stage, distances=None):
        for distance in distances or range(1, stage + 1):
            for sign, goal in ((-1, stage), (1, last - stage)):
                zs = jnp.clip(z + sign * distance, 0, last)
                block = weights.at[g, at(zs, x, c)]
                go.arrive(block, w_sem.at[g, zs], z == goal)
                go.send(block, block, w_across_sem.at[g], across, lambda k: k == goal)
                go.send(block, block, w_side_sem.at[g], sibling, lambda k: k == goal)

    def chain(distance, action):
        for sign in (1, -1):
            zs = jnp.clip(z - sign * distance, 0, last)
            where = lambda k: (k >= distance) if sign == 1 else (k + distance <= last)
            target = above if sign == 1 else below
            more = (lambda k: distance <= k < last) if sign == 1 else (lambda k: 0 < k <= last - distance)
            if distance < last:
                now = jnp.logical_and(z >= distance, z < last) if sign == 1 else jnp.logical_and(z > 0, z <= last - distance)
                action(zs, where, target, (more, now))
            else:
                action(zs, where, target, None)

    def relay(block, arrival, target, more, sem=None):
        if more is not None:
            where, now = more
            pl.when(now)(lambda: go.remote(block, block, arrival, target, sem).start())
            if sem is None:
                go.count(block, where)

    def pass_rows(distance):
        for p in range(PIECES):

            def action(zs, where, target, more):
                block = rows.at[zs, t, bit(p)]
                go.arrive(block, rows_sem.at[zs, p], where(z))
                relay(block, rows_sem.at[zs, p], target, more, relay_sem.at[0] if distance == last - 1 else None)
                go.send(block, block, rows_side_sem.at[zs], other, where)

            chain(distance, action)

    def weights_across(g):
        go.arrive(weights.at[g, pl.ds(0, depth)], w_across_sem.at[g])
        for zs in range(depth):
            block = weights.at[g, at(zs, 1 - x, c)]
            go.send(block, block, w_side_sem.at[g], sibling)

    def weights_beside(g):
        go.arrive(weights.at[g, pl.ds(0, depth * CORES)], w_side_sem.at[g])

    def normalize(zs):
        go.arrive(rows.at[zs, 1 - t], rows_side_sem.at[zs])

        def strip(i, carry):
            r = pl.ds(pl.multiple_of(i * 16, 16), 16)
            halves = [rows[zs, h, r, :].astype(jnp.float32) for h in range(2)]
            total = sum(jnp.sum(a * a, axis=1, keepdims=True) for a in halves)
            factor = lax.rsqrt(total / (2 * half_width) + eps)
            for h in range(2):
                full[zs, r, h * half_width : (h + 1) * half_width] = (
                    halves[h] * factor * gains[h].astype(jnp.float32)
                ).astype(jnp.bfloat16)
            return carry

        lax.fori_loop(0, span // 16, strip, 0)

    lane = lax.broadcasted_iota(jnp.int32, (span, HEAD_SIZE), 1)
    line = lax.broadcasted_iota(jnp.int32, (span, HEAD_SIZE), 0)
    half = HEAD_SIZE // 2
    pair_id = jnp.where(lane < half, lane, lane - half).astype(jnp.float32)
    inverse = jnp.exp(-math.log(rope_base) * pair_id / half)

    def table(zs, carry):
        angles = (order[zs * PLANE + column] * span + line).astype(jnp.float32) * inverse
        cos_t[zs] = jnp.cos(angles)
        sine = jnp.sin(angles)
        sin_t[zs] = jnp.where(lane < half, -sine, sine)
        return carry

    lax.fori_loop(0, depth, table, 0)
    for m in range(PLANE):
        for zs in range(depth):
            i = m * depth + zs
            key_pos[:, i * span : (i + 1) * span] = order[zs * PLANE + m] * span + lax.broadcasted_iota(
                jnp.int32, (1, span), 1
            )
    for copy in own:
        copy.wait()
    go.arrive(gains.at[1 - t], small_sem.at[0])

    middle = jnp.logical_and(z > 0, z < last)
    pass_rows(1)
    spread(1, (0, 1, 2))
    spread(3, (0,))
    normalize(z)
    pass_rows(2)
    spread(2, (0, 1, 2))
    for g in (0, 1, 2):
        take_weights(g, 1)
    normalize(z + 1 - 2 * lax.rem(z, 2))
    take_weights(0, 3)
    go.left(rows.at[z, t], relay_sem.at[0], middle)
    pass_rows(3)
    spread(3, (1, 2))
    for g in (0, 1, 2):
        take_weights(g, 2)
    normalize(lax.rem(z + 2, depth))
    take_weights(1, 3, (1, 2))
    normalize(last - z)
    weights_across(0)
    weights_beside(0)

    tokens = depth * span

    def product(g):
        return jnp.dot(
            full[...].reshape(tokens, 2 * half_width),
            weights[g].reshape(2 * half_width, PAIR),
            preferred_element_type=jnp.float32,
        )

    cosine, sine = cos_t[...].reshape(tokens, HEAD_SIZE), sin_t[...].reshape(tokens, HEAD_SIZE)
    pair = product(0)
    keys = pair[:, :HEAD_SIZE] + bias_p[0:1, :].astype(jnp.float32)
    kvs[column, :, :HEAD_SIZE] = rotate(keys, cosine, sine).astype(jnp.bfloat16)
    kvs[column, :, HEAD_SIZE:] = (pair[:, HEAD_SIZE:] + bias_p[1:2, :].astype(jnp.float32)).astype(jnp.bfloat16)
    go.send(kvs.at[column], kvs.at[column], kv_sem.at[0], across)
    go.send(kvs.at[column], kvs.at[column], kv_sem.at[1], sibling)
    take_weights(1, 3, (3,))
    take_weights(2, 3)

    scale = math.log2(math.e) / math.sqrt(HEAD_SIZE)

    def make_queries(g):
        field = product(g)
        for i in range(2):
            cut = slice(i * HEAD_SIZE, (i + 1) * HEAD_SIZE)
            wide = slice((g - 1) * PAIR + i * HEAD_SIZE, (g - 1) * PAIR + (i + 1) * HEAD_SIZE)
            head = field[:, cut] + bias_b[:, wide].astype(jnp.float32)
            turned = (rotate(head, cosine, sine) * scale).astype(jnp.bfloat16)
            queries[g - 1, :, i * span : (i + 1) * span, :] = turned.reshape(depth, span, HEAD_SIZE)

    weights_across(1)
    weights_beside(1)
    make_queries(1)
    kv_across = kvs.at[(1 - x) * CORES + c]
    go.arrive(kv_across, kv_sem.at[0])
    go.send(kv_across, kv_across, kv_sem.at[1], sibling)
    go.arrive(kvs.at[pl.ds(0, CORES)], kv_sem.at[1])

    def att_piece(g, zs, b):
        return att.at[g, zs, pl.ds(pl.multiple_of(b * span, span), span)]

    def nth(i):
        return jnp.where(i == 0, 0, jnp.where(i == 1, last, jnp.where(i == 2, 1 + c, 2 - c)))

    def attend(g):
        def turn(i, carry):
            b = nth(i)
            scores = lax.dot_general(
                queries[g, b],
                kvs[:, :, :HEAD_SIZE].reshape(PLANE * tokens, HEAD_SIZE),
                (((1,), (1,)), ((), ())),
                preferred_element_type=jnp.float32,
            )
            first = order[b * PLANE + column] * span
            query_pos = first + lax.rem(lax.broadcasted_iota(jnp.int32, (2 * span, 1), 0), span)
            scores = jnp.where(key_pos[...] <= query_pos, scores, -jnp.inf)
            peak = jnp.max(scores, axis=1, keepdims=True)
            shares = jnp.exp2(scores - peak)
            totals = jnp.sum(shares, axis=1, keepdims=True)
            summed = jnp.dot(
                shares.astype(jnp.bfloat16),
                kvs[:, :, HEAD_SIZE:].reshape(PLANE * tokens, HEAD_SIZE),
                preferred_element_type=jnp.float32,
            )
            result = (summed / totals).astype(jnp.bfloat16)
            place = pl.ds(pl.multiple_of(b * span, span), span)
            att[g, z, place, :HEAD_SIZE] = result[:span]
            att[g, z, place, HEAD_SIZE:] = result[span:]
            block = att_piece(g, z, b)
            pl.when(z < last)(lambda: go.remote(block, block, att_sem.at[g, z, b], above).start())
            pl.when(z > 0)(lambda: go.remote(block, block, att_sem.at[g, z, b], below).start())
            return carry

        lax.fori_loop(0, depth, turn, 0)
        go.count(att.at[g, 0], lambda k: k < last)
        go.count(att.at[g, 0], lambda k: k > 0)

    attend(0)
    weights_across(2)
    weights_beside(2)
    make_queries(2)
    attend(1)
    outw_across = outw.at[(1 - x) * CORES + c]
    go.arrive(outw_across, out_sem.at[0])
    go.send(outw_across, outw_across, out_sem.at[1], sibling)
    go.arrive(outw.at[pl.ds(0, CORES)], out_sem.at[1])

    def pass_heads(g, b, distance):
        def action(zs, where, target, more):
            block, sem = att_piece(g, zs, b), att_sem.at[g, zs, b]
            go.arrive(block, sem, where(z))
            relay(block, sem, target, more)

        chain(distance, action)

    halves = 2
    each = PLANE // halves

    def piece(ref, i, h):
        return ref.at[i, pl.ds(h * each, each)]

    def mix_block(b):
        place = pl.ds(pl.multiple_of(b * span, span), span)
        for h in range(halves):
            for m in range(h * each, (h + 1) * each):
                total = None
                for zs in range(depth):
                    for g in range(2):
                        first = zs * 2 * PAIR + g * PAIR
                        term = jnp.dot(
                            att[g, zs, place, :], outw[m, first : first + PAIR, :], preferred_element_type=jnp.float32
                        )
                        total = term if total is None else total + term
                value = total.astype(jnp.bfloat16)

                @pl.when(b == z)
                def _():
                    terms[z, m] = value

                @pl.when(b != z)
                def _():
                    part[b, m] = value

            @pl.when(b != z)
            def _():
                go.remote(piece(part, b, h), piece(terms, z, h), term_sem.at[z, h], (at(b, x, c), t)).start()

    share = depth // 2

    def settle():
        for zs in (1, 2, 0, 3):
            for h in range(halves):
                block = piece(terms, zs, h)
                go.arrive(block, term_sem.at[zs, h], z != zs)
                landing, sem = piece(others, zs % share, h), other_sem.at[zs % share, h]
                go.send(block, landing, sem, other, also=t != zs // share)

    for g in range(2):
        for i in range(depth):
            pass_heads(g, nth(i), 1)
    for i in range(depth):
        for g in range(2):
            pass_heads(g, nth(i), 2)
    for i in range(depth):
        for g in range(2):
            pass_heads(g, nth(i), 3)
        mix_block(nth(i))
    settle()
    go.count(part.at[0], times=depth - 1)
    go.count(others.at[0], times=share)

    width = w_out.shape[1]
    sums = jnp.zeros((span, 1), jnp.float32)
    pieces = [(j, m) for j in range(share) for m in range(PLANE)]
    for j, m in pieces:
        if m % each == 0:
            go.arrive(piece(others, j, m // each), other_sem.at[j, m // each])
        cut = slice((j * PLANE + m) * width, (j * PLANE + m + 1) * width)
        mixed = terms[t * share + j, m].astype(jnp.float32) + others[j, m].astype(jnp.float32)
        attn_out[:, cut] = mixed.astype(jnp.bfloat16)
        stream = rows[z, t, :, cut].astype(jnp.float32) + mixed
        acc[j, m] = stream
        sums = sums + jnp.sum(stream * stream, axis=1, keepdims=True)
    squares[t] = jnp.broadcast_to(sums, (span, span)).T[:8]
    go.send(squares.at[t], squares.at[t], small_sem.at[2], other, sem=small_sem.at[3])
    go.arrive(squares.at[1 - t], small_sem.at[2])
    total = jnp.broadcast_to((squares[0] + squares[1])[:1], (span, span)).T
    factor = lax.rsqrt(total / (2 * half_width) + eps)[:, :1]
    for j, m in pieces:
        cut = slice((j * PLANE + m) * width, (j * PLANE + m + 1) * width)
        normed[:, cut] = (acc[j, m] * factor * post_gain[:, cut].astype(jnp.float32)).astype(jnp.bfloat16)
    go.left(gain, small_sem.at[1])
    go.left(squares.at[t], small_sem.at[3])
    go.finish()


def per_device_by_column(
    hidden_in,
    span_order,
    norm_gain,
    w_query,
    bias_query,
    key_value_weight,
    bias_kv,
    w_out,
    post_gain,
):
    span, half_width = hidden_in.shape
    n_seq = span_order.shape[0]
    depth = n_seq // PLANE
    slab = w_query.shape[0]
    tokens = depth * span
    vmem, hbm, smem = (pl.BlockSpec(memory_space=m) for m in (pltpu.VMEM, pl.ANY, pltpu.SMEM))
    dma = pltpu.SemaphoreType.DMA
    out = jax.ShapeDtypeStruct((span, half_width), jnp.bfloat16)
    bf16 = lambda *shape: pltpu.VMEM(shape, jnp.bfloat16)
    f32 = lambda *shape: pltpu.VMEM(shape, jnp.float32)
    width = w_out.shape[1]
    return pl.pallas_call(
        lambda *refs: column_kernel(depth, *refs),
        out_shape=(out, out),
        in_specs=[hbm, smem, hbm, hbm, vmem, hbm, hbm],
        out_specs=(vmem, vmem),
        scratch_shapes=[
            bf16(depth, 2, span, half_width),
            bf16(depth, span, 2 * half_width),
            bf16(2, 1, half_width),
            bf16(3, n_seq, slab, PAIR),
            bf16(PLANE, w_out.shape[0], width),
            bf16(PLANE, tokens, PAIR),
            bf16(2, depth, 2 * span, HEAD_SIZE),
            bf16(2, depth, tokens, PAIR),
            f32(depth // 2, PLANE, span, width),
            bf16(depth, PLANE, span, width),
            bf16(depth, PLANE, span, width),
            bf16(depth // 2, PLANE, span, width),
            f32(2, 8, span),
            bf16(depth, slab, PAIR),
            f32(depth, span, HEAD_SIZE),
            f32(depth, span, HEAD_SIZE),
            pltpu.VMEM((1, PLANE * tokens), jnp.int32),
            bf16(1, 2 * PAIR),
            bf16(2, HEAD_SIZE),
            bf16(1, half_width),
            bf16(4608, half_width),
            dma((8,)),
            dma((1,)),
            dma((4,)),
            dma((1,)),
            dma((depth, PIECES)),
            dma((depth,)),
            dma((3, depth)),
            dma((3,)),
            dma((3,)),
            dma((2,)),
            dma((2,)),
            dma((2, depth, depth)),
            dma((depth, 2)),
            dma((depth // 2, 2)),
        ],
        compiler_params=pltpu.CompilerParams(
            collective_id=0, has_side_effects=True, vmem_limit_bytes=60 * 1024 * 1024
        ),
        name="sublayer",
    )(
        hidden_in,
        span_order,
        jnp.stack([norm_gain, bias_query, post_gain])[:, None, :],
        w_query,
        key_value_weight,
        bias_kv,
        w_out,
    )


def per_device(*args):
    hidden_in, span_order, w_query, kv_weight = args[0], args[1], args[3], args[5]
    n_seq = span_order.shape[0]
    n_tp = MODEL_WIDTH // hidden_in.shape[1]
    heads = w_query.shape[1] // HEAD_SIZE
    kv_heads = kv_weight.shape[2] // HEAD_SIZE
    if n_tp == 2 and n_seq == 4 * PLANE and kv_heads == 4 and heads == kv_heads * GROUP:
        return per_device_by_column(*args)
    return per_device_by_span(*args)


def solution(mesh):
    placed = (
        P("seq", "tp"),
        P(),
        P("tp"),
        P("seq", "tp"),
        P("tp"),
        P("seq", None, "tp"),
        P(None, "tp"),
        P("tp", "seq"),
        P("tp"),
    )
    return jax.shard_map(
        per_device,
        mesh=mesh,
        in_specs=placed,
        out_specs=(P("seq", "tp"), P("seq", "tp")),
        check_vma=False,
    )
```

```python
import math

import jax
import jax.numpy as jnp
from jax import lax
from jax.experimental import pallas as pl
from jax.experimental.pallas import tpu as pltpu
from jax.sharding import PartitionSpec as P

MODEL_WIDTH = 4096
HEAD_SIZE = 128
GROUP = 4


eps = 1e-06
rope_base = 1000000.0


def apply_rotary(field, token_positions):
    half = field.shape[-1] // 2
    inverse = jnp.exp(-math.log(rope_base) * jnp.arange(half, dtype=jnp.float32) / half)
    angles = token_positions.astype(jnp.float32)[:, None] * inverse[None, :]
    cosine = jnp.cos(angles)[:, None, :]
    sine = jnp.sin(angles)[:, None, :]
    first = field[..., :half]
    second = field[..., half:]
    return jnp.concatenate(
        [first * cosine - second * sine, second * cosine + first * sine], axis=-1
    )


def span_lookup(order, devices):
    table_ids = jnp.arange(order.shape[0], dtype=jnp.int32)
    return jnp.sum(jnp.where(devices[:, None] == table_ids[None, :], order[None, :], 0), axis=1)


def per_device_by_span(
    hidden_in,
    span_order,
    norm_gain,
    w_query,
    bias_query,
    key_value_weight,
    bias_kv,
    w_out,
    post_gain,
):
    tok_rows = hidden_in.shape[0]
    seq_index = lax.axis_index("seq")
    own_span = span_lookup(span_order, jnp.full((1,), seq_index, jnp.int32))[0]
    token_positions = own_span * tok_rows + jnp.arange(tok_rows, dtype=jnp.int32)
    local = hidden_in.astype(jnp.float32)
    raw_rows, gains = (
        lax.all_gather(hidden_in, "tp", axis=1, tiled=True),
        lax.all_gather(norm_gain[None, :], "tp", axis=1, tiled=True),
    )
    full_rows = raw_rows.astype(jnp.float32)
    meansq = jnp.mean(full_rows * full_rows, axis=1, keepdims=True)
    normed_in = (full_rows * lax.rsqrt(meansq + eps) * gains.astype(jnp.float32)).astype(
        jnp.bfloat16
    )
    columns = normed_in
    query_proj = jnp.dot(
        columns,
        lax.all_gather(w_query, "seq", axis=0, tiled=True),
        preferred_element_type=jnp.float32,
    )
    columns = normed_in
    pair_proj = jnp.einsum(
        "tr,rkc->tkc",
        columns,
        lax.all_gather(key_value_weight, "seq", axis=0, tiled=True),
        preferred_element_type=jnp.float32,
    )
    query_heads = w_query.shape[1] // HEAD_SIZE
    kv_heads = key_value_weight.shape[2] // HEAD_SIZE
    query_proj = query_proj + bias_query.astype(jnp.float32)[None, :]
    queries = apply_rotary(
        query_proj.reshape(tok_rows, query_heads, HEAD_SIZE), token_positions
    ).astype(jnp.bfloat16)
    pair_proj = pair_proj + bias_kv.astype(jnp.float32)[None, :, :]
    rotated_keys = apply_rotary(
        pair_proj[:, 0, :].reshape(tok_rows, kv_heads, HEAD_SIZE), token_positions
    )
    rotated_keys = rotated_keys.astype(jnp.bfloat16).reshape(tok_rows, kv_heads * HEAD_SIZE)
    value_rows = pair_proj[:, 1, :].astype(jnp.bfloat16)
    grouped = (
        queries.reshape(tok_rows, kv_heads, GROUP, HEAD_SIZE)
        .transpose(1, 2, 0, 3)
        .reshape(kv_heads, GROUP * tok_rows, HEAD_SIZE)
    )
    query_pos = jnp.tile(token_positions, GROUP)
    last_query = jnp.max(token_positions)
    scale = 1.0 / math.sqrt(HEAD_SIZE)
    start_state = (
        jnp.full((kv_heads, GROUP * tok_rows), -1e30, jnp.float32),
        jnp.zeros((kv_heads, GROUP * tok_rows), jnp.float32),
        jnp.zeros((kv_heads, GROUP * tok_rows, HEAD_SIZE), jnp.float32),
    )
    key_piece = lax.all_gather(rotated_keys, "seq", axis=0, tiled=True)
    value_piece = lax.all_gather(value_rows, "seq", axis=0, tiled=True)
    count = key_piece.shape[0]
    block = math.gcd(count, 1536)

    def visit(step, state):
        first = step * block
        key_block = lax.dynamic_slice_in_dim(key_piece, first, block, 0).reshape(
            block, kv_heads, HEAD_SIZE
        )
        value_block = lax.dynamic_slice_in_dim(value_piece, first, block, 0).reshape(
            block, kv_heads, HEAD_SIZE
        )
        row_ids = first + jnp.arange(block, dtype=jnp.int32)
        key_pos = span_lookup(span_order, row_ids // tok_rows) * tok_rows + row_ids % tok_rows

        def update(current):
            maxima, totals, sums = current
            scores = (
                jnp.einsum("kqd,nkd->kqn", grouped, key_block, preferred_element_type=jnp.float32)
                * scale
            )
            allowed = (key_pos[None, :] <= query_pos[:, None])[None, :, :]
            scores = jnp.where(allowed, scores, -1e30)
            fresh = jnp.maximum(maxima, jnp.max(scores, axis=2))
            weights = jnp.where(allowed, jnp.exp(scores - fresh[:, :, None]), 0.0)
            factor = jnp.exp(maxima - fresh)
            totals = totals * factor + jnp.sum(weights, axis=2)
            sums = sums * factor[:, :, None] + jnp.einsum(
                "kqn,nkd->kqd",
                weights.astype(jnp.bfloat16),
                value_block,
                preferred_element_type=jnp.float32,
            )
            return (fresh, totals, sums)

        return lax.cond(jnp.min(key_pos) <= last_query, update, lambda current: current, state)

    maxima, totals, sums = lax.fori_loop(0, count // block, visit, start_state)
    attended = (sums / totals[:, :, None]).astype(jnp.bfloat16)
    attended = (
        attended.reshape(kv_heads, GROUP, tok_rows, HEAD_SIZE)
        .transpose(2, 0, 1, 3)
        .reshape(tok_rows, query_heads * HEAD_SIZE)
    )
    partial_out = jnp.dot(
        attended,
        lax.all_gather(w_out, "seq", axis=1, tiled=True),
        preferred_element_type=jnp.float32,
    )
    mixed = lax.psum_scatter(
        partial_out.astype(jnp.bfloat16), "tp", scatter_dimension=1, tiled=True
    ).astype(jnp.float32)
    attn_out = mixed.astype(jnp.bfloat16)
    stream = local + mixed
    post_sq = lax.psum(jnp.sum(stream * stream, axis=1), "tp")
    normed = (
        stream
        * lax.rsqrt(post_sq / MODEL_WIDTH + eps)[:, None]
        * post_gain.astype(jnp.float32)[None, :]
    ).astype(jnp.bfloat16)
    return (attn_out, normed)


MESH = pl.DeviceIdType.MESH
CORES = 2
PLANE = 4
PIECES = 2
PAIR = 2 * HEAD_SIZE


def at(z, x, c):
    return z * PLANE + x * CORES + c


class Traffic:
    def __init__(self, depth, z, sem, proxy, peer):
        self.z, self.sem, self.proxy, self.peer = z, sem, proxy, peer
        self.rows = [0] * depth

    def remote(self, source, landing, arrival, target, sem=None):
        return pltpu.make_async_remote_copy(
            src_ref=source,
            dst_ref=landing,
            send_sem=self.sem.at[0] if sem is None else sem,
            recv_sem=arrival,
            device_id=target,
            device_id_type=MESH,
        )

    def count(self, ref, where=None, times=1):
        size = math.prod(ref.shape) * times // self.proxy.shape[1]
        for k in range(len(self.rows)):
            if where is None or where(k):
                self.rows[k] += size

    def send(self, source, landing, arrival, target, where=None, also=None, sem=None):
        when = None if where is None else where(self.z)
        if also is not None:
            when = also if when is None else jnp.logical_and(when, also)
        guarded(when, lambda: self.remote(source, landing, arrival, target, sem).start())
        if sem is None and also is None:
            self.count(source, where)

    def arrive(self, landing, arrival, when=None):
        guarded(when, lambda: self.remote(landing, landing, arrival, self.peer).wait_recv())

    def left(self, source, sem, when=None):
        guarded(when, lambda: self.remote(source, source, sem, self.peer, sem).wait_send())

    def finish(self):
        for k, size in enumerate(self.rows):
            block = self.proxy.at[pl.ds(0, size)]
            self.left(block, self.sem.at[0], self.z == k)


def guarded(when, action):
    if when is None:
        action()
    else:
        pl.when(when)(action)


def rotate(field, cosine, sine):
    return field * cosine + pltpu.roll(field, HEAD_SIZE // 2, 1) * sine


def column_kernel(
    depth,
    hidden, order, gain, post_gain, bias_q, wq, wkv, bias_kv, w_out,
    mixed_out, factor_out, post_out,
    rows, full, gains, weights, outw, kvs, queries, att, part, terms, others, squares,
    kv_pieces, cos_t, sin_t, key_pos, gain_rows, bias_b, bias_p, proxy,
    local_sem, send_sem, small_sem, relay_sem, rows_sem, rows_side_sem,
    w_sem, w_across_sem, w_side_sem, out_end_sem, out_across_sem, out_side_sem, kv_sem, att_sem, term_sem, other_sem,
):
    s, t = lax.axis_index("seq"), lax.axis_index("tp")
    z, x, c = s // PLANE, s % PLANE // CORES, s % CORES
    last = depth - 1
    span, half_width = hidden.shape
    column = x * CORES + c
    sibling, across, other = (at(z, x, 1 - c), t), (at(z, 1 - x, c), t), (s, 1 - t)
    above, below = (at(jnp.minimum(z + 1, last), x, c), t), (at(jnp.maximum(z - 1, 0), x, c), t)

    barrier = pltpu.get_barrier_semaphore()
    peers = [sibling, across, other] + [(at(lax.rem(z + d, depth), x, c), t) for d in range(1, depth)]
    for peer in peers:
        pl.semaphore_signal(barrier, inc=1, device_id=peer, device_id_type=MESH)
    pl.semaphore_wait(barrier, len(peers))

    go = Traffic(depth, z, send_sem, proxy, sibling)
    edge = span // PIECES

    def bit(p):
        return pl.ds(p * edge, edge)

    go.send(gain, gains.at[t], small_sem.at[0], other, sem=small_sem.at[1])
    for p in range(PIECES):
        mine, landing = hidden.at[bit(p)], rows.at[z, t, bit(p)]
        go.send(mine, landing, rows_side_sem.at[z], other)
        go.send(mine, landing, rows_sem.at[z, p], above, lambda k: k < last)
        go.send(mine, landing, rows_sem.at[z, p], below, lambda k: k > 0)
    own = [
        pltpu.make_async_copy(hidden, rows.at[z, t], local_sem.at[0]),
        pltpu.make_async_copy(
            bias_kv.at[:, pl.ds(pl.multiple_of(z * HEAD_SIZE, HEAD_SIZE), HEAD_SIZE)], bias_p, local_sem.at[1]
        ),
        pltpu.make_async_copy(w_out, outw.at[1, column], local_sem.at[2]),
    ]

    def q_piece(g, zt):
        return wq.at[:, pl.ds(pl.multiple_of(zt * 2 * PAIR + (g - 1) * PAIR, PAIR), PAIR)]

    for g in (1, 2):
        own.append(pltpu.make_async_copy(q_piece(g, z), weights.at[g, s], local_sem.at[2 + g]))
    for copy in own:
        copy.start()
    for zt in range(depth):
        for i in range(2):
            kv_pieces[zt, :, i * HEAD_SIZE : (i + 1) * HEAD_SIZE] = wkv[:, i, zt * HEAD_SIZE : (zt + 1) * HEAD_SIZE]
    weights[0, s] = kv_pieces[z]
    for g in (0, 1, 2):
        source = kv_pieces.at[z] if g == 0 else q_piece(g, z)
        go.send(source, weights.at[g, s], w_across_sem.at[g], across)
        go.send(source, weights.at[g, s], w_side_sem.at[g], sibling)
    inner = lambda k: (k > 0) & (k < last)
    outer = lambda k: (k == 0) | (k == last)
    middle = inner(z)
    go.send(w_out, outw.at[1, column], out_across_sem.at[1], across, inner)
    go.send(w_out, outw.at[1, column], out_side_sem.at[1], sibling, inner)
    own_end = jnp.where(z < depth // 2, 0, last)
    gatherer = jnp.where(middle, last - z, jnp.where(z == 0, 1, last - 1))

    def leave_columns(part_id):
        place = pl.ds(part_id * (w_out.shape[0] // 2), w_out.shape[0] // 2)
        landing = outw.at[0, column, place]
        go.send(w_out.at[place], landing, out_end_sem.at[0], (at(gatherer, x, c), t), outer)

    def spread(stage, groups):
        for g in groups:
            for zt, where in ((stage, lambda k: k < stage), (last - stage, lambda k: k > last - stage)):
                source = kv_pieces.at[zt] if g == 0 else q_piece(g, zt)
                go.send(source, weights.at[g, s], w_sem.at[g, z], (at(zt, x, c), t), where)

    def take_weights(g, stage, distances=None):
        for distance in distances or range(1, stage + 1):
            for sign, goal in ((-1, stage), (1, last - stage)):
                zs = jnp.clip(z + sign * distance, 0, last)
                block = weights.at[g, at(zs, x, c)]
                go.arrive(block, w_sem.at[g, zs], z == goal)
                go.send(block, block, w_across_sem.at[g], across, lambda k: k == goal)
                go.send(block, block, w_side_sem.at[g], sibling, lambda k: k == goal)

    def chain(distance, action):
        for sign in (1, -1):
            zs = jnp.clip(z - sign * distance, 0, last)
            where = lambda k: (k >= distance) if sign == 1 else (k + distance <= last)
            target = above if sign == 1 else below
            more = (lambda k: distance <= k < last) if sign == 1 else (lambda k: 0 < k <= last - distance)
            if distance < last:
                now = jnp.logical_and(z >= distance, z < last) if sign == 1 else jnp.logical_and(z > 0, z <= last - distance)
                action(zs, where, target, (more, now))
            else:
                action(zs, where, target, None)

    def relay(block, arrival, target, more, sem=None):
        if more is not None:
            where, now = more
            pl.when(now)(lambda: go.remote(block, block, arrival, target, sem).start())
            if sem is None:
                go.count(block, where)

    def pass_rows(distance):
        for p in range(PIECES):

            def action(zs, where, target, more):
                block = rows.at[zs, t, bit(p)]
                go.arrive(block, rows_sem.at[zs, p], where(z))
                relay(block, rows_sem.at[zs, p], target, more, relay_sem.at[0] if distance == last - 1 else None)
                go.send(block, block, rows_side_sem.at[zs], other, where)

            chain(distance, action)

    def weights_across(g):
        go.arrive(weights.at[g, pl.ds(0, depth)], w_across_sem.at[g])
        for zs in range(depth):
            block = weights.at[g, at(zs, 1 - x, c)]
            go.send(block, block, w_side_sem.at[g], sibling)

    def weights_beside(g):
        go.arrive(weights.at[g, pl.ds(0, depth * CORES)], w_side_sem.at[g])

    def normalize(zs):
        go.arrive(rows.at[zs, 1 - t], rows_side_sem.at[zs])

        def strip(i, carry):
            r = pl.ds(pl.multiple_of(i * 16, 16), 16)
            halves = [rows[zs, h, r, :].astype(jnp.float32) for h in range(2)]
            total = sum(jnp.sum(a * a, axis=1, keepdims=True) for a in halves)
            factor = lax.rsqrt(total / (2 * half_width) + eps)
            for h in range(2):
                full[zs, r, h * half_width : (h + 1) * half_width] = (
                    halves[h] * factor * gain_rows[h]
                ).astype(jnp.bfloat16)
            return carry

        lax.fori_loop(0, span // 16, strip, 0)

    lane = lax.broadcasted_iota(jnp.int32, (span, HEAD_SIZE), 1)
    line = lax.broadcasted_iota(jnp.int32, (span, HEAD_SIZE), 0)
    half = HEAD_SIZE // 2
    pair_id = jnp.where(lane < half, lane, lane - half).astype(jnp.float32)
    inverse = jnp.exp(-math.log(rope_base) * pair_id / half)

    def table(zs, carry):
        angles = (order[zs * PLANE + column] * span + line).astype(jnp.float32) * inverse
        cos_t[zs] = jnp.cos(angles)
        sine = jnp.sin(angles)
        sin_t[zs] = jnp.where(lane < half, -sine, sine)
        return carry

    lax.fori_loop(0, depth, table, 0)
    for m in range(PLANE):
        for zs in range(depth):
            i = m * depth + zs
            key_pos[:, i * span : (i + 1) * span] = order[zs * PLANE + m] * span + lax.broadcasted_iota(
                jnp.int32, (1, span), 1
            )
    for copy in own:
        copy.wait()
    gains[t] = gain[...]
    go.arrive(gains.at[1 - t], small_sem.at[0])
    for h in range(2):
        rows_of = gains[h].astype(jnp.float32)
        for i in range(half_width // HEAD_SIZE):
            gain_rows[h, :, i * HEAD_SIZE : (i + 1) * HEAD_SIZE] = rows_of[i : i + 1]
    bias_b[...] = bias_q[...].astype(jnp.float32)
    post_rows = post_gain[...].astype(jnp.float32)
    for i in range(half_width // HEAD_SIZE):
        post_out[:, i * HEAD_SIZE : (i + 1) * HEAD_SIZE] = post_rows[i : i + 1]

    pass_rows(1)
    spread(1, (0, 1, 2))
    spread(3, (0, 1))
    leave_columns(0)
    normalize(z)
    pass_rows(2)
    spread(2, (0, 1, 2))
    leave_columns(1)
    for g in (0, 1, 2):
        take_weights(g, 1)
    normalize(z + 1 - 2 * lax.rem(z, 2))
    take_weights(0, 3)
    take_weights(1, 3)
    go.left(rows.at[z, t], relay_sem.at[0], middle)
    pass_rows(3)
    spread(3, (2,))
    for g in (0, 1):
        take_weights(g, 2)
    normalize(lax.rem(z + 2, depth))
    take_weights(2, 3, (1,))
    normalize(last - z)
    weights_across(0)
    weights_beside(0)

    tokens = depth * span

    def product(g):
        return jnp.dot(
            full[...].reshape(tokens, 2 * half_width),
            weights[g].reshape(2 * half_width, PAIR),
            preferred_element_type=jnp.float32,
        )

    cosine, sine = cos_t[...].reshape(tokens, HEAD_SIZE), sin_t[...].reshape(tokens, HEAD_SIZE)
    pair = product(0)
    keys = pair[:, :HEAD_SIZE] + bias_p[0:1, :].astype(jnp.float32)
    kvs[column, :, :HEAD_SIZE] = rotate(keys, cosine, sine).astype(jnp.bfloat16)
    kvs[column, :, HEAD_SIZE:] = (pair[:, HEAD_SIZE:] + bias_p[1:2, :].astype(jnp.float32)).astype(jnp.bfloat16)
    go.send(kvs.at[column], kvs.at[column], kv_sem.at[0], across)
    go.send(kvs.at[column], kvs.at[column], kv_sem.at[1], sibling)
    take_weights(2, 2)
    take_weights(2, 3, (2, 3))

    @pl.when(middle)
    def _():
        block = outw.at[0, column]
        go.arrive(block, out_end_sem.at[0])
        go.remote(block, block, out_across_sem.at[0], across).start()
        go.remote(block, block, out_side_sem.at[0], sibling).start()

    go.count(outw.at[0, 0], inner, times=2)

    scale = math.log2(math.e) / math.sqrt(HEAD_SIZE)

    def make_queries(g):
        field = product(g)
        for i in range(2):
            cut = slice(i * HEAD_SIZE, (i + 1) * HEAD_SIZE)
            head = field[:, cut] + bias_b[pl.ds(z * GROUP + (g - 1) * 2 + i, 1), :]
            turned = (rotate(head, cosine, sine) * scale).astype(jnp.bfloat16)
            queries[g - 1, :, i * span : (i + 1) * span, :] = turned.reshape(depth, span, HEAD_SIZE)

    weights_across(1)
    weights_beside(1)
    make_queries(1)
    kv_across = kvs.at[(1 - x) * CORES + c]
    go.arrive(kv_across, kv_sem.at[0])
    go.send(kv_across, kv_across, kv_sem.at[1], sibling)
    go.arrive(kvs.at[pl.ds(0, CORES)], kv_sem.at[1])

    def att_piece(g, zs, b):
        return att.at[g, zs, pl.ds(pl.multiple_of(b * span, span), span)]

    def nth(i):
        return jnp.where(i == 0, 0, jnp.where(i == 1, last, jnp.where(i == 2, 1 + c, 2 - c)))

    def attend(g):
        def turn(i, carry):
            b = nth(i)
            scores = lax.dot_general(
                queries[g, b],
                kvs[:, :, :HEAD_SIZE].reshape(PLANE * tokens, HEAD_SIZE),
                (((1,), (1,)), ((), ())),
                preferred_element_type=jnp.float32,
            )
            first = order[b * PLANE + column] * span
            query_pos = first + lax.rem(lax.broadcasted_iota(jnp.int32, (2 * span, 1), 0), span)
            scores = jnp.where(key_pos[...] <= query_pos, scores, -jnp.inf)
            peak = jnp.max(scores, axis=1, keepdims=True)
            shares = jnp.exp2(scores - peak)
            totals = jnp.sum(shares, axis=1, keepdims=True)
            summed = jnp.dot(
                shares.astype(jnp.bfloat16),
                kvs[:, :, HEAD_SIZE:].reshape(PLANE * tokens, HEAD_SIZE),
                preferred_element_type=jnp.float32,
            )
            result = (summed / totals).astype(jnp.bfloat16)
            place = pl.ds(pl.multiple_of(b * span, span), span)
            att[g, z, place, :HEAD_SIZE] = result[:span]
            att[g, z, place, HEAD_SIZE:] = result[span:]
            block = att_piece(g, z, b)
            go.remote(block, block, att_sem.at[g, z, b], (at(gatherer, x, c), t)).start()
            return carry

        lax.fori_loop(0, depth, turn, 0)
        go.count(att.at[g, 0])

    attend(0)
    weights_across(2)
    weights_beside(2)
    make_queries(2)

    def hand_on(g, i):
        block, sem = att_piece(g, own_end, nth(i)), att_sem.at[g, own_end, nth(i)]
        go.arrive(block, sem)
        go.remote(block, block, sem, (at(last - z, x, c), t)).start()

    @pl.when(middle)
    def _():
        for i in range(depth):
            hand_on(0, i)

    attend(1)
    halves = 2
    each = PLANE // halves
    share = depth // 2

    def piece(ref, i, h):
        return ref.at[i, pl.ds(h * each, each)]

    def mix_block(b):
        place = pl.ds(pl.multiple_of(b * span, span), span)
        for e, owner in ((0, own_end), (1, z)):
            for h in range(halves):
                for m in range(h * each, (h + 1) * each):
                    total = None
                    for zs in range(depth):
                        for g in range(2):
                            first = zs * 2 * PAIR + g * PAIR
                            term = jnp.dot(
                                att[g, zs, place, :],
                                outw[e, m, first : first + PAIR, :],
                                preferred_element_type=jnp.float32,
                            )
                            total = term if total is None else total + term
                    value = total.astype(jnp.bfloat16)

                    @pl.when(b == z)
                    def _():
                        terms[owner, m] = value

                    @pl.when(b != z)
                    def _():
                        part[e, b, m] = value

                @pl.when(b != z)
                def _():
                    source = piece(part.at[e], b, h)
                    go.remote(source, piece(terms, owner, h), term_sem.at[owner, h], (at(b, x, c), t)).start()

    @pl.when(middle)
    def _():
        def side_columns(e):
            block = outw.at[e, (1 - x) * CORES + c]
            go.arrive(block, out_across_sem.at[e])
            go.remote(block, block, out_side_sem.at[e], sibling).start()

        side_columns(1)
        for i in range(depth):
            hand_on(1, i)
        side_columns(0)
        for e in (1, 0):
            go.arrive(outw.at[e, pl.ds(0, CORES)], out_side_sem.at[e])
        for i in range(depth):
            for zs in (last - z, last - own_end):
                for g in range(2):
                    go.arrive(att_piece(g, zs, nth(i)), att_sem.at[g, zs, nth(i)])
            mix_block(nth(i))

    go.count(outw.at[0, 0], inner, times=2)
    go.count(att.at[:, 0], inner)
    go.count(part.at[0, 0], inner, times=2 * (depth - 1))

    near = jnp.where(z < share, 0, share)
    for e in range(2):
        for h in range(halves):
            for first in (near, share - near):
                maker = jnp.where(first == 0, 1, last - 1)
                index = jnp.where(first == 0, e, 1 - e)
                block = piece(terms, first + index, h)
                go.arrive(block, term_sem.at[first + index, h], z != maker)
                go.send(block, piece(others, index, h), other_sem.at[index, h], other, also=t != first // share)
    go.count(others.at[0], times=share)

    width = w_out.shape[1]
    sums = jnp.zeros((span, 1), jnp.float32)
    pieces = [(j, m) for j in range(share) for m in range(PLANE)]
    for j, m in pieces:
        if m % each == 0:
            go.arrive(piece(others, j, m // each), other_sem.at[j, m // each])
        cut = slice((j * PLANE + m) * width, (j * PLANE + m + 1) * width)
        mixed = terms[t * share + j, m].astype(jnp.float32) + others[j, m].astype(jnp.float32)
        mixed_out[:, cut] = mixed
        stream = rows[z, t, :, cut].astype(jnp.float32) + mixed
        sums = sums + jnp.sum(stream * stream, axis=1, keepdims=True)
    squares[t] = jnp.broadcast_to(sums, (span, span)).T[:8]
    go.send(squares.at[t], squares.at[t], small_sem.at[2], other, sem=small_sem.at[3])
    go.arrive(squares.at[1 - t], small_sem.at[2])
    total = (squares[0] + squares[1])[:1]
    factor_out[...] = lax.rsqrt(total / (2 * half_width) + eps)
    go.left(gain, small_sem.at[1])
    go.left(squares.at[t], small_sem.at[3])
    go.finish()


def per_device_by_column(
    hidden_in,
    span_order,
    norm_gain,
    w_query,
    bias_query,
    key_value_weight,
    bias_kv,
    w_out,
    post_gain,
):
    span, half_width = hidden_in.shape
    n_seq = span_order.shape[0]
    depth = n_seq // PLANE
    slab = w_query.shape[0]
    tokens = depth * span
    vmem, hbm, smem = (pl.BlockSpec(memory_space=m) for m in (pltpu.VMEM, pl.ANY, pltpu.SMEM))
    dma = pltpu.SemaphoreType.DMA
    bf16 = lambda *shape: pltpu.VMEM(shape, jnp.bfloat16)
    f32 = lambda *shape: pltpu.VMEM(shape, jnp.float32)
    width = w_out.shape[1]
    f32_out = lambda *shape: jax.ShapeDtypeStruct(shape, jnp.float32)
    mixed, factor, post = pl.pallas_call(
        lambda *refs: column_kernel(depth, *refs),
        out_shape=(f32_out(span, half_width), f32_out(1, span), f32_out(1, half_width)),
        in_specs=[hbm, smem, vmem, vmem, vmem, hbm, vmem, hbm, hbm],
        out_specs=(vmem, vmem, vmem),
        scratch_shapes=[
            bf16(depth, 2, span, half_width),
            bf16(depth, span, 2 * half_width),
            bf16(2, half_width // HEAD_SIZE, HEAD_SIZE),
            bf16(3, n_seq, slab, PAIR),
            bf16(2, PLANE, w_out.shape[0], width),
            bf16(PLANE, tokens, PAIR),
            bf16(2, depth, 2 * span, HEAD_SIZE),
            bf16(2, depth, tokens, PAIR),
            bf16(2, depth, PLANE, span, width),
            bf16(depth, PLANE, span, width),
            bf16(depth // 2, PLANE, span, width),
            f32(2, 8, span),
            bf16(depth, slab, PAIR),
            f32(depth, span, HEAD_SIZE),
            f32(depth, span, HEAD_SIZE),
            pltpu.VMEM((1, PLANE * tokens), jnp.int32),
            f32(2, 1, half_width),
            f32(half_width // HEAD_SIZE, HEAD_SIZE),
            bf16(2, HEAD_SIZE),
            bf16(5120, half_width),
            dma((5,)),
            dma((1,)),
            dma((4,)),
            dma((1,)),
            dma((depth, PIECES)),
            dma((depth,)),
            dma((3, depth)),
            dma((3,)),
            dma((3,)),
            dma((1,)),
            dma((2,)),
            dma((2,)),
            dma((2,)),
            dma((2, depth, depth)),
            dma((depth, 2)),
            dma((depth // 2, 2)),
        ],
        compiler_params=pltpu.CompilerParams(
            collective_id=0, has_side_effects=True, vmem_limit_bytes=60 * 1024 * 1024
        ),
        name="sublayer",
    )(
        hidden_in,
        span_order,
        norm_gain.reshape(-1, HEAD_SIZE),
        post_gain.reshape(-1, HEAD_SIZE),
        bias_query.reshape(-1, HEAD_SIZE),
        w_query,
        key_value_weight,
        bias_kv,
        w_out,
    )
    stream = hidden_in.astype(jnp.float32) + mixed
    normed = (stream * factor.reshape(span, 1) * post).astype(jnp.bfloat16)
    return (mixed.astype(jnp.bfloat16), normed)


def per_device(*args):
    hidden_in, span_order, w_query, kv_weight = args[0], args[1], args[3], args[5]
    n_seq = span_order.shape[0]
    n_tp = MODEL_WIDTH // hidden_in.shape[1]
    heads = w_query.shape[1] // HEAD_SIZE
    kv_heads = kv_weight.shape[2] // HEAD_SIZE
    if n_tp == 2 and n_seq == 4 * PLANE and kv_heads == 4 and heads == kv_heads * GROUP:
        return per_device_by_column(*args)
    return per_device_by_span(*args)


def solution(mesh):
    placed = (
        P("seq", "tp"),
        P(),
        P("tp"),
        P("seq", "tp"),
        P("tp"),
        P("seq", None, "tp"),
        P(None, "tp"),
        P("tp", "seq"),
        P("tp"),
    )
    return jax.shard_map(
        per_device,
        mesh=mesh,
        in_specs=placed,
        out_specs=(P("seq", "tp"), P("seq", "tp")),
        check_vma=False,
    )
```

```python
import math

import jax
import jax.numpy as jnp
from jax import lax
from jax.experimental import pallas as pl
from jax.experimental.pallas import tpu as pltpu
from jax.sharding import PartitionSpec as P

MODEL_WIDTH = 4096
HEAD_SIZE = 128
GROUP = 4


eps = 1e-06
rope_base = 1000000.0


def apply_rotary(field, token_positions):
    half = field.shape[-1] // 2
    inverse = jnp.exp(-math.log(rope_base) * jnp.arange(half, dtype=jnp.float32) / half)
    angles = token_positions.astype(jnp.float32)[:, None] * inverse[None, :]
    cosine = jnp.cos(angles)[:, None, :]
    sine = jnp.sin(angles)[:, None, :]
    first = field[..., :half]
    second = field[..., half:]
    return jnp.concatenate(
        [first * cosine - second * sine, second * cosine + first * sine], axis=-1
    )


def span_lookup(order, devices):
    table_ids = jnp.arange(order.shape[0], dtype=jnp.int32)
    return jnp.sum(jnp.where(devices[:, None] == table_ids[None, :], order[None, :], 0), axis=1)


def per_device_by_span(
    hidden_in,
    span_order,
    norm_gain,
    w_query,
    bias_query,
    key_value_weight,
    bias_kv,
    w_out,
    post_gain,
):
    tok_rows = hidden_in.shape[0]
    seq_index = lax.axis_index("seq")
    own_span = span_lookup(span_order, jnp.full((1,), seq_index, jnp.int32))[0]
    token_positions = own_span * tok_rows + jnp.arange(tok_rows, dtype=jnp.int32)
    local = hidden_in.astype(jnp.float32)
    raw_rows, gains = (
        lax.all_gather(hidden_in, "tp", axis=1, tiled=True),
        lax.all_gather(norm_gain[None, :], "tp", axis=1, tiled=True),
    )
    full_rows = raw_rows.astype(jnp.float32)
    meansq = jnp.mean(full_rows * full_rows, axis=1, keepdims=True)
    normed_in = (full_rows * lax.rsqrt(meansq + eps) * gains.astype(jnp.float32)).astype(
        jnp.bfloat16
    )
    columns = normed_in
    query_proj = jnp.dot(
        columns,
        lax.all_gather(w_query, "seq", axis=0, tiled=True),
        preferred_element_type=jnp.float32,
    )
    columns = normed_in
    pair_proj = jnp.einsum(
        "tr,rkc->tkc",
        columns,
        lax.all_gather(key_value_weight, "seq", axis=0, tiled=True),
        preferred_element_type=jnp.float32,
    )
    query_heads = w_query.shape[1] // HEAD_SIZE
    kv_heads = key_value_weight.shape[2] // HEAD_SIZE
    query_proj = query_proj + bias_query.astype(jnp.float32)[None, :]
    queries = apply_rotary(
        query_proj.reshape(tok_rows, query_heads, HEAD_SIZE), token_positions
    ).astype(jnp.bfloat16)
    pair_proj = pair_proj + bias_kv.astype(jnp.float32)[None, :, :]
    rotated_keys = apply_rotary(
        pair_proj[:, 0, :].reshape(tok_rows, kv_heads, HEAD_SIZE), token_positions
    )
    rotated_keys = rotated_keys.astype(jnp.bfloat16).reshape(tok_rows, kv_heads * HEAD_SIZE)
    value_rows = pair_proj[:, 1, :].astype(jnp.bfloat16)
    grouped = (
        queries.reshape(tok_rows, kv_heads, GROUP, HEAD_SIZE)
        .transpose(1, 2, 0, 3)
        .reshape(kv_heads, GROUP * tok_rows, HEAD_SIZE)
    )
    query_pos = jnp.tile(token_positions, GROUP)
    last_query = jnp.max(token_positions)
    scale = 1.0 / math.sqrt(HEAD_SIZE)
    start_state = (
        jnp.full((kv_heads, GROUP * tok_rows), -1e30, jnp.float32),
        jnp.zeros((kv_heads, GROUP * tok_rows), jnp.float32),
        jnp.zeros((kv_heads, GROUP * tok_rows, HEAD_SIZE), jnp.float32),
    )
    key_piece = lax.all_gather(rotated_keys, "seq", axis=0, tiled=True)
    value_piece = lax.all_gather(value_rows, "seq", axis=0, tiled=True)
    count = key_piece.shape[0]
    block = math.gcd(count, 1536)

    def visit(step, state):
        first = step * block
        key_block = lax.dynamic_slice_in_dim(key_piece, first, block, 0).reshape(
            block, kv_heads, HEAD_SIZE
        )
        value_block = lax.dynamic_slice_in_dim(value_piece, first, block, 0).reshape(
            block, kv_heads, HEAD_SIZE
        )
        row_ids = first + jnp.arange(block, dtype=jnp.int32)
        key_pos = span_lookup(span_order, row_ids // tok_rows) * tok_rows + row_ids % tok_rows

        def update(current):
            maxima, totals, sums = current
            scores = (
                jnp.einsum("kqd,nkd->kqn", grouped, key_block, preferred_element_type=jnp.float32)
                * scale
            )
            allowed = (key_pos[None, :] <= query_pos[:, None])[None, :, :]
            scores = jnp.where(allowed, scores, -1e30)
            fresh = jnp.maximum(maxima, jnp.max(scores, axis=2))
            weights = jnp.where(allowed, jnp.exp(scores - fresh[:, :, None]), 0.0)
            factor = jnp.exp(maxima - fresh)
            totals = totals * factor + jnp.sum(weights, axis=2)
            sums = sums * factor[:, :, None] + jnp.einsum(
                "kqn,nkd->kqd",
                weights.astype(jnp.bfloat16),
                value_block,
                preferred_element_type=jnp.float32,
            )
            return (fresh, totals, sums)

        return lax.cond(jnp.min(key_pos) <= last_query, update, lambda current: current, state)

    maxima, totals, sums = lax.fori_loop(0, count // block, visit, start_state)
    attended = (sums / totals[:, :, None]).astype(jnp.bfloat16)
    attended = (
        attended.reshape(kv_heads, GROUP, tok_rows, HEAD_SIZE)
        .transpose(2, 0, 1, 3)
        .reshape(tok_rows, query_heads * HEAD_SIZE)
    )
    partial_out = jnp.dot(
        attended,
        lax.all_gather(w_out, "seq", axis=1, tiled=True),
        preferred_element_type=jnp.float32,
    )
    mixed = lax.psum_scatter(
        partial_out.astype(jnp.bfloat16), "tp", scatter_dimension=1, tiled=True
    ).astype(jnp.float32)
    attn_out = mixed.astype(jnp.bfloat16)
    stream = local + mixed
    post_sq = lax.psum(jnp.sum(stream * stream, axis=1), "tp")
    normed = (
        stream
        * lax.rsqrt(post_sq / MODEL_WIDTH + eps)[:, None]
        * post_gain.astype(jnp.float32)[None, :]
    ).astype(jnp.bfloat16)
    return (attn_out, normed)


MESH = pl.DeviceIdType.MESH
CORES = 2
PLANE = 4
PIECES = 2
PAIR = 2 * HEAD_SIZE


def at(z, x, c):
    return z * PLANE + x * CORES + c


class Traffic:
    def __init__(self, depth, z, sem, proxy, peer):
        self.z, self.sem, self.proxy, self.peer = z, sem, proxy, peer
        self.rows = [0] * depth

    def remote(self, source, landing, arrival, target, sem=None):
        return pltpu.make_async_remote_copy(
            src_ref=source,
            dst_ref=landing,
            send_sem=self.sem.at[0] if sem is None else sem,
            recv_sem=arrival,
            device_id=target,
            device_id_type=MESH,
        )

    def count(self, ref, where=None, times=1):
        size = math.prod(ref.shape) * times // self.proxy.shape[1]
        for k in range(len(self.rows)):
            if where is None or where(k):
                self.rows[k] += size

    def send(self, source, landing, arrival, target, where=None, also=None, sem=None):
        when = None if where is None else where(self.z)
        if also is not None:
            when = also if when is None else jnp.logical_and(when, also)
        guarded(when, lambda: self.remote(source, landing, arrival, target, sem).start())
        if sem is None and also is None:
            self.count(source, where)

    def arrive(self, landing, arrival, when=None):
        guarded(when, lambda: self.remote(landing, landing, arrival, self.peer).wait_recv())

    def left(self, source, sem, when=None):
        guarded(when, lambda: self.remote(source, source, sem, self.peer, sem).wait_send())

    def finish(self):
        for k, size in enumerate(self.rows):
            block = self.proxy.at[pl.ds(0, size)]
            self.left(block, self.sem.at[0], self.z == k)


def guarded(when, action):
    if when is None:
        action()
    else:
        pl.when(when)(action)


def rotate(field, cosine, sine):
    return field * cosine + pltpu.roll(field, HEAD_SIZE // 2, 1) * sine


def column_kernel(
    depth,
    hidden, order, gain, post_gain, bias_q, wq, wkv, bias_kv, w_out,
    mixed_out, factor_out, post_out,
    rows, full, gains, weights, outw, kvs, queries, att, part, terms, others, squares,
    kv_pieces, cos_t, sin_t, key_pos, gain_rows, bias_b, bias_p, mixed_rows, proxy,
    local_sem, send_sem, small_sem, relay_sem, rows_sem, rows_side_sem,
    w_sem, w_across_sem, w_side_sem, out_end_sem, out_across_sem, out_side_sem, kv_sem, att_sem, term_sem, other_sem,
):
    s, t = lax.axis_index("seq"), lax.axis_index("tp")
    z, x, c = s // PLANE, s % PLANE // CORES, s % CORES
    last = depth - 1
    span, half_width = hidden.shape
    column = x * CORES + c
    sibling, across, other = (at(z, x, 1 - c), t), (at(z, 1 - x, c), t), (s, 1 - t)
    above, below = (at(jnp.minimum(z + 1, last), x, c), t), (at(jnp.maximum(z - 1, 0), x, c), t)

    barrier = pltpu.get_barrier_semaphore()
    peers = [sibling, across, other] + [(at(lax.rem(z + d, depth), x, c), t) for d in range(1, depth)]
    for peer in peers:
        pl.semaphore_signal(barrier, inc=1, device_id=peer, device_id_type=MESH)
    pl.semaphore_wait(barrier, len(peers))

    go = Traffic(depth, z, send_sem, proxy, sibling)
    edge = span // PIECES

    def bit(p):
        return pl.ds(p * edge, edge)

    go.send(gain, gains.at[t], small_sem.at[0], other, sem=small_sem.at[1])
    for p in range(PIECES):
        mine, landing = hidden.at[bit(p)], rows.at[z, t, bit(p)]
        go.send(mine, landing, rows_side_sem.at[z], other)
        go.send(mine, landing, rows_sem.at[z, p], above, lambda k: k < last)
        go.send(mine, landing, rows_sem.at[z, p], below, lambda k: k > 0)
    own = [
        pltpu.make_async_copy(hidden, rows.at[z, t], local_sem.at[0]),
        pltpu.make_async_copy(
            bias_kv.at[:, pl.ds(pl.multiple_of(z * HEAD_SIZE, HEAD_SIZE), HEAD_SIZE)], bias_p, local_sem.at[1]
        ),
        pltpu.make_async_copy(w_out, outw.at[1, column], local_sem.at[2]),
    ]

    def q_piece(g, zt):
        return wq.at[:, pl.ds(pl.multiple_of(zt * 2 * PAIR + (g - 1) * PAIR, PAIR), PAIR)]

    for g in (1, 2):
        own.append(pltpu.make_async_copy(q_piece(g, z), weights.at[g, s], local_sem.at[2 + g]))
    for copy in own:
        copy.start()
    for zt in range(depth):
        for i in range(2):
            kv_pieces[zt, :, i * HEAD_SIZE : (i + 1) * HEAD_SIZE] = wkv[:, i, zt * HEAD_SIZE : (zt + 1) * HEAD_SIZE]
    weights[0, s] = kv_pieces[z]
    for g in (0, 1, 2):
        source = kv_pieces.at[z] if g == 0 else q_piece(g, z)
        go.send(source, weights.at[g, s], w_across_sem.at[g], across)
        go.send(source, weights.at[g, s], w_side_sem.at[g], sibling)
    inner = lambda k: (k > 0) & (k < last)
    outer = lambda k: (k == 0) | (k == last)
    middle = inner(z)
    go.send(w_out, outw.at[1, column], out_across_sem.at[1], across, inner)
    go.send(w_out, outw.at[1, column], out_side_sem.at[1], sibling, inner)
    own_end = jnp.where(z < depth // 2, 0, last)
    gatherer = jnp.where(middle, last - z, jnp.where(z == 0, 1, last - 1))

    def leave_columns(part_id):
        place = pl.ds(part_id * (w_out.shape[0] // 2), w_out.shape[0] // 2)
        landing = outw.at[0, column, place]
        go.send(w_out.at[place], landing, out_end_sem.at[0], (at(gatherer, x, c), t), outer)

    def spread(stage, groups):
        for g in groups:
            for zt, where in ((stage, lambda k: k < stage), (last - stage, lambda k: k > last - stage)):
                source = kv_pieces.at[zt] if g == 0 else q_piece(g, zt)
                go.send(source, weights.at[g, s], w_sem.at[g, z], (at(zt, x, c), t), where)

    def take_weights(g, stage, distances=None):
        for distance in distances or range(1, stage + 1):
            for sign, goal in ((-1, stage), (1, last - stage)):
                zs = jnp.clip(z + sign * distance, 0, last)
                block = weights.at[g, at(zs, x, c)]
                go.arrive(block, w_sem.at[g, zs], z == goal)
                go.send(block, block, w_across_sem.at[g], across, lambda k: k == goal)
                go.send(block, block, w_side_sem.at[g], sibling, lambda k: k == goal)

    def chain(distance, action):
        for sign in (1, -1):
            zs = jnp.clip(z - sign * distance, 0, last)
            where = lambda k: (k >= distance) if sign == 1 else (k + distance <= last)
            target = above if sign == 1 else below
            more = (lambda k: distance <= k < last) if sign == 1 else (lambda k: 0 < k <= last - distance)
            if distance < last:
                now = jnp.logical_and(z >= distance, z < last) if sign == 1 else jnp.logical_and(z > 0, z <= last - distance)
                action(zs, where, target, (more, now))
            else:
                action(zs, where, target, None)

    def relay(block, arrival, target, more, sem=None):
        if more is not None:
            where, now = more
            pl.when(now)(lambda: go.remote(block, block, arrival, target, sem).start())
            if sem is None:
                go.count(block, where)

    def pass_rows(distance):
        for p in range(PIECES):

            def action(zs, where, target, more):
                block = rows.at[zs, t, bit(p)]
                go.arrive(block, rows_sem.at[zs, p], where(z))
                relay(block, rows_sem.at[zs, p], target, more, relay_sem.at[0] if distance == last - 1 else None)
                go.send(block, block, rows_side_sem.at[zs], other, where)

            chain(distance, action)

    def weights_across(g):
        go.arrive(weights.at[g, pl.ds(0, depth)], w_across_sem.at[g])
        for zs in range(depth):
            block = weights.at[g, at(zs, 1 - x, c)]
            go.send(block, block, w_side_sem.at[g], sibling)

    def weights_beside(g):
        go.arrive(weights.at[g, pl.ds(0, depth * CORES)], w_side_sem.at[g])

    def normalize(zs):
        go.arrive(rows.at[zs, 1 - t], rows_side_sem.at[zs])

        def strip(i, carry):
            r = pl.ds(pl.multiple_of(i * 16, 16), 16)
            halves = [rows[zs, h, r, :].astype(jnp.float32) for h in range(2)]
            total = sum(jnp.sum(a * a, axis=1, keepdims=True) for a in halves)
            factor = lax.rsqrt(total / (2 * half_width) + eps)
            for h in range(2):
                full[zs, r, h * half_width : (h + 1) * half_width] = (
                    halves[h] * factor * gain_rows[h]
                ).astype(jnp.bfloat16)
            return carry

        lax.fori_loop(0, span // 16, strip, 0)

    lane = lax.broadcasted_iota(jnp.int32, (span, HEAD_SIZE), 1)
    line = lax.broadcasted_iota(jnp.int32, (span, HEAD_SIZE), 0)
    half = HEAD_SIZE // 2
    pair_id = jnp.where(lane < half, lane, lane - half).astype(jnp.float32)
    inverse = jnp.exp(-math.log(rope_base) * pair_id / half)

    def table(zs, carry):
        angles = (order[zs * PLANE + column] * span + line).astype(jnp.float32) * inverse
        cos_t[zs] = jnp.cos(angles)
        sine = jnp.sin(angles)
        sin_t[zs] = jnp.where(lane < half, -sine, sine)
        return carry

    lax.fori_loop(0, depth, table, 0)
    for m in range(PLANE):
        for zs in range(depth):
            i = m * depth + zs
            key_pos[:, i * span : (i + 1) * span] = order[zs * PLANE + m] * span + lax.broadcasted_iota(
                jnp.int32, (1, span), 1
            )
    for copy in own:
        copy.wait()
    gains[t] = gain[...]
    go.arrive(gains.at[1 - t], small_sem.at[0])
    for h in range(2):
        rows_of = gains[h].astype(jnp.float32)
        for i in range(half_width // HEAD_SIZE):
            gain_rows[h, :, i * HEAD_SIZE : (i + 1) * HEAD_SIZE] = rows_of[i : i + 1]
    bias_b[...] = bias_q[...].astype(jnp.float32)
    post_rows = post_gain[...].astype(jnp.float32)
    for i in range(half_width // HEAD_SIZE):
        post_out[:, i * HEAD_SIZE : (i + 1) * HEAD_SIZE] = post_rows[i : i + 1]

    pass_rows(1)
    spread(1, (0, 1, 2))
    spread(3, (0,))
    leave_columns(0)
    normalize(z)
    pass_rows(2)
    spread(2, (0, 1, 2))
    for g in (0, 1, 2):
        take_weights(g, 1)
    normalize(z + 1 - 2 * lax.rem(z, 2))
    take_weights(0, 3)
    take_weights(0, 2)
    go.left(rows.at[z, t], relay_sem.at[0], middle)
    pass_rows(3)
    spread(3, (1,))
    leave_columns(1)
    take_weights(1, 2)
    normalize(lax.rem(z + 2, depth))
    take_weights(1, 3, (1, 2))
    normalize(last - z)
    weights_across(0)
    weights_beside(0)

    tokens = depth * span

    def product(g):
        return jnp.dot(
            full[...].reshape(tokens, 2 * half_width),
            weights[g].reshape(2 * half_width, PAIR),
            preferred_element_type=jnp.float32,
        )

    cosine, sine = cos_t[...].reshape(tokens, HEAD_SIZE), sin_t[...].reshape(tokens, HEAD_SIZE)
    pair = product(0)
    keys = pair[:, :HEAD_SIZE] + bias_p[0:1, :].astype(jnp.float32)
    kvs[column, :, :HEAD_SIZE] = rotate(keys, cosine, sine).astype(jnp.bfloat16)
    kvs[column, :, HEAD_SIZE:] = (pair[:, HEAD_SIZE:] + bias_p[1:2, :].astype(jnp.float32)).astype(jnp.bfloat16)
    go.send(kvs.at[column], kvs.at[column], kv_sem.at[0], across)
    go.send(kvs.at[column], kvs.at[column], kv_sem.at[1], sibling)
    spread(3, (2,))
    take_weights(2, 2)
    take_weights(1, 3, (3,))
    take_weights(2, 3)

    scale = math.log2(math.e) / math.sqrt(HEAD_SIZE)

    def make_queries(g):
        field = product(g)
        for i in range(2):
            cut = slice(i * HEAD_SIZE, (i + 1) * HEAD_SIZE)
            head = field[:, cut] + bias_b[pl.ds(z * GROUP + (g - 1) * 2 + i, 1), :]
            turned = (rotate(head, cosine, sine) * scale).astype(jnp.bfloat16)
            queries[g - 1, :, i * span : (i + 1) * span, :] = turned.reshape(depth, span, HEAD_SIZE)

    weights_across(1)
    weights_beside(1)
    make_queries(1)
    kv_across = kvs.at[(1 - x) * CORES + c]
    go.arrive(kv_across, kv_sem.at[0])
    go.send(kv_across, kv_across, kv_sem.at[1], sibling)
    go.arrive(kvs.at[pl.ds(0, CORES)], kv_sem.at[1])

    def att_piece(g, zs, b):
        return att.at[g, zs, pl.ds(pl.multiple_of(b * span, span), span)]

    def nth(i):
        return jnp.where(i == 0, 0, jnp.where(i == 1, last, jnp.where(i == 2, 1 + c, 2 - c)))

    def attend(g, first, end):
        def turn(i, carry):
            b = nth(i)
            scores = lax.dot_general(
                queries[g, b],
                kvs[:, :, :HEAD_SIZE].reshape(PLANE * tokens, HEAD_SIZE),
                (((1,), (1,)), ((), ())),
                preferred_element_type=jnp.float32,
            )
            start = order[b * PLANE + column] * span
            query_pos = start + lax.rem(lax.broadcasted_iota(jnp.int32, (2 * span, 1), 0), span)
            scores = jnp.where(key_pos[...] <= query_pos, scores, -jnp.inf)
            peak = jnp.max(scores, axis=1, keepdims=True)
            shares = jnp.exp2(scores - peak)
            totals = jnp.sum(shares, axis=1, keepdims=True)
            summed = jnp.dot(
                shares.astype(jnp.bfloat16),
                kvs[:, :, HEAD_SIZE:].reshape(PLANE * tokens, HEAD_SIZE),
                preferred_element_type=jnp.float32,
            )
            result = (summed / totals).astype(jnp.bfloat16)
            place = pl.ds(pl.multiple_of(b * span, span), span)
            att[g, z, place, :HEAD_SIZE] = result[:span]
            att[g, z, place, HEAD_SIZE:] = result[span:]
            block = att_piece(g, z, b)
            go.remote(block, block, att_sem.at[g, z, b], (at(gatherer, x, c), t)).start()
            return carry

        lax.fori_loop(first, end, turn, 0)

    attend(0, 0, depth)

    @pl.when(middle)
    def _():
        block = outw.at[0, column]
        go.arrive(block, out_end_sem.at[0])
        go.remote(block, block, out_across_sem.at[0], across).start()
        go.remote(block, block, out_side_sem.at[0], sibling).start()

    go.count(outw.at[0, 0], inner, times=2)
    weights_across(2)
    weights_beside(2)
    make_queries(2)
    attend(1, 0, depth)
    go.count(att.at[0, 0], times=2)

    def hand_on(g, i):
        block, sem = att_piece(g, own_end, nth(i)), att_sem.at[g, own_end, nth(i)]
        go.arrive(block, sem)
        go.remote(block, block, sem, (at(last - z, x, c), t)).start()

    halves = 2
    each = PLANE // halves
    share = depth // 2

    def piece(ref, i, h):
        return ref.at[i, pl.ds(h * each, each)]

    def mix_block(e, b):
        place = pl.ds(pl.multiple_of(b * span, span), span)
        owner = own_end if e == 0 else z
        for h in range(halves):
            for m in range(h * each, (h + 1) * each):
                total = None
                for zs in range(depth):
                    for g in range(2):
                        first = zs * 2 * PAIR + g * PAIR
                        term = jnp.dot(
                            att[g, zs, place, :],
                            outw[e, m, first : first + PAIR, :],
                            preferred_element_type=jnp.float32,
                        )
                        total = term if total is None else total + term
                value = total.astype(jnp.bfloat16)

                @pl.when(b == z)
                def _():
                    terms[owner, m] = value

                @pl.when(b != z)
                def _():
                    part[e, b, m] = value

            @pl.when(b != z)
            def _():
                source = piece(part.at[e], b, h)
                go.remote(source, piece(terms, owner, h), term_sem.at[owner, h], (at(b, x, c), t)).start()

    @pl.when(middle)
    def _():
        def side_columns(e):
            block = outw.at[e, (1 - x) * CORES + c]
            go.arrive(block, out_across_sem.at[e])
            go.remote(block, block, out_side_sem.at[e], sibling).start()

        side_columns(1)
        for g in range(2):
            for i in range(depth):
                hand_on(g, i)
        go.arrive(outw.at[1, pl.ds(0, CORES)], out_side_sem.at[1])
        for i in range(depth):
            for zs in (last - z, last - own_end):
                for g in range(2):
                    go.arrive(att_piece(g, zs, nth(i)), att_sem.at[g, zs, nth(i)])
            mix_block(1, nth(i))
            if i == 1:
                side_columns(0)
        go.arrive(outw.at[0, pl.ds(0, CORES)], out_side_sem.at[0])
        for i in range(depth):
            mix_block(0, nth(i))

    go.count(outw.at[0, 0], inner, times=2)
    go.count(att.at[:, 0], inner)
    go.count(part.at[0, 0], inner, times=2 * (depth - 1))

    near = jnp.where(z < share, 0, share)
    for e in (1, 0):
        for h in range(halves):
            for first in (near, share - near):
                maker = jnp.where(first == 0, 1, last - 1)
                index = jnp.where(first == 0, e, 1 - e)
                block = piece(terms, first + index, h)
                go.arrive(block, term_sem.at[first + index, h], z != maker)
                go.send(block, piece(others, index, h), other_sem.at[index, h], other, also=t != first // share)
    go.count(others.at[0], times=share)

    width = w_out.shape[1]
    sums = jnp.zeros((span, 1), jnp.float32)
    pieces = [(j, m) for j in range(share) for m in range(PLANE)]
    for j, m in pieces:
        if m % each == 0:
            go.arrive(piece(others, j, m // each), other_sem.at[j, m // each])
        cut = slice((j * PLANE + m) * width, (j * PLANE + m + 1) * width)
        mixed = terms[t * share + j, m].astype(jnp.float32) + others[j, m].astype(jnp.float32)
        mixed_rows[:, cut] = mixed
        stream = rows[z, t, :, cut].astype(jnp.float32) + mixed
        sums = sums + jnp.sum(stream * stream, axis=1, keepdims=True)
    write = pltpu.make_async_copy(mixed_rows, mixed_out, local_sem.at[0])
    write.start()
    squares[t] = jnp.broadcast_to(sums, (span, span)).T[:8]
    go.send(squares.at[t], squares.at[t], small_sem.at[2], other, sem=small_sem.at[3])
    go.arrive(squares.at[1 - t], small_sem.at[2])
    total = (squares[0] + squares[1])[:1]
    factor_out[...] = lax.rsqrt(total / (2 * half_width) + eps)
    write.wait()
    go.left(gain, small_sem.at[1])
    go.left(squares.at[t], small_sem.at[3])
    go.finish()


def per_device_by_column(
    hidden_in,
    span_order,
    norm_gain,
    w_query,
    bias_query,
    key_value_weight,
    bias_kv,
    w_out,
    post_gain,
):
    span, half_width = hidden_in.shape
    n_seq = span_order.shape[0]
    depth = n_seq // PLANE
    slab = w_query.shape[0]
    tokens = depth * span
    vmem, hbm, smem = (pl.BlockSpec(memory_space=m) for m in (pltpu.VMEM, pl.ANY, pltpu.SMEM))
    dma = pltpu.SemaphoreType.DMA
    bf16 = lambda *shape: pltpu.VMEM(shape, jnp.bfloat16)
    f32 = lambda *shape: pltpu.VMEM(shape, jnp.float32)
    width = w_out.shape[1]
    f32_out = lambda *shape: jax.ShapeDtypeStruct(shape, jnp.float32)
    mixed, factor, post = pl.pallas_call(
        lambda *refs: column_kernel(depth, *refs),
        out_shape=(f32_out(span, half_width), f32_out(1, span), f32_out(1, half_width)),
        in_specs=[hbm, smem, vmem, vmem, vmem, hbm, vmem, hbm, hbm],
        out_specs=(hbm, vmem, vmem),
        scratch_shapes=[
            bf16(depth, 2, span, half_width),
            bf16(depth, span, 2 * half_width),
            bf16(2, half_width // HEAD_SIZE, HEAD_SIZE),
            bf16(3, n_seq, slab, PAIR),
            bf16(2, PLANE, w_out.shape[0], width),
            bf16(PLANE, tokens, PAIR),
            bf16(2, depth, 2 * span, HEAD_SIZE),
            bf16(2, depth, tokens, PAIR),
            bf16(2, depth, PLANE, span, width),
            bf16(depth, PLANE, span, width),
            bf16(depth // 2, PLANE, span, width),
            f32(2, 8, span),
            bf16(depth, slab, PAIR),
            f32(depth, span, HEAD_SIZE),
            f32(depth, span, HEAD_SIZE),
            pltpu.VMEM((1, PLANE * tokens), jnp.int32),
            f32(2, 1, half_width),
            f32(half_width // HEAD_SIZE, HEAD_SIZE),
            bf16(2, HEAD_SIZE),
            f32(span, half_width),
            bf16(5120, half_width),
            dma((5,)),
            dma((1,)),
            dma((4,)),
            dma((1,)),
            dma((depth, PIECES)),
            dma((depth,)),
            dma((3, depth)),
            dma((3,)),
            dma((3,)),
            dma((1,)),
            dma((2,)),
            dma((2,)),
            dma((2,)),
            dma((2, depth, depth)),
            dma((depth, 2)),
            dma((depth // 2, 2)),
        ],
        compiler_params=pltpu.CompilerParams(
            collective_id=0, has_side_effects=True, vmem_limit_bytes=60 * 1024 * 1024
        ),
        name="sublayer",
    )(
        hidden_in,
        span_order,
        norm_gain.reshape(-1, HEAD_SIZE),
        post_gain.reshape(-1, HEAD_SIZE),
        bias_query.reshape(-1, HEAD_SIZE),
        w_query,
        key_value_weight,
        bias_kv,
        w_out,
    )
    stream = hidden_in.astype(jnp.float32) + mixed
    normed = (stream * factor.reshape(span, 1) * post).astype(jnp.bfloat16)
    return (mixed.astype(jnp.bfloat16), normed)


def per_device(*args):
    hidden_in, span_order, w_query, kv_weight = args[0], args[1], args[3], args[5]
    n_seq = span_order.shape[0]
    n_tp = MODEL_WIDTH // hidden_in.shape[1]
    heads = w_query.shape[1] // HEAD_SIZE
    kv_heads = kv_weight.shape[2] // HEAD_SIZE
    if n_tp == 2 and n_seq == 4 * PLANE and kv_heads == 4 and heads == kv_heads * GROUP:
        return per_device_by_column(*args)
    return per_device_by_span(*args)


def solution(mesh):
    placed = (
        P("seq", "tp"),
        P(),
        P("tp"),
        P("seq", "tp"),
        P("tp"),
        P("seq", None, "tp"),
        P(None, "tp"),
        P("tp", "seq"),
        P("tp"),
    )
    return jax.shard_map(
        per_device,
        mesh=mesh,
        in_specs=placed,
        out_specs=(P("seq", "tp"), P("seq", "tp")),
        check_vma=False,
    )
```

```python
import math

import jax
import jax.numpy as jnp
from jax import lax
from jax.experimental import pallas as pl
from jax.experimental.pallas import tpu as pltpu
from jax.sharding import PartitionSpec as P

MODEL_WIDTH = 4096
HEAD_SIZE = 128
GROUP = 4


eps = 1e-06
rope_base = 1000000.0


def apply_rotary(field, token_positions):
    half = field.shape[-1] // 2
    inverse = jnp.exp(-math.log(rope_base) * jnp.arange(half, dtype=jnp.float32) / half)
    angles = token_positions.astype(jnp.float32)[:, None] * inverse[None, :]
    cosine = jnp.cos(angles)[:, None, :]
    sine = jnp.sin(angles)[:, None, :]
    first = field[..., :half]
    second = field[..., half:]
    return jnp.concatenate(
        [first * cosine - second * sine, second * cosine + first * sine], axis=-1
    )


def span_lookup(order, devices):
    table_ids = jnp.arange(order.shape[0], dtype=jnp.int32)
    return jnp.sum(jnp.where(devices[:, None] == table_ids[None, :], order[None, :], 0), axis=1)


def per_device_by_span(
    hidden_in,
    span_order,
    norm_gain,
    w_query,
    bias_query,
    key_value_weight,
    bias_kv,
    w_out,
    post_gain,
):
    tok_rows = hidden_in.shape[0]
    seq_index = lax.axis_index("seq")
    own_span = span_lookup(span_order, jnp.full((1,), seq_index, jnp.int32))[0]
    token_positions = own_span * tok_rows + jnp.arange(tok_rows, dtype=jnp.int32)
    local = hidden_in.astype(jnp.float32)
    raw_rows, gains = (
        lax.all_gather(hidden_in, "tp", axis=1, tiled=True),
        lax.all_gather(norm_gain[None, :], "tp", axis=1, tiled=True),
    )
    full_rows = raw_rows.astype(jnp.float32)
    meansq = jnp.mean(full_rows * full_rows, axis=1, keepdims=True)
    normed_in = (full_rows * lax.rsqrt(meansq + eps) * gains.astype(jnp.float32)).astype(
        jnp.bfloat16
    )
    columns = normed_in
    query_proj = jnp.dot(
        columns,
        lax.all_gather(w_query, "seq", axis=0, tiled=True),
        preferred_element_type=jnp.float32,
    )
    columns = normed_in
    pair_proj = jnp.einsum(
        "tr,rkc->tkc",
        columns,
        lax.all_gather(key_value_weight, "seq", axis=0, tiled=True),
        preferred_element_type=jnp.float32,
    )
    query_heads = w_query.shape[1] // HEAD_SIZE
    kv_heads = key_value_weight.shape[2] // HEAD_SIZE
    query_proj = query_proj + bias_query.astype(jnp.float32)[None, :]
    queries = apply_rotary(
        query_proj.reshape(tok_rows, query_heads, HEAD_SIZE), token_positions
    ).astype(jnp.bfloat16)
    pair_proj = pair_proj + bias_kv.astype(jnp.float32)[None, :, :]
    rotated_keys = apply_rotary(
        pair_proj[:, 0, :].reshape(tok_rows, kv_heads, HEAD_SIZE), token_positions
    )
    rotated_keys = rotated_keys.astype(jnp.bfloat16).reshape(tok_rows, kv_heads * HEAD_SIZE)
    value_rows = pair_proj[:, 1, :].astype(jnp.bfloat16)
    grouped = (
        queries.reshape(tok_rows, kv_heads, GROUP, HEAD_SIZE)
        .transpose(1, 2, 0, 3)
        .reshape(kv_heads, GROUP * tok_rows, HEAD_SIZE)
    )
    query_pos = jnp.tile(token_positions, GROUP)
    last_query = jnp.max(token_positions)
    scale = 1.0 / math.sqrt(HEAD_SIZE)
    start_state = (
        jnp.full((kv_heads, GROUP * tok_rows), -1e30, jnp.float32),
        jnp.zeros((kv_heads, GROUP * tok_rows), jnp.float32),
        jnp.zeros((kv_heads, GROUP * tok_rows, HEAD_SIZE), jnp.float32),
    )
    key_piece = lax.all_gather(rotated_keys, "seq", axis=0, tiled=True)
    value_piece = lax.all_gather(value_rows, "seq", axis=0, tiled=True)
    count = key_piece.shape[0]
    block = math.gcd(count, 1536)

    def visit(step, state):
        first = step * block
        key_block = lax.dynamic_slice_in_dim(key_piece, first, block, 0).reshape(
            block, kv_heads, HEAD_SIZE
        )
        value_block = lax.dynamic_slice_in_dim(value_piece, first, block, 0).reshape(
            block, kv_heads, HEAD_SIZE
        )
        row_ids = first + jnp.arange(block, dtype=jnp.int32)
        key_pos = span_lookup(span_order, row_ids // tok_rows) * tok_rows + row_ids % tok_rows

        def update(current):
            maxima, totals, sums = current
            scores = (
                jnp.einsum("kqd,nkd->kqn", grouped, key_block, preferred_element_type=jnp.float32)
                * scale
            )
            allowed = (key_pos[None, :] <= query_pos[:, None])[None, :, :]
            scores = jnp.where(allowed, scores, -1e30)
            fresh = jnp.maximum(maxima, jnp.max(scores, axis=2))
            weights = jnp.where(allowed, jnp.exp(scores - fresh[:, :, None]), 0.0)
            factor = jnp.exp(maxima - fresh)
            totals = totals * factor + jnp.sum(weights, axis=2)
            sums = sums * factor[:, :, None] + jnp.einsum(
                "kqn,nkd->kqd",
                weights.astype(jnp.bfloat16),
                value_block,
                preferred_element_type=jnp.float32,
            )
            return (fresh, totals, sums)

        return lax.cond(jnp.min(key_pos) <= last_query, update, lambda current: current, state)

    maxima, totals, sums = lax.fori_loop(0, count // block, visit, start_state)
    attended = (sums / totals[:, :, None]).astype(jnp.bfloat16)
    attended = (
        attended.reshape(kv_heads, GROUP, tok_rows, HEAD_SIZE)
        .transpose(2, 0, 1, 3)
        .reshape(tok_rows, query_heads * HEAD_SIZE)
    )
    partial_out = jnp.dot(
        attended,
        lax.all_gather(w_out, "seq", axis=1, tiled=True),
        preferred_element_type=jnp.float32,
    )
    mixed = lax.psum_scatter(
        partial_out.astype(jnp.bfloat16), "tp", scatter_dimension=1, tiled=True
    ).astype(jnp.float32)
    attn_out = mixed.astype(jnp.bfloat16)
    stream = local + mixed
    post_sq = lax.psum(jnp.sum(stream * stream, axis=1), "tp")
    normed = (
        stream
        * lax.rsqrt(post_sq / MODEL_WIDTH + eps)[:, None]
        * post_gain.astype(jnp.float32)[None, :]
    ).astype(jnp.bfloat16)
    return (attn_out, normed)


MESH = pl.DeviceIdType.MESH
CORES = 2
PLANE = 4
PIECES = 2
PAIR = 2 * HEAD_SIZE


def at(z, x, c):
    return z * PLANE + x * CORES + c


class Traffic:
    def __init__(self, depth, z, sem, proxy, peer):
        self.z, self.sem, self.proxy, self.peer = z, sem, proxy, peer
        self.rows, self.epoch = [[0] * depth, [0] * depth], 0

    def remote(self, source, landing, arrival, target, sem=None):
        return pltpu.make_async_remote_copy(
            src_ref=source,
            dst_ref=landing,
            send_sem=self.sem.at[self.epoch] if sem is None else sem,
            recv_sem=arrival,
            device_id=target,
            device_id_type=MESH,
        )

    def count(self, ref, where=None, times=1):
        size = math.prod(ref.shape) * times // self.proxy.shape[1]
        rows = self.rows[self.epoch]
        for k in range(len(rows)):
            if where is None or where(k):
                rows[k] += size

    def send(self, source, landing, arrival, target, where=None, also=None, sem=None):
        when = None if where is None else where(self.z)
        if also is not None:
            when = also if when is None else jnp.logical_and(when, also)
        guarded(when, lambda: self.remote(source, landing, arrival, target, sem).start())
        if sem is None and also is None:
            self.count(source, where)

    def arrive(self, landing, arrival, when=None):
        guarded(when, lambda: self.remote(landing, landing, arrival, self.peer).wait_recv())

    def left(self, source, sem, when=None):
        guarded(when, lambda: self.remote(source, source, sem, self.peer, sem).wait_send())

    def finish(self):
        for epoch, rows in enumerate(self.rows):
            for k, size in enumerate(rows):
                block = self.proxy.at[pl.ds(0, size)]
                self.left(block, self.sem.at[epoch], self.z == k)


def guarded(when, action):
    if when is None:
        action()
    else:
        pl.when(when)(action)


def rotate(field, cosine, sine):
    return field * cosine + pltpu.roll(field, HEAD_SIZE // 2, 1) * sine


def column_kernel(
    depth,
    hidden, order, gain, post_gain, bias_q, wq, wkv, bias_kv, w_out,
    mixed_out, factor_out, post_out,
    rows, full, gains, weights, outw, kvs, queries, att, part, terms, others, squares,
    kv_pieces, cos_t, sin_t, key_pos, gain_rows, bias_b, bias_p, early, premixed, mixed_rows, proxy,
    local_sem, send_sem, small_sem, relay_sem, rows_sem, rows_side_sem,
    w_sem, w_across_sem, w_side_sem, out_end_sem, out_across_sem, out_side_sem, kv_sem, att_sem, term_sem, other_sem,
):
    s, t = lax.axis_index("seq"), lax.axis_index("tp")
    z, x, c = s // PLANE, s % PLANE // CORES, s % CORES
    last = depth - 1
    span, half_width = hidden.shape
    slab = wq.shape[0]
    column = x * CORES + c
    sibling, across, other = (at(z, x, 1 - c), t), (at(z, 1 - x, c), t), (s, 1 - t)
    above, below = (at(jnp.minimum(z + 1, last), x, c), t), (at(jnp.maximum(z - 1, 0), x, c), t)

    barrier = pltpu.get_barrier_semaphore()
    peers = [sibling, across, other] + [(at(lax.rem(z + d, depth), x, c), t) for d in range(1, depth)]
    for peer in peers:
        pl.semaphore_signal(barrier, inc=1, device_id=peer, device_id_type=MESH)
    pl.semaphore_wait(barrier, len(peers))

    go = Traffic(depth, z, send_sem, proxy, sibling)
    edge = span // PIECES

    def bit(p):
        return pl.ds(p * edge, edge)

    go.send(gain, gains.at[t], small_sem.at[0], other, sem=small_sem.at[1])
    for p in range(PIECES):
        mine, landing = hidden.at[bit(p)], rows.at[z, t, bit(p)]
        go.send(mine, landing, rows_side_sem.at[z], other)
        go.send(mine, landing, rows_sem.at[z, p], above, lambda k: k < last)
        go.send(mine, landing, rows_sem.at[z, p], below, lambda k: k > 0)
    own = [
        pltpu.make_async_copy(hidden, rows.at[z, t], local_sem.at[0]),
        pltpu.make_async_copy(
            bias_kv.at[:, pl.ds(pl.multiple_of(z * HEAD_SIZE, HEAD_SIZE), HEAD_SIZE)], bias_p, local_sem.at[1]
        ),
        pltpu.make_async_copy(w_out, outw.at[1, column], local_sem.at[2]),
    ]

    def q_piece(g, zt):
        return wq.at[:, pl.ds(pl.multiple_of(zt * 2 * PAIR + (g - 1) * PAIR, PAIR), PAIR)]

    for g in (1, 2):
        own.append(pltpu.make_async_copy(q_piece(g, z), weights.at[g, c, s // CORES], local_sem.at[2 + g]))
    for copy in own:
        copy.start()
    for zt in range(depth):
        for i in range(2):
            kv_pieces[zt, :, i * HEAD_SIZE : (i + 1) * HEAD_SIZE] = wkv[:, i, zt * HEAD_SIZE : (zt + 1) * HEAD_SIZE]
    weights[0, c, s // CORES] = kv_pieces[z]
    for g in (0, 1, 2):
        source = kv_pieces.at[z] if g == 0 else q_piece(g, z)
        go.send(source, weights.at[g, c, s // CORES], w_across_sem.at[g], across)
        go.send(source, weights.at[g, c, s // CORES], w_side_sem.at[g], sibling)
    inner = lambda k: (k > 0) & (k < last)
    outer = lambda k: (k == 0) | (k == last)
    middle = inner(z)
    go.send(w_out, outw.at[1, column], out_across_sem.at[1], across, inner)
    go.send(w_out, outw.at[1, column], out_side_sem.at[1], sibling, inner)
    own_end = jnp.where(z < depth // 2, 0, last)
    gatherer = jnp.where(middle, last - z, jnp.where(z == 0, 1, last - 1))

    def leave_columns(part_id):
        place = pl.ds(part_id * (w_out.shape[0] // 2), w_out.shape[0] // 2)
        landing = outw.at[0, column, place]
        go.send(w_out.at[place], landing, out_end_sem.at[0], (at(gatherer, x, c), t), outer)

    def spread(stage, groups):
        for g in groups:
            for zt, where in ((stage, lambda k: k < stage), (last - stage, lambda k: k > last - stage)):
                source = kv_pieces.at[zt] if g == 0 else q_piece(g, zt)
                go.send(source, weights.at[g, c, s // CORES], w_sem.at[g, z], (at(zt, x, c), t), where)

    def take_weights(g, stage, distances=None):
        for distance in distances or range(1, stage + 1):
            for sign, goal in ((-1, stage), (1, last - stage)):
                zs = jnp.clip(z + sign * distance, 0, last)
                block = weights.at[g, c, zs * CORES + x]
                go.arrive(block, w_sem.at[g, zs], z == goal)
                go.send(block, block, w_across_sem.at[g], across, lambda k: k == goal)
                go.send(block, block, w_side_sem.at[g], sibling, lambda k: k == goal)

    def chain(distance, action):
        for sign in (1, -1):
            zs = jnp.clip(z - sign * distance, 0, last)
            where = lambda k: (k >= distance) if sign == 1 else (k + distance <= last)
            target = above if sign == 1 else below
            more = (lambda k: distance <= k < last) if sign == 1 else (lambda k: 0 < k <= last - distance)
            if distance < last:
                now = jnp.logical_and(z >= distance, z < last) if sign == 1 else jnp.logical_and(z > 0, z <= last - distance)
                action(zs, where, target, (more, now))
            else:
                action(zs, where, target, None)

    def relay(block, arrival, target, more, sem=None):
        if more is not None:
            where, now = more
            pl.when(now)(lambda: go.remote(block, block, arrival, target, sem).start())
            if sem is None:
                go.count(block, where)

    def pass_rows(distance):
        for p in range(PIECES):

            def action(zs, where, target, more):
                block = rows.at[zs, t, bit(p)]
                go.arrive(block, rows_sem.at[zs, p], where(z))
                relay(block, rows_sem.at[zs, p], target, more, relay_sem.at[0] if distance == last - 1 else None)
                go.send(block, block, rows_side_sem.at[zs], other, where)

            chain(distance, action)

    def weights_across(g):
        go.arrive(weights.at[g, c, pl.ds(0, depth)], w_across_sem.at[g])
        for zs in range(depth):
            block = weights.at[g, c, zs * CORES + 1 - x]
            go.send(block, block, w_side_sem.at[g], sibling)

    def weights_beside(g):
        go.arrive(weights.at[g, 1 - c], w_side_sem.at[g])

    def normalize(zs):
        go.arrive(rows.at[zs, 1 - t], rows_side_sem.at[zs])

        def strip(i, carry):
            r = pl.ds(pl.multiple_of(i * 16, 16), 16)
            halves = [rows[zs, h, r, :].astype(jnp.float32) for h in range(2)]
            total = sum(jnp.sum(a * a, axis=1, keepdims=True) for a in halves)
            factor = lax.rsqrt(total / (2 * half_width) + eps)
            for h in range(2):
                value = (halves[h] * factor * gain_rows[h]).astype(jnp.bfloat16)
                for i in range(half_width // slab):
                    j, core = divmod(h * (half_width // slab) + i, CORES)
                    full[core, zs, r, j * slab : (j + 1) * slab] = value[:, i * slab : (i + 1) * slab]
            return carry

        lax.fori_loop(0, span // 16, strip, 0)

    lane = lax.broadcasted_iota(jnp.int32, (span, HEAD_SIZE), 1)
    line = lax.broadcasted_iota(jnp.int32, (span, HEAD_SIZE), 0)
    half = HEAD_SIZE // 2
    pair_id = jnp.where(lane < half, lane, lane - half).astype(jnp.float32)
    inverse = jnp.exp(-math.log(rope_base) * pair_id / half)

    def table(zs, carry):
        angles = (order[zs * PLANE + column] * span + line).astype(jnp.float32) * inverse
        cos_t[zs] = jnp.cos(angles)
        sine = jnp.sin(angles)
        sin_t[zs] = jnp.where(lane < half, -sine, sine)
        return carry

    lax.fori_loop(0, depth, table, 0)
    for m in range(PLANE):
        for zs in range(depth):
            i = m * depth + zs
            key_pos[:, i * span : (i + 1) * span] = order[zs * PLANE + m] * span + lax.broadcasted_iota(
                jnp.int32, (1, span), 1
            )
    for copy in own:
        copy.wait()
    gains[t] = gain[...]
    go.arrive(gains.at[1 - t], small_sem.at[0])
    for h in range(2):
        rows_of = gains[h].astype(jnp.float32)
        for i in range(half_width // HEAD_SIZE):
            gain_rows[h, :, i * HEAD_SIZE : (i + 1) * HEAD_SIZE] = rows_of[i : i + 1]
    bias_b[...] = bias_q[...].astype(jnp.float32)
    post_rows = post_gain[...].astype(jnp.float32)
    for i in range(half_width // HEAD_SIZE):
        post_out[:, i * HEAD_SIZE : (i + 1) * HEAD_SIZE] = post_rows[i : i + 1]

    pass_rows(1)
    spread(1, (0, 1, 2))
    spread(3, (0,))
    leave_columns(0)
    normalize(z)
    pass_rows(2)
    spread(2, (0, 1, 2))
    for g in (0, 1, 2):
        take_weights(g, 1)
    normalize(z + 1 - 2 * lax.rem(z, 2))
    take_weights(0, 3)
    take_weights(0, 2)
    go.left(rows.at[z, t], relay_sem.at[0], middle)
    pass_rows(3)
    spread(3, (1,))
    leave_columns(1)
    take_weights(1, 2)
    normalize(lax.rem(z + 2, depth))
    take_weights(1, 3, (1, 2))
    normalize(last - z)
    weights_across(0)

    tokens = depth * span

    def kv_block(i):
        return kvs.at[i]

    def product(g, core):
        return jnp.dot(
            full[core].reshape(tokens, half_width),
            weights[g, core].reshape(half_width, PAIR),
            preferred_element_type=jnp.float32,
        )

    def whole_product(g):
        early[...] = product(g, c)
        weights_beside(g)
        return early[...] + product(g, 1 - c)

    cosine, sine = cos_t[...].reshape(tokens, HEAD_SIZE), sin_t[...].reshape(tokens, HEAD_SIZE)
    pair = whole_product(0)
    keys = pair[:, :HEAD_SIZE] + bias_p[0:1, :].astype(jnp.float32)
    kvs[column, :, :HEAD_SIZE] = rotate(keys, cosine, sine).astype(jnp.bfloat16)
    kvs[column, :, HEAD_SIZE:] = (pair[:, HEAD_SIZE:] + bias_p[1:2, :].astype(jnp.float32)).astype(jnp.bfloat16)
    go.send(kv_block(column), kv_block(column), kv_sem.at[0], across)
    go.send(kv_block(column), kv_block(column), kv_sem.at[1], sibling)
    spread(3, (2,))
    take_weights(2, 2)
    take_weights(1, 3, (3,))
    take_weights(2, 3)

    go.epoch = 1
    scale = math.log2(math.e) / math.sqrt(HEAD_SIZE)

    def make_queries(g):
        field = whole_product(g)
        for i in range(2):
            cut = slice(i * HEAD_SIZE, (i + 1) * HEAD_SIZE)
            head = field[:, cut] + bias_b[pl.ds(z * GROUP + (g - 1) * 2 + i, 1), :]
            turned = (rotate(head, cosine, sine) * scale).astype(jnp.bfloat16)
            queries[g - 1, :, i * span : (i + 1) * span, :] = turned.reshape(depth, span, HEAD_SIZE)

    weights_across(1)
    make_queries(1)
    kv_across = kv_block((1 - x) * CORES + c)
    go.arrive(kv_across, kv_sem.at[0])
    go.send(kv_across, kv_across, kv_sem.at[1], sibling)
    go.arrive(kvs.at[pl.ds(0, CORES)], kv_sem.at[1])

    def att_piece(g, zs, b):
        return att.at[g, zs, pl.ds(pl.multiple_of(b * span, span), span)]

    def nth(i):
        return jnp.where(i == 0, 0, jnp.where(i == 1, last, jnp.where(i == 2, 1 + c, 2 - c)))

    def attend(g, first, end):
        def turn(i, carry):
            b = nth(i)
            scores = lax.dot_general(
                queries[g, b],
                kvs[:, :, :HEAD_SIZE].reshape(PLANE * tokens, HEAD_SIZE),
                (((1,), (1,)), ((), ())),
                preferred_element_type=jnp.float32,
            )
            start = order[b * PLANE + column] * span
            query_pos = start + lax.rem(lax.broadcasted_iota(jnp.int32, (2 * span, 1), 0), span)
            scores = jnp.where(key_pos[...] <= query_pos, scores, -jnp.inf)
            peak = jnp.max(scores, axis=1, keepdims=True)
            shares = jnp.exp2(scores - peak)
            totals = jnp.sum(shares, axis=1, keepdims=True)
            summed = jnp.dot(
                shares.astype(jnp.bfloat16),
                kvs[:, :, HEAD_SIZE:].reshape(PLANE * tokens, HEAD_SIZE),
                preferred_element_type=jnp.float32,
            )
            result = (summed / totals).astype(jnp.bfloat16)
            place = pl.ds(pl.multiple_of(b * span, span), span)
            att[g, z, place, :HEAD_SIZE] = result[:span]
            att[g, z, place, HEAD_SIZE:] = result[span:]
            block = att_piece(g, z, b)
            go.remote(block, block, att_sem.at[g, z, b], (at(gatherer, x, c), t)).start()
            return carry

        lax.fori_loop(first, end, turn, 0)

    attend(0, 0, depth)

    @pl.when(middle)
    def _():
        block = outw.at[0, column]
        go.arrive(block, out_end_sem.at[0])
        go.remote(block, block, out_across_sem.at[0], across).start()
        go.remote(block, block, out_side_sem.at[0], sibling).start()

    go.count(outw.at[0, 0], inner, times=2)
    weights_across(2)
    make_queries(2)
    attend(1, 0, depth)
    go.count(att.at[0, 0], times=2)

    def hand_on(g, i):
        block, sem = att_piece(g, own_end, nth(i)), att_sem.at[g, own_end, nth(i)]
        go.arrive(block, sem)
        go.remote(block, block, sem, (at(last - z, x, c), t)).start()

    halves = PLANE
    each = PLANE // halves
    share = depth // 2

    def piece(ref, i, h):
        return ref.at[i, pl.ds(h * each, each)]

    def term(e, m, g, zs, place):
        first = zs * 2 * PAIR + g * PAIR
        return jnp.dot(att[g, zs, place, :], outw[e, m, first : first + PAIR, :], preferred_element_type=jnp.float32)

    def premix():
        for m in range(PLANE):
            premixed[m] = sum(term(1, m, g, zs, slice(None)) for zs in range(1, last) for g in range(2))

    def mix_block(e, b):
        place = pl.ds(pl.multiple_of(b * span, span), span)
        owner = own_end if e == 0 else z
        for h in range(halves):
            for m in range(h * each, (h + 1) * each):
                total = sum(term(e, m, g, zs, place) for zs in ((0, last) if e else range(depth)) for g in range(2))
                if e:
                    total = total + premixed[m, place, :]
                value = total.astype(jnp.bfloat16)

                @pl.when(b == z)
                def _():
                    terms[owner, m] = value

                @pl.when(b != z)
                def _():
                    part[e, b, m] = value

            @pl.when(b != z)
            def _():
                source = piece(part.at[e], b, h)
                go.remote(source, piece(terms, owner, h), term_sem.at[owner, h], (at(b, x, c), t)).start()

    @pl.when(middle)
    def _():
        def side_columns(e):
            block = outw.at[e, (1 - x) * CORES + c]
            go.arrive(block, out_across_sem.at[e])
            go.remote(block, block, out_side_sem.at[e], sibling).start()

        side_columns(1)
        for i in range(depth):
            hand_on(0, i)
        go.arrive(outw.at[1, pl.ds(0, CORES)], out_side_sem.at[1])
        for i in range(depth):
            for g in range(2):
                go.arrive(att_piece(g, last - z, nth(i)), att_sem.at[g, last - z, nth(i)])
        premix()

        def mix_own(i):
            for g in range(2):
                go.arrive(att_piece(g, last - own_end, nth(i)), att_sem.at[g, last - own_end, nth(i)])
            mix_block(1, nth(i))

        for i in range(depth - 1):
            hand_on(1, i)
        mix_own(0)
        hand_on(1, depth - 1)
        mix_own(1)
        side_columns(0)
        mix_own(2)
        go.arrive(outw.at[0, pl.ds(0, CORES)], out_side_sem.at[0])
        for i in range(depth - 1):
            mix_block(0, nth(i))
        mix_own(depth - 1)
        mix_block(0, nth(depth - 1))

    go.count(outw.at[0, 0], inner, times=2)
    go.count(att.at[:, 0], inner)
    go.count(part.at[0, 0], inner, times=2 * (depth - 1))

    near = jnp.where(z < share, 0, share)
    for e in (1, 0):
        for h in range(halves):
            for first in (near, share - near):
                maker = jnp.where(first == 0, 1, last - 1)
                index = jnp.where(first == 0, e, 1 - e)
                block = piece(terms, first + index, h)
                go.arrive(block, term_sem.at[first + index, h], z != maker)
                go.send(block, piece(others, index, h), other_sem.at[index, h], other, also=t != first // share)
    go.count(others.at[0], times=share)

    width = w_out.shape[1]
    sums = jnp.zeros((span, 1), jnp.float32)
    pieces = [(j, m) for j in range(share) for m in range(PLANE)]
    for j, m in pieces:
        if m % each == 0:
            go.arrive(piece(others, j, m // each), other_sem.at[j, m // each])
        cut = slice((j * PLANE + m) * width, (j * PLANE + m + 1) * width)
        mixed = terms[t * share + j, m].astype(jnp.float32) + others[j, m].astype(jnp.float32)
        mixed_rows[:, cut] = mixed
        stream = rows[z, t, :, cut].astype(jnp.float32) + mixed
        sums = sums + jnp.sum(stream * stream, axis=1, keepdims=True)
    write = pltpu.make_async_copy(mixed_rows, mixed_out, local_sem.at[0])
    write.start()
    squares[t] = jnp.broadcast_to(sums, (span, span)).T[:8]
    go.send(squares.at[t], squares.at[t], small_sem.at[2], other, sem=small_sem.at[3])
    go.arrive(squares.at[1 - t], small_sem.at[2])
    total = (squares[0] + squares[1])[:1]
    factor_out[...] = lax.rsqrt(total / (2 * half_width) + eps)
    write.wait()
    go.left(gain, small_sem.at[1])
    go.left(squares.at[t], small_sem.at[3])
    go.finish()


def per_device_by_column(
    hidden_in,
    span_order,
    norm_gain,
    w_query,
    bias_query,
    key_value_weight,
    bias_kv,
    w_out,
    post_gain,
):
    span, half_width = hidden_in.shape
    n_seq = span_order.shape[0]
    depth = n_seq // PLANE
    slab = w_query.shape[0]
    tokens = depth * span
    vmem, hbm, smem = (pl.BlockSpec(memory_space=m) for m in (pltpu.VMEM, pl.ANY, pltpu.SMEM))
    dma = pltpu.SemaphoreType.DMA
    bf16 = lambda *shape: pltpu.VMEM(shape, jnp.bfloat16)
    f32 = lambda *shape: pltpu.VMEM(shape, jnp.float32)
    width = w_out.shape[1]
    f32_out = lambda *shape: jax.ShapeDtypeStruct(shape, jnp.float32)
    mixed, factor, post = pl.pallas_call(
        lambda *refs: column_kernel(depth, *refs),
        out_shape=(f32_out(span, half_width), f32_out(1, span), f32_out(1, half_width)),
        in_specs=[hbm, smem, vmem, vmem, vmem, hbm, vmem, hbm, hbm],
        out_specs=(hbm, vmem, vmem),
        scratch_shapes=[
            bf16(depth, 2, span, half_width),
            bf16(CORES, depth, span, half_width),
            bf16(2, half_width // HEAD_SIZE, HEAD_SIZE),
            bf16(3, CORES, n_seq // CORES, slab, PAIR),
            bf16(2, PLANE, w_out.shape[0], width),
            bf16(PLANE, tokens, PAIR),
            bf16(2, depth, 2 * span, HEAD_SIZE),
            bf16(2, depth, tokens, PAIR),
            bf16(2, depth, PLANE, span, width),
            bf16(depth, PLANE, span, width),
            bf16(depth // 2, PLANE, span, width),
            f32(2, 8, span),
            bf16(depth, slab, PAIR),
            f32(depth, span, HEAD_SIZE),
            f32(depth, span, HEAD_SIZE),
            pltpu.VMEM((1, PLANE * tokens), jnp.int32),
            f32(2, 1, half_width),
            f32(half_width // HEAD_SIZE, HEAD_SIZE),
            bf16(2, HEAD_SIZE),
            f32(tokens, PAIR),
            f32(PLANE, tokens, width),
            f32(span, half_width),
            bf16(3072, half_width),
            dma((5,)),
            dma((2,)),
            dma((4,)),
            dma((1,)),
            dma((depth, PIECES)),
            dma((depth,)),
            dma((3, depth)),
            dma((3,)),
            dma((3,)),
            dma((1,)),
            dma((2,)),
            dma((2,)),
            dma((2,)),
            dma((2, depth, depth)),
            dma((depth, PLANE)),
            dma((depth // 2, PLANE)),
        ],
        compiler_params=pltpu.CompilerParams(
            collective_id=0, has_side_effects=True, vmem_limit_bytes=60 * 1024 * 1024
        ),
        name="sublayer",
    )(
        hidden_in,
        span_order,
        norm_gain.reshape(-1, HEAD_SIZE),
        post_gain.reshape(-1, HEAD_SIZE),
        bias_query.reshape(-1, HEAD_SIZE),
        w_query,
        key_value_weight,
        bias_kv,
        w_out,
    )
    stream = hidden_in.astype(jnp.float32) + mixed
    normed = (stream * factor.reshape(span, 1) * post).astype(jnp.bfloat16)
    return (mixed.astype(jnp.bfloat16), normed)


def per_device(*args):
    hidden_in, span_order, w_query, kv_weight = args[0], args[1], args[3], args[5]
    n_seq = span_order.shape[0]
    n_tp = MODEL_WIDTH // hidden_in.shape[1]
    heads = w_query.shape[1] // HEAD_SIZE
    kv_heads = kv_weight.shape[2] // HEAD_SIZE
    if n_tp == 2 and n_seq == 4 * PLANE and kv_heads == 4 and heads == kv_heads * GROUP:
        return per_device_by_column(*args)
    return per_device_by_span(*args)


def solution(mesh):
    placed = (
        P("seq", "tp"),
        P(),
        P("tp"),
        P("seq", "tp"),
        P("tp"),
        P("seq", None, "tp"),
        P(None, "tp"),
        P("tp", "seq"),
        P("tp"),
    )
    return jax.shard_map(
        per_device,
        mesh=mesh,
        in_specs=placed,
        out_specs=(P("seq", "tp"), P("seq", "tp")),
        check_vma=False,
    )
```

```python
import math

import jax
import jax.numpy as jnp
from jax import lax
from jax.experimental import pallas as pl
from jax.experimental.pallas import tpu as pltpu
from jax.sharding import PartitionSpec as P

MODEL_WIDTH = 4096
HEAD_SIZE = 128
GROUP = 4


eps = 1e-06
rope_base = 1000000.0


def apply_rotary(field, token_positions):
    half = field.shape[-1] // 2
    inverse = jnp.exp(-math.log(rope_base) * jnp.arange(half, dtype=jnp.float32) / half)
    angles = token_positions.astype(jnp.float32)[:, None] * inverse[None, :]
    cosine = jnp.cos(angles)[:, None, :]
    sine = jnp.sin(angles)[:, None, :]
    first = field[..., :half]
    second = field[..., half:]
    return jnp.concatenate(
        [first * cosine - second * sine, second * cosine + first * sine], axis=-1
    )


def span_lookup(order, devices):
    table_ids = jnp.arange(order.shape[0], dtype=jnp.int32)
    return jnp.sum(jnp.where(devices[:, None] == table_ids[None, :], order[None, :], 0), axis=1)


def per_device_by_span(
    hidden_in,
    span_order,
    norm_gain,
    w_query,
    bias_query,
    key_value_weight,
    bias_kv,
    w_out,
    post_gain,
):
    tok_rows = hidden_in.shape[0]
    seq_index = lax.axis_index("seq")
    own_span = span_lookup(span_order, jnp.full((1,), seq_index, jnp.int32))[0]
    token_positions = own_span * tok_rows + jnp.arange(tok_rows, dtype=jnp.int32)
    local = hidden_in.astype(jnp.float32)
    raw_rows, gains = (
        lax.all_gather(hidden_in, "tp", axis=1, tiled=True),
        lax.all_gather(norm_gain[None, :], "tp", axis=1, tiled=True),
    )
    full_rows = raw_rows.astype(jnp.float32)
    meansq = jnp.mean(full_rows * full_rows, axis=1, keepdims=True)
    normed_in = (full_rows * lax.rsqrt(meansq + eps) * gains.astype(jnp.float32)).astype(
        jnp.bfloat16
    )
    columns = normed_in
    query_proj = jnp.dot(
        columns,
        lax.all_gather(w_query, "seq", axis=0, tiled=True),
        preferred_element_type=jnp.float32,
    )
    columns = normed_in
    pair_proj = jnp.einsum(
        "tr,rkc->tkc",
        columns,
        lax.all_gather(key_value_weight, "seq", axis=0, tiled=True),
        preferred_element_type=jnp.float32,
    )
    query_heads = w_query.shape[1] // HEAD_SIZE
    kv_heads = key_value_weight.shape[2] // HEAD_SIZE
    query_proj = query_proj + bias_query.astype(jnp.float32)[None, :]
    queries = apply_rotary(
        query_proj.reshape(tok_rows, query_heads, HEAD_SIZE), token_positions
    ).astype(jnp.bfloat16)
    pair_proj = pair_proj + bias_kv.astype(jnp.float32)[None, :, :]
    rotated_keys = apply_rotary(
        pair_proj[:, 0, :].reshape(tok_rows, kv_heads, HEAD_SIZE), token_positions
    )
    rotated_keys = rotated_keys.astype(jnp.bfloat16).reshape(tok_rows, kv_heads * HEAD_SIZE)
    value_rows = pair_proj[:, 1, :].astype(jnp.bfloat16)
    grouped = (
        queries.reshape(tok_rows, kv_heads, GROUP, HEAD_SIZE)
        .transpose(1, 2, 0, 3)
        .reshape(kv_heads, GROUP * tok_rows, HEAD_SIZE)
    )
    query_pos = jnp.tile(token_positions, GROUP)
    last_query = jnp.max(token_positions)
    scale = 1.0 / math.sqrt(HEAD_SIZE)
    start_state = (
        jnp.full((kv_heads, GROUP * tok_rows), -1e30, jnp.float32),
        jnp.zeros((kv_heads, GROUP * tok_rows), jnp.float32),
        jnp.zeros((kv_heads, GROUP * tok_rows, HEAD_SIZE), jnp.float32),
    )
    key_piece = lax.all_gather(rotated_keys, "seq", axis=0, tiled=True)
    value_piece = lax.all_gather(value_rows, "seq", axis=0, tiled=True)
    count = key_piece.shape[0]
    block = math.gcd(count, 1536)

    def visit(step, state):
        first = step * block
        key_block = lax.dynamic_slice_in_dim(key_piece, first, block, 0).reshape(
            block, kv_heads, HEAD_SIZE
        )
        value_block = lax.dynamic_slice_in_dim(value_piece, first, block, 0).reshape(
            block, kv_heads, HEAD_SIZE
        )
        row_ids = first + jnp.arange(block, dtype=jnp.int32)
        key_pos = span_lookup(span_order, row_ids // tok_rows) * tok_rows + row_ids % tok_rows

        def update(current):
            maxima, totals, sums = current
            scores = (
                jnp.einsum("kqd,nkd->kqn", grouped, key_block, preferred_element_type=jnp.float32)
                * scale
            )
            allowed = (key_pos[None, :] <= query_pos[:, None])[None, :, :]
            scores = jnp.where(allowed, scores, -1e30)
            fresh = jnp.maximum(maxima, jnp.max(scores, axis=2))
            weights = jnp.where(allowed, jnp.exp(scores - fresh[:, :, None]), 0.0)
            factor = jnp.exp(maxima - fresh)
            totals = totals * factor + jnp.sum(weights, axis=2)
            sums = sums * factor[:, :, None] + jnp.einsum(
                "kqn,nkd->kqd",
                weights.astype(jnp.bfloat16),
                value_block,
                preferred_element_type=jnp.float32,
            )
            return (fresh, totals, sums)

        return lax.cond(jnp.min(key_pos) <= last_query, update, lambda current: current, state)

    maxima, totals, sums = lax.fori_loop(0, count // block, visit, start_state)
    attended = (sums / totals[:, :, None]).astype(jnp.bfloat16)
    attended = (
        attended.reshape(kv_heads, GROUP, tok_rows, HEAD_SIZE)
        .transpose(2, 0, 1, 3)
        .reshape(tok_rows, query_heads * HEAD_SIZE)
    )
    partial_out = jnp.dot(
        attended,
        lax.all_gather(w_out, "seq", axis=1, tiled=True),
        preferred_element_type=jnp.float32,
    )
    mixed = lax.psum_scatter(
        partial_out.astype(jnp.bfloat16), "tp", scatter_dimension=1, tiled=True
    ).astype(jnp.float32)
    attn_out = mixed.astype(jnp.bfloat16)
    stream = local + mixed
    post_sq = lax.psum(jnp.sum(stream * stream, axis=1), "tp")
    normed = (
        stream
        * lax.rsqrt(post_sq / MODEL_WIDTH + eps)[:, None]
        * post_gain.astype(jnp.float32)[None, :]
    ).astype(jnp.bfloat16)
    return (attn_out, normed)


MESH = pl.DeviceIdType.MESH
CORES = 2
PLANE = 4
PIECES = 2
PAIR = 2 * HEAD_SIZE


def at(z, x, c):
    return z * PLANE + x * CORES + c


class Traffic:
    def __init__(self, depth, z, sem, proxy, peer):
        self.z, self.sem, self.proxy, self.peer = z, sem, proxy, peer
        self.rows, self.epoch = [[0] * depth, [0] * depth], 0

    def remote(self, source, landing, arrival, target, sem=None):
        return pltpu.make_async_remote_copy(
            src_ref=source,
            dst_ref=landing,
            send_sem=self.sem.at[self.epoch] if sem is None else sem,
            recv_sem=arrival,
            device_id=target,
            device_id_type=MESH,
        )

    def count(self, ref, where=None, times=1):
        size = math.prod(ref.shape) * times // self.proxy.shape[1]
        rows = self.rows[self.epoch]
        for k in range(len(rows)):
            if where is None or where(k):
                rows[k] += size

    def send(self, source, landing, arrival, target, where=None, also=None, sem=None):
        when = None if where is None else where(self.z)
        if also is not None:
            when = also if when is None else jnp.logical_and(when, also)
        guarded(when, lambda: self.remote(source, landing, arrival, target, sem).start())
        if sem is None and also is None:
            self.count(source, where)

    def arrive(self, landing, arrival, when=None):
        guarded(when, lambda: self.remote(landing, landing, arrival, self.peer).wait_recv())

    def left(self, source, sem, when=None):
        guarded(when, lambda: self.remote(source, source, sem, self.peer, sem).wait_send())

    def finish(self):
        for epoch, rows in enumerate(self.rows):
            for k, size in enumerate(rows):
                block = self.proxy.at[pl.ds(0, size)]
                self.left(block, self.sem.at[epoch], self.z == k)


def guarded(when, action):
    if when is None:
        action()
    else:
        pl.when(when)(action)


def rotate(field, cosine, sine):
    return field * cosine + pltpu.roll(field, HEAD_SIZE // 2, 1) * sine


def column_kernel(
    depth,
    hidden, order, gain, post_gain, bias_q, wq, wkv, bias_kv, w_out,
    mixed_out, factor_out, post_out,
    rows, full, gains, weights, outw, kvs, queries, att, part, terms, others, squares,
    kv_pieces, cos_t, sin_t, key_pos, gain_rows, bias_b, bias_p, early, premixed, mixed_rows, proxy,
    local_sem, send_sem, small_sem, relay_sem, rows_sem, rows_side_sem,
    w_sem, w_across_sem, w_side_sem, out_end_sem, out_across_sem, out_side_sem, kv_sem, att_sem, term_sem, other_sem, cross_sem,
):
    s, t = lax.axis_index("seq"), lax.axis_index("tp")
    z, x, c = s // PLANE, s % PLANE // CORES, s % CORES
    last = depth - 1
    span, half_width = hidden.shape
    slab = wq.shape[0]
    column = x * CORES + c
    sibling, across, other = (at(z, x, 1 - c), t), (at(z, 1 - x, c), t), (s, 1 - t)
    above, below = (at(jnp.minimum(z + 1, last), x, c), t), (at(jnp.maximum(z - 1, 0), x, c), t)

    barrier = pltpu.get_barrier_semaphore()
    peers = [sibling, across, other] + [(at(lax.rem(z + d, depth), x, c), t) for d in range(1, depth)]
    peers += [(at(lax.rem(z + d, depth), x, c), 1 - t) for d in range(1, depth)]
    for peer in peers:
        pl.semaphore_signal(barrier, inc=1, device_id=peer, device_id_type=MESH)
    pl.semaphore_wait(barrier, len(peers))

    go = Traffic(depth, z, send_sem, proxy, sibling)
    edge = span // PIECES

    def bit(p):
        return pl.ds(p * edge, edge)

    go.send(gain, gains.at[t], small_sem.at[0], other, sem=small_sem.at[1])
    for p in range(PIECES):
        mine, landing = hidden.at[bit(p)], rows.at[z, t, bit(p)]
        go.send(mine, landing, rows_side_sem.at[z], other)
        go.send(mine, landing, rows_sem.at[z, p], above, lambda k: k < last)
        go.send(mine, landing, rows_sem.at[z, p], below, lambda k: k > 0)
    own = [
        pltpu.make_async_copy(hidden, rows.at[z, t], local_sem.at[0]),
        pltpu.make_async_copy(
            bias_kv.at[:, pl.ds(pl.multiple_of(z * HEAD_SIZE, HEAD_SIZE), HEAD_SIZE)], bias_p, local_sem.at[1]
        ),
        pltpu.make_async_copy(w_out, outw.at[1, column], local_sem.at[2]),
    ]

    def q_piece(g, zt):
        return wq.at[:, pl.ds(pl.multiple_of(zt * 2 * PAIR + (g - 1) * PAIR, PAIR), PAIR)]

    for g in (1, 2):
        own.append(pltpu.make_async_copy(q_piece(g, z), weights.at[g, c, s // CORES], local_sem.at[2 + g]))
    for copy in own:
        copy.start()
    for zt in range(depth):
        for i in range(2):
            kv_pieces[zt, :, i * HEAD_SIZE : (i + 1) * HEAD_SIZE] = wkv[:, i, zt * HEAD_SIZE : (zt + 1) * HEAD_SIZE]
    weights[0, c, s // CORES] = kv_pieces[z]
    for g in (0, 1, 2):
        source = kv_pieces.at[z] if g == 0 else q_piece(g, z)
        go.send(source, weights.at[g, c, s // CORES], w_across_sem.at[g], across)
        go.send(source, weights.at[g, c, s // CORES], w_side_sem.at[g], sibling)
    inner = lambda k: (k > 0) & (k < last)
    outer = lambda k: (k == 0) | (k == last)
    middle = inner(z)
    go.send(w_out, outw.at[1, column], out_across_sem.at[1], across, inner)
    go.send(w_out, outw.at[1, column], out_side_sem.at[1], sibling, inner)
    own_end = jnp.where(z < depth // 2, 0, last)
    gatherer = jnp.where(middle, last - z, jnp.where(z == 0, 1, last - 1))

    def leave_columns(part_id):
        place = pl.ds(part_id * (w_out.shape[0] // 2), w_out.shape[0] // 2)
        landing = outw.at[0, column, place]
        go.send(w_out.at[place], landing, out_end_sem.at[0], (at(gatherer, x, c), t), outer)

    def spread(stage, groups, least=1):
        for g in groups:
            for zt, where in (
                (stage, lambda k: k <= stage - least),
                (last - stage, lambda k: k >= last - stage + least),
            ):
                source = kv_pieces.at[zt] if g == 0 else q_piece(g, zt)
                go.send(source, weights.at[g, c, s // CORES], w_sem.at[g, z], (at(zt, x, c), t), where)

    def spread_near(stage, g):
        for zt, source in ((stage, stage - 1), (last - stage, last - stage + 1)):
            go.send(q_piece(g, zt), weights.at[g, c, s // CORES], w_sem.at[g, z], (at(zt, x, c), t), lambda k: k == source)

    def take_weights(g, stage, distances=None):
        for distance in distances or range(1, stage + 1):
            for sign, goal in ((-1, stage), (1, last - stage)):
                zs = jnp.clip(z + sign * distance, 0, last)
                block = weights.at[g, c, zs * CORES + x]
                go.arrive(block, w_sem.at[g, zs], z == goal)
                go.send(block, block, w_across_sem.at[g], across, lambda k: k == goal)
                go.send(block, block, w_side_sem.at[g], sibling, lambda k: k == goal)

    def chain(distance, action):
        for sign in (1, -1):
            zs = jnp.clip(z - sign * distance, 0, last)
            where = lambda k: (k >= distance) if sign == 1 else (k + distance <= last)
            target = above if sign == 1 else below
            more = (lambda k: distance <= k < last) if sign == 1 else (lambda k: 0 < k <= last - distance)
            if distance < last:
                now = jnp.logical_and(z >= distance, z < last) if sign == 1 else jnp.logical_and(z > 0, z <= last - distance)
                action(zs, where, target, (more, now))
            else:
                action(zs, where, target, None)

    def relay(block, arrival, target, more, sem=None):
        if more is not None:
            where, now = more
            pl.when(now)(lambda: go.remote(block, block, arrival, target, sem).start())
            if sem is None:
                go.count(block, where)

    def pass_rows(distance):
        for p in range(PIECES):

            def action(zs, where, target, more):
                block = rows.at[zs, t, bit(p)]
                go.arrive(block, rows_sem.at[zs, p], where(z))
                relay(block, rows_sem.at[zs, p], target, more, relay_sem.at[0] if distance == last - 1 else None)
                go.send(block, block, rows_side_sem.at[zs], other, where)

            chain(distance, action)

    def weights_across(g):
        go.arrive(weights.at[g, c, pl.ds(0, depth)], w_across_sem.at[g])
        for zs in range(depth):
            block = weights.at[g, c, zs * CORES + 1 - x]
            go.send(block, block, w_side_sem.at[g], sibling)

    def weights_beside(g):
        go.arrive(weights.at[g, 1 - c], w_side_sem.at[g])

    def normalize(zs):
        go.arrive(rows.at[zs, 1 - t], rows_side_sem.at[zs])

        def strip(i, carry):
            r = pl.ds(pl.multiple_of(i * 16, 16), 16)
            halves = [rows[zs, h, r, :].astype(jnp.float32) for h in range(2)]
            total = sum(jnp.sum(a * a, axis=1, keepdims=True) for a in halves)
            factor = lax.rsqrt(total / (2 * half_width) + eps)
            for h in range(2):
                value = (halves[h] * factor * gain_rows[h]).astype(jnp.bfloat16)
                for i in range(half_width // slab):
                    j, core = divmod(h * (half_width // slab) + i, CORES)
                    full[core, zs, r, j * slab : (j + 1) * slab] = value[:, i * slab : (i + 1) * slab]
            return carry

        lax.fori_loop(0, span // 16, strip, 0)

    lane = lax.broadcasted_iota(jnp.int32, (span, HEAD_SIZE), 1)
    line = lax.broadcasted_iota(jnp.int32, (span, HEAD_SIZE), 0)
    half = HEAD_SIZE // 2
    pair_id = jnp.where(lane < half, lane, lane - half).astype(jnp.float32)
    inverse = jnp.exp(-math.log(rope_base) * pair_id / half)

    def table(zs, carry):
        angles = (order[zs * PLANE + column] * span + line).astype(jnp.float32) * inverse
        cos_t[zs] = jnp.cos(angles)
        sine = jnp.sin(angles)
        sin_t[zs] = jnp.where(lane < half, -sine, sine)
        return carry

    lax.fori_loop(0, depth, table, 0)
    for m in range(PLANE):
        for zs in range(depth):
            i = m * depth + zs
            key_pos[:, i * span : (i + 1) * span] = order[zs * PLANE + m] * span + lax.broadcasted_iota(
                jnp.int32, (1, span), 1
            )
    for copy in own:
        copy.wait()
    gains[t] = gain[...]
    go.arrive(gains.at[1 - t], small_sem.at[0])
    for h in range(2):
        rows_of = gains[h].astype(jnp.float32)
        for i in range(half_width // HEAD_SIZE):
            gain_rows[h, :, i * HEAD_SIZE : (i + 1) * HEAD_SIZE] = rows_of[i : i + 1]
    bias_b[...] = bias_q[...].astype(jnp.float32)
    post_rows = post_gain[...].astype(jnp.float32)
    for i in range(half_width // HEAD_SIZE):
        post_out[:, i * HEAD_SIZE : (i + 1) * HEAD_SIZE] = post_rows[i : i + 1]

    pass_rows(1)
    spread(1, (0, 1, 2))
    spread(3, (0,))
    spread_near(3, 1)
    leave_columns(0)
    normalize(z)
    pass_rows(2)
    spread(2, (0, 1, 2))
    for g in (0, 1, 2):
        take_weights(g, 1)
    normalize(z + 1 - 2 * lax.rem(z, 2))
    take_weights(0, 3)
    take_weights(1, 3, (1,))
    take_weights(0, 2)
    go.left(rows.at[z, t], relay_sem.at[0], middle)
    pass_rows(3)
    spread(3, (1,), 2)
    leave_columns(1)
    take_weights(1, 2)
    normalize(lax.rem(z + 2, depth))
    take_weights(1, 3, (2, 3))
    normalize(last - z)
    weights_across(0)

    tokens = depth * span

    def kv_block(i):
        return kvs.at[i]

    def product(g, core):
        return jnp.dot(
            full[core].reshape(tokens, half_width),
            weights[g, core].reshape(half_width, PAIR),
            preferred_element_type=jnp.float32,
        )

    def whole_product(g):
        early[...] = product(g, c)
        weights_beside(g)
        return early[...] + product(g, 1 - c)

    cosine, sine = cos_t[...].reshape(tokens, HEAD_SIZE), sin_t[...].reshape(tokens, HEAD_SIZE)
    pair = whole_product(0)
    keys = pair[:, :HEAD_SIZE] + bias_p[0:1, :].astype(jnp.float32)
    kvs[column, :, :HEAD_SIZE] = rotate(keys, cosine, sine).astype(jnp.bfloat16)
    kvs[column, :, HEAD_SIZE:] = (pair[:, HEAD_SIZE:] + bias_p[1:2, :].astype(jnp.float32)).astype(jnp.bfloat16)
    go.send(kv_block(column), kv_block(column), kv_sem.at[0], across)
    go.send(kv_block(column), kv_block(column), kv_sem.at[1], sibling)
    spread(3, (2,))
    take_weights(2, 2)
    take_weights(2, 3)

    go.epoch = 1
    scale = math.log2(math.e) / math.sqrt(HEAD_SIZE)

    def make_queries(g):
        field = whole_product(g)
        for i in range(2):
            cut = slice(i * HEAD_SIZE, (i + 1) * HEAD_SIZE)
            head = field[:, cut] + bias_b[pl.ds(z * GROUP + (g - 1) * 2 + i, 1), :]
            turned = (rotate(head, cosine, sine) * scale).astype(jnp.bfloat16)
            queries[g - 1, :, i * span : (i + 1) * span, :] = turned.reshape(depth, span, HEAD_SIZE)

    weights_across(1)
    make_queries(1)
    kv_across = kv_block((1 - x) * CORES + c)
    go.arrive(kv_across, kv_sem.at[0])
    go.send(kv_across, kv_across, kv_sem.at[1], sibling)
    go.arrive(kvs.at[pl.ds(0, CORES)], kv_sem.at[1])

    def att_piece(g, zs, b):
        return att.at[g, zs, pl.ds(pl.multiple_of(b * span, span), span)]

    def nth(i):
        return jnp.where(i == 0, 0, jnp.where(i == 1, last, jnp.where(i == 2, 1 + c, 2 - c)))

    def attend(g, first, end):
        def turn(i, carry):
            b = nth(i)
            scores = lax.dot_general(
                queries[g, b],
                kvs[:, :, :HEAD_SIZE].reshape(PLANE * tokens, HEAD_SIZE),
                (((1,), (1,)), ((), ())),
                preferred_element_type=jnp.float32,
            )
            start = order[b * PLANE + column] * span
            query_pos = start + lax.rem(lax.broadcasted_iota(jnp.int32, (2 * span, 1), 0), span)
            scores = jnp.where(key_pos[...] <= query_pos, scores, -jnp.inf)
            peak = jnp.max(scores, axis=1, keepdims=True)
            shares = jnp.exp2(scores - peak)
            totals = jnp.sum(shares, axis=1, keepdims=True)
            summed = jnp.dot(
                shares.astype(jnp.bfloat16),
                kvs[:, :, HEAD_SIZE:].reshape(PLANE * tokens, HEAD_SIZE),
                preferred_element_type=jnp.float32,
            )
            result = (summed / totals).astype(jnp.bfloat16)
            place = pl.ds(pl.multiple_of(b * span, span), span)
            att[g, z, place, :HEAD_SIZE] = result[:span]
            att[g, z, place, HEAD_SIZE:] = result[span:]
            block = att_piece(g, z, b)
            go.remote(block, block, att_sem.at[g, z, b], (at(gatherer, x, c), t)).start()
            return carry

        lax.fori_loop(first, end, turn, 0)

    attend(0, 0, depth)

    @pl.when(middle)
    def _():
        block = outw.at[0, column]
        go.arrive(block, out_end_sem.at[0])
        go.remote(block, block, out_across_sem.at[0], across).start()
        go.remote(block, block, out_side_sem.at[0], sibling).start()

    go.count(outw.at[0, 0], inner, times=2)
    weights_across(2)
    make_queries(2)
    attend(1, 0, depth)
    go.count(att.at[0, 0], times=2)

    def hand_on(g, i):
        block, sem = att_piece(g, own_end, nth(i)), att_sem.at[g, own_end, nth(i)]
        go.arrive(block, sem)
        go.remote(block, block, sem, (at(last - z, x, c), t)).start()

    halves = PLANE
    each = PLANE // halves
    share = depth // 2

    def piece(ref, i, h):
        return ref.at[i, pl.ds(h * each, each)]

    def term(e, m, g, zs, place):
        first = zs * 2 * PAIR + g * PAIR
        return jnp.dot(att[g, zs, place, :], outw[e, m, first : first + PAIR, :], preferred_element_type=jnp.float32)

    def premix():
        for m in range(PLANE):
            premixed[m] = sum(term(1, m, g, zs, slice(None)) for zs in range(1, last) for g in range(2))

    def mix_block(e, b):
        place = pl.ds(pl.multiple_of(b * span, span), span)
        owner = own_end if e == 0 else z
        for h in range(halves):
            for m in range(h * each, (h + 1) * each):
                total = sum(term(e, m, g, zs, place) for zs in ((0, last) if e else range(depth)) for g in range(2))
                if e:
                    total = total + premixed[m, place, :]
                value = total.astype(jnp.bfloat16)

                @pl.when(b == z)
                def _():
                    terms[owner, m] = value

                @pl.when(b != z)
                def _():
                    part[e, b, m] = value

            index = lax.rem(owner, share)
            stays = owner // share == t

            @pl.when(jnp.logical_and(b != z, stays))
            def _():
                source = piece(part.at[e], b, h)
                go.remote(source, piece(terms, owner, h), term_sem.at[owner, h], (at(b, x, c), t)).start()

            @pl.when(jnp.logical_and(b != z, jnp.logical_not(stays)))
            def _():
                source = piece(part.at[e], b, h)
                go.remote(source, piece(others, index, h), other_sem.at[index, h], (at(b, x, c), 1 - t)).start()

            @pl.when(jnp.logical_and(b == z, jnp.logical_not(stays)))
            def _():
                source = piece(terms, owner, h)
                go.remote(source, piece(others, index, h), other_sem.at[index, h], other, cross_sem.at[0]).start()

    @pl.when(middle)
    def _():
        def side_columns(e):
            block = outw.at[e, (1 - x) * CORES + c]
            go.arrive(block, out_across_sem.at[e])
            go.remote(block, block, out_side_sem.at[e], sibling).start()

        side_columns(1)
        for i in range(depth):
            hand_on(0, i)
        go.arrive(outw.at[1, pl.ds(0, CORES)], out_side_sem.at[1])
        for i in range(depth):
            for g in range(2):
                go.arrive(att_piece(g, last - z, nth(i)), att_sem.at[g, last - z, nth(i)])
        premix()

        def mix_own(i):
            for g in range(2):
                go.arrive(att_piece(g, last - own_end, nth(i)), att_sem.at[g, last - own_end, nth(i)])
            mix_block(1, nth(i))

        for i in range(depth - 1):
            hand_on(1, i)
        mix_own(0)
        hand_on(1, depth - 1)
        mix_own(1)
        side_columns(0)
        mix_own(2)
        go.arrive(outw.at[0, pl.ds(0, CORES)], out_side_sem.at[0])
        for i in range(depth - 1):
            mix_block(0, nth(i))
        mix_own(depth - 1)
        mix_block(0, nth(depth - 1))

    go.count(outw.at[0, 0], inner, times=2)
    go.count(att.at[:, 0], inner)
    go.count(part.at[0, 0], inner, times=2 * (depth - 1))

    crosses = jnp.logical_and(middle, t != z // share)
    maker = jnp.where(t == 0, 1, last - 1)
    width = w_out.shape[1]
    sums = jnp.zeros((span, 1), jnp.float32)
    pieces = [(j, m) for j in range(share) for m in range(PLANE)]
    for j, m in pieces:
        if m % each == 0:
            h = m // each
            go.arrive(piece(terms, t * share + j, h), term_sem.at[t * share + j, h], z != maker)
            go.arrive(piece(others, j, h), other_sem.at[j, h])
        cut = slice((j * PLANE + m) * width, (j * PLANE + m + 1) * width)
        mixed = terms[t * share + j, m].astype(jnp.float32) + others[j, m].astype(jnp.float32)
        mixed_rows[:, cut] = mixed
        stream = rows[z, t, :, cut].astype(jnp.float32) + mixed
        sums = sums + jnp.sum(stream * stream, axis=1, keepdims=True)
    write = pltpu.make_async_copy(mixed_rows, mixed_out, local_sem.at[0])
    write.start()
    squares[t] = jnp.broadcast_to(sums, (span, span)).T[:8]
    go.send(squares.at[t], squares.at[t], small_sem.at[2], other, sem=small_sem.at[3])
    go.arrive(squares.at[1 - t], small_sem.at[2])
    total = (squares[0] + squares[1])[:1]
    factor_out[...] = lax.rsqrt(total / (2 * half_width) + eps)
    write.wait()
    go.left(others, cross_sem.at[0], crosses)
    go.left(gain, small_sem.at[1])
    go.left(squares.at[t], small_sem.at[3])
    go.finish()


def per_device_by_column(
    hidden_in,
    span_order,
    norm_gain,
    w_query,
    bias_query,
    key_value_weight,
    bias_kv,
    w_out,
    post_gain,
):
    span, half_width = hidden_in.shape
    n_seq = span_order.shape[0]
    depth = n_seq // PLANE
    slab = w_query.shape[0]
    tokens = depth * span
    vmem, hbm, smem = (pl.BlockSpec(memory_space=m) for m in (pltpu.VMEM, pl.ANY, pltpu.SMEM))
    dma = pltpu.SemaphoreType.DMA
    bf16 = lambda *shape: pltpu.VMEM(shape, jnp.bfloat16)
    f32 = lambda *shape: pltpu.VMEM(shape, jnp.float32)
    width = w_out.shape[1]
    f32_out = lambda *shape: jax.ShapeDtypeStruct(shape, jnp.float32)
    mixed, factor, post = pl.pallas_call(
        lambda *refs: column_kernel(depth, *refs),
        out_shape=(f32_out(span, half_width), f32_out(1, span), f32_out(1, half_width)),
        in_specs=[hbm, smem, vmem, vmem, vmem, hbm, vmem, hbm, hbm],
        out_specs=(hbm, vmem, vmem),
        scratch_shapes=[
            bf16(depth, 2, span, half_width),
            bf16(CORES, depth, span, half_width),
            bf16(2, half_width // HEAD_SIZE, HEAD_SIZE),
            bf16(3, CORES, n_seq // CORES, slab, PAIR),
            bf16(2, PLANE, w_out.shape[0], width),
            bf16(PLANE, tokens, PAIR),
            bf16(2, depth, 2 * span, HEAD_SIZE),
            bf16(2, depth, tokens, PAIR),
            bf16(2, depth, PLANE, span, width),
            bf16(depth, PLANE, span, width),
            bf16(depth // 2, PLANE, span, width),
            f32(2, 8, span),
            bf16(depth, slab, PAIR),
            f32(depth, span, HEAD_SIZE),
            f32(depth, span, HEAD_SIZE),
            pltpu.VMEM((1, PLANE * tokens), jnp.int32),
            f32(2, 1, half_width),
            f32(half_width // HEAD_SIZE, HEAD_SIZE),
            bf16(2, HEAD_SIZE),
            f32(tokens, PAIR),
            f32(PLANE, tokens, width),
            f32(span, half_width),
            bf16(3072, half_width),
            dma((5,)),
            dma((2,)),
            dma((4,)),
            dma((1,)),
            dma((depth, PIECES)),
            dma((depth,)),
            dma((3, depth)),
            dma((3,)),
            dma((3,)),
            dma((1,)),
            dma((2,)),
            dma((2,)),
            dma((2,)),
            dma((2, depth, depth)),
            dma((depth, PLANE)),
            dma((depth // 2, PLANE)),
            dma((1,)),
        ],
        compiler_params=pltpu.CompilerParams(
            collective_id=0, has_side_effects=True, vmem_limit_bytes=60 * 1024 * 1024
        ),
        name="sublayer",
    )(
        hidden_in,
        span_order,
        norm_gain.reshape(-1, HEAD_SIZE),
        post_gain.reshape(-1, HEAD_SIZE),
        bias_query.reshape(-1, HEAD_SIZE),
        w_query,
        key_value_weight,
        bias_kv,
        w_out,
    )
    stream = hidden_in.astype(jnp.float32) + mixed
    normed = (stream * factor.reshape(span, 1) * post).astype(jnp.bfloat16)
    return (mixed.astype(jnp.bfloat16), normed)


def per_device(*args):
    hidden_in, span_order, w_query, kv_weight = args[0], args[1], args[3], args[5]
    n_seq = span_order.shape[0]
    n_tp = MODEL_WIDTH // hidden_in.shape[1]
    heads = w_query.shape[1] // HEAD_SIZE
    kv_heads = kv_weight.shape[2] // HEAD_SIZE
    if n_tp == 2 and n_seq == 4 * PLANE and kv_heads == 4 and heads == kv_heads * GROUP:
        return per_device_by_column(*args)
    return per_device_by_span(*args)


def solution(mesh):
    placed = (
        P("seq", "tp"),
        P(),
        P("tp"),
        P("seq", "tp"),
        P("tp"),
        P("seq", None, "tp"),
        P(None, "tp"),
        P("tp", "seq"),
        P("tp"),
    )
    return jax.shard_map(
        per_device,
        mesh=mesh,
        in_specs=placed,
        out_specs=(P("seq", "tp"), P("seq", "tp")),
        check_vma=False,
    )
```

```python
import math

import jax
import jax.numpy as jnp
from jax import lax
from jax.experimental import pallas as pl
from jax.experimental.pallas import tpu as pltpu
from jax.sharding import PartitionSpec as P

MODEL_WIDTH = 4096
HEAD_SIZE = 128
GROUP = 4


eps = 1e-06
rope_base = 1000000.0


def apply_rotary(field, token_positions):
    half = field.shape[-1] // 2
    inverse = jnp.exp(-math.log(rope_base) * jnp.arange(half, dtype=jnp.float32) / half)
    angles = token_positions.astype(jnp.float32)[:, None] * inverse[None, :]
    cosine = jnp.cos(angles)[:, None, :]
    sine = jnp.sin(angles)[:, None, :]
    first = field[..., :half]
    second = field[..., half:]
    return jnp.concatenate(
        [first * cosine - second * sine, second * cosine + first * sine], axis=-1
    )


def span_lookup(order, devices):
    table_ids = jnp.arange(order.shape[0], dtype=jnp.int32)
    return jnp.sum(jnp.where(devices[:, None] == table_ids[None, :], order[None, :], 0), axis=1)


def per_device_by_span(
    hidden_in,
    span_order,
    norm_gain,
    w_query,
    bias_query,
    key_value_weight,
    bias_kv,
    w_out,
    post_gain,
):
    tok_rows = hidden_in.shape[0]
    seq_index = lax.axis_index("seq")
    own_span = span_lookup(span_order, jnp.full((1,), seq_index, jnp.int32))[0]
    token_positions = own_span * tok_rows + jnp.arange(tok_rows, dtype=jnp.int32)
    local = hidden_in.astype(jnp.float32)
    raw_rows, gains = (
        lax.all_gather(hidden_in, "tp", axis=1, tiled=True),
        lax.all_gather(norm_gain[None, :], "tp", axis=1, tiled=True),
    )
    full_rows = raw_rows.astype(jnp.float32)
    meansq = jnp.mean(full_rows * full_rows, axis=1, keepdims=True)
    normed_in = (full_rows * lax.rsqrt(meansq + eps) * gains.astype(jnp.float32)).astype(
        jnp.bfloat16
    )
    columns = normed_in
    query_proj = jnp.dot(
        columns,
        lax.all_gather(w_query, "seq", axis=0, tiled=True),
        preferred_element_type=jnp.float32,
    )
    columns = normed_in
    pair_proj = jnp.einsum(
        "tr,rkc->tkc",
        columns,
        lax.all_gather(key_value_weight, "seq", axis=0, tiled=True),
        preferred_element_type=jnp.float32,
    )
    query_heads = w_query.shape[1] // HEAD_SIZE
    kv_heads = key_value_weight.shape[2] // HEAD_SIZE
    query_proj = query_proj + bias_query.astype(jnp.float32)[None, :]
    queries = apply_rotary(
        query_proj.reshape(tok_rows, query_heads, HEAD_SIZE), token_positions
    ).astype(jnp.bfloat16)
    pair_proj = pair_proj + bias_kv.astype(jnp.float32)[None, :, :]
    rotated_keys = apply_rotary(
        pair_proj[:, 0, :].reshape(tok_rows, kv_heads, HEAD_SIZE), token_positions
    )
    rotated_keys = rotated_keys.astype(jnp.bfloat16).reshape(tok_rows, kv_heads * HEAD_SIZE)
    value_rows = pair_proj[:, 1, :].astype(jnp.bfloat16)
    grouped = (
        queries.reshape(tok_rows, kv_heads, GROUP, HEAD_SIZE)
        .transpose(1, 2, 0, 3)
        .reshape(kv_heads, GROUP * tok_rows, HEAD_SIZE)
    )
    query_pos = jnp.tile(token_positions, GROUP)
    last_query = jnp.max(token_positions)
    scale = 1.0 / math.sqrt(HEAD_SIZE)
    start_state = (
        jnp.full((kv_heads, GROUP * tok_rows), -1e30, jnp.float32),
        jnp.zeros((kv_heads, GROUP * tok_rows), jnp.float32),
        jnp.zeros((kv_heads, GROUP * tok_rows, HEAD_SIZE), jnp.float32),
    )
    key_piece = lax.all_gather(rotated_keys, "seq", axis=0, tiled=True)
    value_piece = lax.all_gather(value_rows, "seq", axis=0, tiled=True)
    count = key_piece.shape[0]
    block = math.gcd(count, 1536)

    def visit(step, state):
        first = step * block
        key_block = lax.dynamic_slice_in_dim(key_piece, first, block, 0).reshape(
            block, kv_heads, HEAD_SIZE
        )
        value_block = lax.dynamic_slice_in_dim(value_piece, first, block, 0).reshape(
            block, kv_heads, HEAD_SIZE
        )
        row_ids = first + jnp.arange(block, dtype=jnp.int32)
        key_pos = span_lookup(span_order, row_ids // tok_rows) * tok_rows + row_ids % tok_rows

        def update(current):
            maxima, totals, sums = current
            scores = (
                jnp.einsum("kqd,nkd->kqn", grouped, key_block, preferred_element_type=jnp.float32)
                * scale
            )
            allowed = (key_pos[None, :] <= query_pos[:, None])[None, :, :]
            scores = jnp.where(allowed, scores, -1e30)
            fresh = jnp.maximum(maxima, jnp.max(scores, axis=2))
            weights = jnp.where(allowed, jnp.exp(scores - fresh[:, :, None]), 0.0)
            factor = jnp.exp(maxima - fresh)
            totals = totals * factor + jnp.sum(weights, axis=2)
            sums = sums * factor[:, :, None] + jnp.einsum(
                "kqn,nkd->kqd",
                weights.astype(jnp.bfloat16),
                value_block,
                preferred_element_type=jnp.float32,
            )
            return (fresh, totals, sums)

        return lax.cond(jnp.min(key_pos) <= last_query, update, lambda current: current, state)

    maxima, totals, sums = lax.fori_loop(0, count // block, visit, start_state)
    attended = (sums / totals[:, :, None]).astype(jnp.bfloat16)
    attended = (
        attended.reshape(kv_heads, GROUP, tok_rows, HEAD_SIZE)
        .transpose(2, 0, 1, 3)
        .reshape(tok_rows, query_heads * HEAD_SIZE)
    )
    partial_out = jnp.dot(
        attended,
        lax.all_gather(w_out, "seq", axis=1, tiled=True),
        preferred_element_type=jnp.float32,
    )
    mixed = lax.psum_scatter(
        partial_out.astype(jnp.bfloat16), "tp", scatter_dimension=1, tiled=True
    ).astype(jnp.float32)
    attn_out = mixed.astype(jnp.bfloat16)
    stream = local + mixed
    post_sq = lax.psum(jnp.sum(stream * stream, axis=1), "tp")
    normed = (
        stream
        * lax.rsqrt(post_sq / MODEL_WIDTH + eps)[:, None]
        * post_gain.astype(jnp.float32)[None, :]
    ).astype(jnp.bfloat16)
    return (attn_out, normed)


MESH = pl.DeviceIdType.MESH
CORES = 2
PLANE = 4
PIECES = 4
PAIR = 2 * HEAD_SIZE


def at(z, x, c):
    return z * PLANE + x * CORES + c


class Traffic:
    def __init__(self, depth, z, sem, proxy, peer):
        self.z, self.sem, self.proxy, self.peer = z, sem, proxy, peer
        self.rows, self.epoch = [[0] * depth, [0] * depth], 0

    def remote(self, source, landing, arrival, target, sem=None):
        return pltpu.make_async_remote_copy(
            src_ref=source,
            dst_ref=landing,
            send_sem=self.sem.at[self.epoch] if sem is None else sem,
            recv_sem=arrival,
            device_id=target,
            device_id_type=MESH,
        )

    def count(self, ref, where=None, times=1):
        size = math.prod(ref.shape) * times // self.proxy.shape[1]
        rows = self.rows[self.epoch]
        for k in range(len(rows)):
            if where is None or where(k):
                rows[k] += size

    def send(self, source, landing, arrival, target, where=None, also=None, sem=None):
        when = None if where is None else where(self.z)
        if also is not None:
            when = also if when is None else jnp.logical_and(when, also)
        guarded(when, lambda: self.remote(source, landing, arrival, target, sem).start())
        if sem is None and also is None:
            self.count(source, where)

    def arrive(self, landing, arrival, when=None):
        guarded(when, lambda: self.remote(landing, landing, arrival, self.peer).wait_recv())

    def left(self, source, sem, when=None):
        guarded(when, lambda: self.remote(source, source, sem, self.peer, sem).wait_send())

    def finish(self):
        for epoch, rows in enumerate(self.rows):
            for k, size in enumerate(rows):
                block = self.proxy.at[pl.ds(0, size)]
                self.left(block, self.sem.at[epoch], self.z == k)


def guarded(when, action):
    if when is None:
        action()
    else:
        pl.when(when)(action)


def rotate(field, cosine, sine):
    return field * cosine + pltpu.roll(field, HEAD_SIZE // 2, 1) * sine


def column_kernel(
    depth,
    hidden, order, gain, post_gain, bias_q, wq, wkv, bias_kv, w_out,
    mixed_out, factor_out, post_out,
    rows, full, gains, weights, outw, kvs, queries, att, part, terms, others, squares,
    kv_pieces, cos_t, sin_t, key_pos, gain_rows, bias_b, bias_p, early, premixed, mixed_rows, proxy,
    local_sem, send_sem, small_sem, relay_sem, rows_sem, rows_side_sem,
    w_sem, w_across_sem, w_side_sem, out_end_sem, out_across_sem, out_side_sem, kv_sem, att_sem, term_sem, other_sem, cross_sem,
):
    s, t = lax.axis_index("seq"), lax.axis_index("tp")
    z, x, c = s // PLANE, s % PLANE // CORES, s % CORES
    last = depth - 1
    span, half_width = hidden.shape
    slab = wq.shape[0]
    column = x * CORES + c
    sibling, across, other = (at(z, x, 1 - c), t), (at(z, 1 - x, c), t), (s, 1 - t)
    above, below = (at(jnp.minimum(z + 1, last), x, c), t), (at(jnp.maximum(z - 1, 0), x, c), t)

    barrier = pltpu.get_barrier_semaphore()
    peers = [sibling, across, other] + [(at(lax.rem(z + d, depth), x, c), t) for d in range(1, depth)]
    peers += [(at(lax.rem(z + d, depth), x, c), 1 - t) for d in range(1, depth)]
    for peer in peers:
        pl.semaphore_signal(barrier, inc=1, device_id=peer, device_id_type=MESH)
    pl.semaphore_wait(barrier, len(peers))

    go = Traffic(depth, z, send_sem, proxy, sibling)
    edge = span // PIECES

    def bit(p):
        return pl.ds(p * edge, edge)

    go.send(gain, gains.at[t], small_sem.at[0], other, sem=small_sem.at[1])
    for p in range(PIECES):
        mine, landing = hidden.at[bit(p)], rows.at[z, t, bit(p)]
        go.send(mine, landing, rows_side_sem.at[z], other)
        go.send(mine, landing, rows_sem.at[z, p], above, lambda k: k < last)
        go.send(mine, landing, rows_sem.at[z, p], below, lambda k: k > 0)
    own = [
        pltpu.make_async_copy(hidden, rows.at[z, t], local_sem.at[0]),
        pltpu.make_async_copy(
            bias_kv.at[:, pl.ds(pl.multiple_of(z * HEAD_SIZE, HEAD_SIZE), HEAD_SIZE)], bias_p, local_sem.at[1]
        ),
        pltpu.make_async_copy(w_out, outw.at[1, column], local_sem.at[2]),
    ]

    def q_piece(g, zt):
        return wq.at[:, pl.ds(pl.multiple_of(zt * 2 * PAIR + (g - 1) * PAIR, PAIR), PAIR)]

    for g in (1, 2):
        own.append(pltpu.make_async_copy(q_piece(g, z), weights.at[g, c, s // CORES], local_sem.at[2 + g]))
    for copy in own:
        copy.start()
    for zt in range(depth):
        for i in range(2):
            kv_pieces[zt, :, i * HEAD_SIZE : (i + 1) * HEAD_SIZE] = wkv[:, i, zt * HEAD_SIZE : (zt + 1) * HEAD_SIZE]
    weights[0, c, s // CORES] = kv_pieces[z]
    for g in (0, 1, 2):
        source = kv_pieces.at[z] if g == 0 else q_piece(g, z)
        go.send(source, weights.at[g, c, s // CORES], w_across_sem.at[g], across)
        go.send(source, weights.at[g, c, s // CORES], w_side_sem.at[g], sibling)
    inner = lambda k: (k > 0) & (k < last)
    outer = lambda k: (k == 0) | (k == last)
    middle = inner(z)
    go.send(w_out, outw.at[1, column], out_across_sem.at[1], across, inner)
    go.send(w_out, outw.at[1, column], out_side_sem.at[1], sibling, inner)
    own_end = jnp.where(z < depth // 2, 0, last)
    gatherer = jnp.where(middle, last - z, jnp.where(z == 0, 1, last - 1))

    def leave_columns(part_id):
        place = pl.ds(part_id * (w_out.shape[0] // 2), w_out.shape[0] // 2)
        landing = outw.at[0, column, place]
        go.send(w_out.at[place], landing, out_end_sem.at[0], (at(gatherer, x, c), t), outer)

    def spread(stage, groups, least=1):
        for g in groups:
            for zt, where in (
                (stage, lambda k: k <= stage - least),
                (last - stage, lambda k: k >= last - stage + least),
            ):
                source = kv_pieces.at[zt] if g == 0 else q_piece(g, zt)
                go.send(source, weights.at[g, c, s // CORES], w_sem.at[g, z], (at(zt, x, c), t), where)

    def spread_near(stage, g):
        for zt, source in ((stage, stage - 1), (last - stage, last - stage + 1)):
            go.send(q_piece(g, zt), weights.at[g, c, s // CORES], w_sem.at[g, z], (at(zt, x, c), t), lambda k: k == source)

    def take_weights(g, stage, distances=None):
        for distance in distances or range(1, stage + 1):
            for sign, goal in ((-1, stage), (1, last - stage)):
                zs = jnp.clip(z + sign * distance, 0, last)
                block = weights.at[g, c, zs * CORES + x]
                go.arrive(block, w_sem.at[g, zs], z == goal)
                go.send(block, block, w_across_sem.at[g], across, lambda k: k == goal)
                go.send(block, block, w_side_sem.at[g], sibling, lambda k: k == goal)

    def chain(distance, action):
        for sign in (1, -1):
            zs = jnp.clip(z - sign * distance, 0, last)
            where = lambda k: (k >= distance) if sign == 1 else (k + distance <= last)
            target = above if sign == 1 else below
            more = (lambda k: distance <= k < last) if sign == 1 else (lambda k: 0 < k <= last - distance)
            if distance < last:
                now = jnp.logical_and(z >= distance, z < last) if sign == 1 else jnp.logical_and(z > 0, z <= last - distance)
                action(zs, where, target, (more, now))
            else:
                action(zs, where, target, None)

    def relay(block, arrival, target, more, sem=None):
        if more is not None:
            where, now = more
            pl.when(now)(lambda: go.remote(block, block, arrival, target, sem).start())
            if sem is None:
                go.count(block, where)

    def pass_rows(distance):
        for p in range(PIECES):

            def action(zs, where, target, more):
                block = rows.at[zs, t, bit(p)]
                go.arrive(block, rows_sem.at[zs, p], where(z))
                relay(block, rows_sem.at[zs, p], target, more, relay_sem.at[0] if distance == last - 1 else None)
                go.send(block, block, rows_side_sem.at[zs], other, where)

            chain(distance, action)

    def weights_across(g):
        go.arrive(weights.at[g, c, pl.ds(0, depth)], w_across_sem.at[g])
        for zs in range(depth):
            block = weights.at[g, c, zs * CORES + 1 - x]
            go.send(block, block, w_side_sem.at[g], sibling)

    def weights_beside(g):
        go.arrive(weights.at[g, 1 - c], w_side_sem.at[g])

    def normalize(zs):
        go.arrive(rows.at[zs, 1 - t], rows_side_sem.at[zs])

        def strip(i, carry):
            r = pl.ds(pl.multiple_of(i * 16, 16), 16)
            halves = [rows[zs, h, r, :].astype(jnp.float32) for h in range(2)]
            total = sum(jnp.sum(a * a, axis=1, keepdims=True) for a in halves)
            factor = lax.rsqrt(total / (2 * half_width) + eps)
            for h in range(2):
                value = (halves[h] * factor * gain_rows[h]).astype(jnp.bfloat16)
                for i in range(half_width // slab):
                    j, core = divmod(h * (half_width // slab) + i, CORES)
                    full[core, zs, r, j * slab : (j + 1) * slab] = value[:, i * slab : (i + 1) * slab]
            return carry

        lax.fori_loop(0, span // 16, strip, 0)

    lane = lax.broadcasted_iota(jnp.int32, (span, HEAD_SIZE), 1)
    line = lax.broadcasted_iota(jnp.int32, (span, HEAD_SIZE), 0)
    half = HEAD_SIZE // 2
    pair_id = jnp.where(lane < half, lane, lane - half).astype(jnp.float32)
    inverse = jnp.exp(-math.log(rope_base) * pair_id / half)

    def table(zs, carry):
        angles = (order[zs * PLANE + column] * span + line).astype(jnp.float32) * inverse
        cos_t[zs] = jnp.cos(angles)
        sine = jnp.sin(angles)
        sin_t[zs] = jnp.where(lane < half, -sine, sine)
        return carry

    lax.fori_loop(0, depth, table, 0)
    for m in range(PLANE):
        for zs in range(depth):
            i = m * depth + zs
            key_pos[:, i * span : (i + 1) * span] = order[zs * PLANE + m] * span + lax.broadcasted_iota(
                jnp.int32, (1, span), 1
            )
    for copy in own:
        copy.wait()
    gains[t] = gain[...]
    go.arrive(gains.at[1 - t], small_sem.at[0])
    for h in range(2):
        rows_of = gains[h].astype(jnp.float32)
        for i in range(half_width // HEAD_SIZE):
            gain_rows[h, :, i * HEAD_SIZE : (i + 1) * HEAD_SIZE] = rows_of[i : i + 1]
    bias_b[...] = bias_q[...].astype(jnp.float32)
    post_rows = post_gain[...].astype(jnp.float32)
    for i in range(half_width // HEAD_SIZE):
        post_out[:, i * HEAD_SIZE : (i + 1) * HEAD_SIZE] = post_rows[i : i + 1]

    pass_rows(1)
    spread(1, (0, 1, 2))
    spread(3, (0,))
    spread_near(3, 1)
    leave_columns(0)
    normalize(z)
    pass_rows(2)
    spread(2, (0, 1, 2))
    for g in (0, 1, 2):
        take_weights(g, 1)
    normalize(z + 1 - 2 * lax.rem(z, 2))
    take_weights(0, 3)
    take_weights(1, 3, (1,))
    take_weights(0, 2)
    go.left(rows.at[z, t], relay_sem.at[0], middle)
    pass_rows(3)
    spread(3, (1,), 2)
    leave_columns(1)
    take_weights(1, 2)
    normalize(lax.rem(z + 2, depth))
    take_weights(1, 3, (2, 3))
    normalize(last - z)
    weights_across(0)

    tokens = depth * span

    def kv_block(i):
        return kvs.at[i]

    def product(g, core):
        return jnp.dot(
            full[core].reshape(tokens, half_width),
            weights[g, core].reshape(half_width, PAIR),
            preferred_element_type=jnp.float32,
        )

    def whole_product(g):
        early[...] = product(g, c)
        weights_beside(g)
        return early[...] + product(g, 1 - c)

    cosine, sine = cos_t[...].reshape(tokens, HEAD_SIZE), sin_t[...].reshape(tokens, HEAD_SIZE)
    pair = whole_product(0)
    keys = pair[:, :HEAD_SIZE] + bias_p[0:1, :].astype(jnp.float32)
    kvs[column, :, :HEAD_SIZE] = rotate(keys, cosine, sine).astype(jnp.bfloat16)
    kvs[column, :, HEAD_SIZE:] = (pair[:, HEAD_SIZE:] + bias_p[1:2, :].astype(jnp.float32)).astype(jnp.bfloat16)
    go.send(kv_block(column), kv_block(column), kv_sem.at[0], across)
    go.send(kv_block(column), kv_block(column), kv_sem.at[1], sibling)
    spread(3, (2,))
    take_weights(2, 2)
    take_weights(2, 3)

    go.epoch = 1
    scale = math.log2(math.e) / math.sqrt(HEAD_SIZE)

    def make_queries(g):
        field = whole_product(g)
        for i in range(2):
            cut = slice(i * HEAD_SIZE, (i + 1) * HEAD_SIZE)
            head = field[:, cut] + bias_b[pl.ds(z * GROUP + (g - 1) * 2 + i, 1), :]
            turned = (rotate(head, cosine, sine) * scale).astype(jnp.bfloat16)
            queries[g - 1, :, i * span : (i + 1) * span, :] = turned.reshape(depth, span, HEAD_SIZE)

    weights_across(1)
    make_queries(1)
    kv_across = kv_block((1 - x) * CORES + c)
    go.arrive(kv_across, kv_sem.at[0])
    go.send(kv_across, kv_across, kv_sem.at[1], sibling)
    go.arrive(kvs.at[pl.ds(0, CORES)], kv_sem.at[1])

    def att_piece(g, zs, b):
        return att.at[g, zs, pl.ds(pl.multiple_of(b * span, span), span)]

    def nth(i):
        return jnp.where(i == 0, 0, jnp.where(i == 1, last, jnp.where(i == 2, 1 + c, 2 - c)))

    def attend(g, first, end):
        def turn(i, carry):
            b = nth(i)
            scores = lax.dot_general(
                queries[g, b],
                kvs[:, :, :HEAD_SIZE].reshape(PLANE * tokens, HEAD_SIZE),
                (((1,), (1,)), ((), ())),
                preferred_element_type=jnp.float32,
            )
            start = order[b * PLANE + column] * span
            query_pos = start + lax.rem(lax.broadcasted_iota(jnp.int32, (2 * span, 1), 0), span)
            scores = jnp.where(key_pos[...] <= query_pos, scores, -jnp.inf)
            peak = jnp.max(scores, axis=1, keepdims=True)
            shares = jnp.exp2(scores - peak)
            totals = jnp.sum(shares, axis=1, keepdims=True)
            summed = jnp.dot(
                shares.astype(jnp.bfloat16),
                kvs[:, :, HEAD_SIZE:].reshape(PLANE * tokens, HEAD_SIZE),
                preferred_element_type=jnp.float32,
            )
            result = (summed / totals).astype(jnp.bfloat16)
            place = pl.ds(pl.multiple_of(b * span, span), span)
            att[g, z, place, :HEAD_SIZE] = result[:span]
            att[g, z, place, HEAD_SIZE:] = result[span:]
            block = att_piece(g, z, b)
            go.remote(block, block, att_sem.at[g, z, b], (at(gatherer, x, c), t)).start()
            return carry

        lax.fori_loop(first, end, turn, 0)

    attend(0, 0, depth)

    @pl.when(middle)
    def _():
        block = outw.at[0, column]
        go.arrive(block, out_end_sem.at[0])
        go.remote(block, block, out_across_sem.at[0], across).start()
        go.remote(block, block, out_side_sem.at[0], sibling).start()

    go.count(outw.at[0, 0], inner, times=2)
    weights_across(2)
    make_queries(2)
    attend(1, 0, depth)
    go.count(att.at[0, 0], times=2)

    def hand_on(g, i):
        block, sem = att_piece(g, own_end, nth(i)), att_sem.at[g, own_end, nth(i)]
        go.arrive(block, sem)
        go.remote(block, block, sem, (at(last - z, x, c), t)).start()

    halves = PLANE
    each = PLANE // halves
    share = depth // 2

    def piece(ref, i, h):
        return ref.at[i, pl.ds(h * each, each)]

    def term(e, m, g, zs, place):
        first = zs * 2 * PAIR + g * PAIR
        return jnp.dot(att[g, zs, place, :], outw[e, m, first : first + PAIR, :], preferred_element_type=jnp.float32)

    def premix():
        for m in range(PLANE):
            premixed[m] = sum(term(1, m, g, zs, slice(None)) for zs in range(1, last) for g in range(2))

    def mix_block(e, b):
        place = pl.ds(pl.multiple_of(b * span, span), span)
        owner = own_end if e == 0 else z
        for h in range(halves):
            for m in range(h * each, (h + 1) * each):
                total = sum(term(e, m, g, zs, place) for zs in ((0, last) if e else range(depth)) for g in range(2))
                if e:
                    total = total + premixed[m, place, :]
                value = total.astype(jnp.bfloat16)

                @pl.when(b == z)
                def _():
                    terms[owner, m] = value

                @pl.when(b != z)
                def _():
                    part[e, b, m] = value

            index = lax.rem(owner, share)
            stays = owner // share == t

            @pl.when(jnp.logical_and(b != z, stays))
            def _():
                source = piece(part.at[e], b, h)
                go.remote(source, piece(terms, owner, h), term_sem.at[owner, h], (at(b, x, c), t)).start()

            @pl.when(jnp.logical_and(b != z, jnp.logical_not(stays)))
            def _():
                source = piece(part.at[e], b, h)
                go.remote(source, piece(others, index, h), other_sem.at[index, h], (at(b, x, c), 1 - t)).start()

            @pl.when(jnp.logical_and(b == z, jnp.logical_not(stays)))
            def _():
                source = piece(terms, owner, h)
                go.remote(source, piece(others, index, h), other_sem.at[index, h], other, cross_sem.at[0]).start()

    @pl.when(middle)
    def _():
        def side_columns(e):
            block = outw.at[e, (1 - x) * CORES + c]
            go.arrive(block, out_across_sem.at[e])
            go.remote(block, block, out_side_sem.at[e], sibling).start()

        side_columns(1)
        for i in range(depth):
            hand_on(0, i)
        go.arrive(outw.at[1, pl.ds(0, CORES)], out_side_sem.at[1])
        for i in range(depth):
            for g in range(2):
                go.arrive(att_piece(g, last - z, nth(i)), att_sem.at[g, last - z, nth(i)])
        premix()

        def mix_own(i):
            for g in range(2):
                go.arrive(att_piece(g, last - own_end, nth(i)), att_sem.at[g, last - own_end, nth(i)])
            mix_block(1, nth(i))

        for i in range(depth - 1):
            hand_on(1, i)
        mix_own(0)
        hand_on(1, depth - 1)
        mix_own(1)
        side_columns(0)
        mix_own(2)
        go.arrive(outw.at[0, pl.ds(0, CORES)], out_side_sem.at[0])
        for i in range(depth - 1):
            mix_block(0, nth(i))
        mix_own(depth - 1)
        mix_block(0, nth(depth - 1))

    go.count(outw.at[0, 0], inner, times=2)
    go.count(att.at[:, 0], inner)
    go.count(part.at[0, 0], inner, times=2 * (depth - 1))

    crosses = jnp.logical_and(middle, t != z // share)
    maker = jnp.where(t == 0, 1, last - 1)
    width = w_out.shape[1]
    sums = jnp.zeros((span, 1), jnp.float32)
    pieces = [(j, m) for j in range(share) for m in range(PLANE)]
    for j, m in pieces:
        if m % each == 0:
            h = m // each
            go.arrive(piece(terms, t * share + j, h), term_sem.at[t * share + j, h], z != maker)
            go.arrive(piece(others, j, h), other_sem.at[j, h])
        cut = slice((j * PLANE + m) * width, (j * PLANE + m + 1) * width)
        mixed = terms[t * share + j, m].astype(jnp.float32) + others[j, m].astype(jnp.float32)
        mixed_rows[:, cut] = mixed
        stream = rows[z, t, :, cut].astype(jnp.float32) + mixed
        sums = sums + jnp.sum(stream * stream, axis=1, keepdims=True)
    write = pltpu.make_async_copy(mixed_rows, mixed_out, local_sem.at[0])
    write.start()
    squares[t] = jnp.broadcast_to(sums, (span, span)).T[:8]
    go.send(squares.at[t], squares.at[t], small_sem.at[2], other, sem=small_sem.at[3])
    go.arrive(squares.at[1 - t], small_sem.at[2])
    total = (squares[0] + squares[1])[:1]
    factor_out[...] = lax.rsqrt(total / (2 * half_width) + eps)
    write.wait()
    go.left(others, cross_sem.at[0], crosses)
    go.left(gain, small_sem.at[1])
    go.left(squares.at[t], small_sem.at[3])
    go.finish()


def per_device_by_column(
    hidden_in,
    span_order,
    norm_gain,
    w_query,
    bias_query,
    key_value_weight,
    bias_kv,
    w_out,
    post_gain,
):
    span, half_width = hidden_in.shape
    n_seq = span_order.shape[0]
    depth = n_seq // PLANE
    slab = w_query.shape[0]
    tokens = depth * span
    vmem, hbm, smem = (pl.BlockSpec(memory_space=m) for m in (pltpu.VMEM, pl.ANY, pltpu.SMEM))
    dma = pltpu.SemaphoreType.DMA
    bf16 = lambda *shape: pltpu.VMEM(shape, jnp.bfloat16)
    f32 = lambda *shape: pltpu.VMEM(shape, jnp.float32)
    width = w_out.shape[1]
    f32_out = lambda *shape: jax.ShapeDtypeStruct(shape, jnp.float32)
    mixed, factor, post = pl.pallas_call(
        lambda *refs: column_kernel(depth, *refs),
        out_shape=(f32_out(span, half_width), f32_out(1, span), f32_out(1, half_width)),
        in_specs=[hbm, smem, vmem, vmem, vmem, hbm, vmem, hbm, hbm],
        out_specs=(hbm, vmem, vmem),
        scratch_shapes=[
            bf16(depth, 2, span, half_width),
            bf16(CORES, depth, span, half_width),
            bf16(2, half_width // HEAD_SIZE, HEAD_SIZE),
            bf16(3, CORES, n_seq // CORES, slab, PAIR),
            bf16(2, PLANE, w_out.shape[0], width),
            bf16(PLANE, tokens, PAIR),
            bf16(2, depth, 2 * span, HEAD_SIZE),
            bf16(2, depth, tokens, PAIR),
            bf16(2, depth, PLANE, span, width),
            bf16(depth, PLANE, span, width),
            bf16(depth // 2, PLANE, span, width),
            f32(2, 8, span),
            bf16(depth, slab, PAIR),
            f32(depth, span, HEAD_SIZE),
            f32(depth, span, HEAD_SIZE),
            pltpu.VMEM((1, PLANE * tokens), jnp.int32),
            f32(2, 1, half_width),
            f32(half_width // HEAD_SIZE, HEAD_SIZE),
            bf16(2, HEAD_SIZE),
            f32(tokens, PAIR),
            f32(PLANE, tokens, width),
            f32(span, half_width),
            bf16(3072, half_width),
            dma((5,)),
            dma((2,)),
            dma((4,)),
            dma((1,)),
            dma((depth, PIECES)),
            dma((depth,)),
            dma((3, depth)),
            dma((3,)),
            dma((3,)),
            dma((1,)),
            dma((2,)),
            dma((2,)),
            dma((2,)),
            dma((2, depth, depth)),
            dma((depth, PLANE)),
            dma((depth // 2, PLANE)),
            dma((1,)),
        ],
        compiler_params=pltpu.CompilerParams(
            collective_id=0, has_side_effects=True, vmem_limit_bytes=60 * 1024 * 1024
        ),
        name="sublayer",
    )(
        hidden_in,
        span_order,
        norm_gain.reshape(-1, HEAD_SIZE),
        post_gain.reshape(-1, HEAD_SIZE),
        bias_query.reshape(-1, HEAD_SIZE),
        w_query,
        key_value_weight,
        bias_kv,
        w_out,
    )
    stream = hidden_in.astype(jnp.float32) + mixed
    normed = (stream * factor.reshape(span, 1) * post).astype(jnp.bfloat16)
    return (mixed.astype(jnp.bfloat16), normed)


def per_device(*args):
    hidden_in, span_order, w_query, kv_weight = args[0], args[1], args[3], args[5]
    n_seq = span_order.shape[0]
    n_tp = MODEL_WIDTH // hidden_in.shape[1]
    heads = w_query.shape[1] // HEAD_SIZE
    kv_heads = kv_weight.shape[2] // HEAD_SIZE
    if n_tp == 2 and n_seq == 4 * PLANE and kv_heads == 4 and heads == kv_heads * GROUP:
        return per_device_by_column(*args)
    return per_device_by_span(*args)


def solution(mesh):
    placed = (
        P("seq", "tp"),
        P(),
        P("tp"),
        P("seq", "tp"),
        P("tp"),
        P("seq", None, "tp"),
        P(None, "tp"),
        P("tp", "seq"),
        P("tp"),
    )
    return jax.shard_map(
        per_device,
        mesh=mesh,
        in_specs=placed,
        out_specs=(P("seq", "tp"), P("seq", "tp")),
        check_vma=False,
    )
```
